32 devices in a mesh: batch: 4 (over y, z), group: 8 (over x, core).
Axes of the slice: x: 4, y: 2, z: 2, core: 2. Of those that a mesh axis runs over, the one named last changes fastest.
The devices are a block of a 4x4x8 slice.
Arguments:
- sort_keys: float32 [16384], P(('batch', 'group')), parts along dimension 0
- seg_ids: int32 [16384], P(('batch', 'group')), parts along dimension 0
- payload: bfloat16 [16384, 4096], P(('batch', 'group')), parts along dimension 0
Outputs:
- output: bfloat16 [16384, 4096], P(('batch', 'group')), parts along dimension 0
There are 4 independent parts. The reference program is written for one: setup_inputs(seed, part) draws one part's arguments, and reference() takes and returns one part's arrays. A program takes and returns all parts, laid end to end along the dimension named above; each array names one.
All inputs are finite; a program needn't handle non-finite values.
Results may differ from the reference program's by a relative error of at most 0.00654141.
Values are sent between devices in bfloat16 or wider.
A program may use at most 768 MiB of HBM per device.

```python
import jax
import jax.numpy as jnp
from jax import lax

GROUP = 8
ROWS_DEV = 512
WIDTH = 4096
TOTAL = GROUP * ROWS_DEV
PAIR = ROWS_DEV // GROUP


def combine_runs(left_part, right_part):
    left_flag, left_rows = left_part
    right_flag, right_rows = right_part
    joined = jnp.where(right_flag[..., None], right_rows, left_rows + right_rows)
    return jnp.logical_or(left_flag, right_flag), joined


def draw_layout(base_key):
    phase_key, size_key, tie_key, place_key, cut_key, base_id_key = jax.random.split(base_key, 6)
    half_pair = PAIR // 2
    dev_phase = jax.random.permutation(phase_key, GROUP)
    bound_no = jnp.arange(1, GROUP, dtype=jnp.int32)
    bound_phase = (dev_phase[:, None] + bound_no[None, :]) % GROUP
    shift_size = jax.random.randint(size_key, (GROUP, GROUP - 1), 0, half_pair + 1)
    cut_shift = jnp.where(bound_phase < GROUP // 2, jnp.maximum(shift_size, 1), -shift_size)
    cut_shift = jnp.where(bound_phase == GROUP // 2, 0, cut_shift)
    full_dev = dev_phase == GROUP - 2
    cut_shift = cut_shift.at[:, 0].set(jnp.where(full_dev, -half_pair, cut_shift[:, 0]))
    cut_shift = cut_shift.at[:, 1].set(jnp.where(full_dev, half_pair, cut_shift[:, 1]))
    band_cuts = bound_no[None, :] * PAIR + cut_shift
    local_rank = jnp.arange(ROWS_DEV, dtype=jnp.int32)

    def band_search(cut_row):
        return jnp.searchsorted(cut_row, local_rank, side='right')

    band_of = jax.vmap(band_search)(band_cuts).astype(jnp.int32)
    prev_band = jnp.maximum(band_of - 1, 0)
    band_low = jnp.take_along_axis(band_cuts, prev_band, axis=1)
    band_phase = jnp.take_along_axis(bound_phase, prev_band, axis=1)
    lead_row = (band_of >= 1) & (local_rank[None, :] == band_low) & (band_phase == GROUP // 2)
    tie_break = jax.random.permutation(tie_key, TOTAL).reshape(GROUP, ROWS_DEV)
    rank_score = band_of * (TOTAL + 1) + jnp.where(lead_row, 0, tie_break + 1)
    score_order = jnp.argsort(rank_score.reshape(-1), stable=True)
    global_rank = jnp.argsort(score_order, stable=True).astype(jnp.int32).reshape(GROUP, ROWS_DEV)
    place_keys = jax.random.split(place_key, GROUP)

    def place_rows(row_key):
        return jax.random.permutation(row_key, ROWS_DEV)

    placement = jax.vmap(place_rows)(place_keys)
    rank_at = jnp.take_along_axis(global_rank, placement, axis=1).reshape(TOTAL)
    seg_cuts = jnp.sort(jax.random.randint(cut_key, (GROUP - 1,), 1, TOTAL))
    first_id = jax.random.randint(base_id_key, (), 0, 1000)
    seg_ids = (jnp.searchsorted(seg_cuts, rank_at, side='right') + first_id).astype(jnp.int32)
    return rank_at, seg_ids


def setup_inputs(seed: int = 0, part: int = 0) -> dict:
    base_key = jax.random.fold_in(jax.random.key(seed), part)
    layout_key, payload_key = jax.random.split(base_key, 2)
    rank_at, seg_ids = draw_layout(layout_key)
    centred = (2 * rank_at + 1 - TOTAL).astype(jnp.float32) / TOTAL
    sort_keys = centred * centred * centred
    noise = jax.random.normal(payload_key, (TOTAL, WIDTH), jnp.float32)
    payload = (noise * ROWS_DEV ** -0.5).astype(jnp.bfloat16)
    return {'sort_keys': sort_keys, 'seg_ids': seg_ids, 'payload': payload}


def reference(sort_keys, seg_ids, payload):
    row_pos = jnp.arange(sort_keys.shape[0], dtype=jnp.int32)
    _, seg_sorted, sort_order = lax.sort((sort_keys, seg_ids, row_pos), num_keys=1)
    run_rows = payload[sort_order].astype(jnp.float32)
    first_flag = jnp.ones((1,), dtype=jnp.bool_)
    run_start = jnp.concatenate([first_flag, seg_sorted[1:] != seg_sorted[:-1]])
    _, scanned = lax.associative_scan(combine_runs, (run_start, run_rows))
    _, back_order = lax.sort((sort_order, row_pos), num_keys=1)
    return scanned[back_order].astype(jnp.bfloat16)
```

```python
import functools

import jax
import jax.numpy as jnp
from jax import lax
from jax.experimental import pallas as pl
from jax.experimental.pallas import tpu as pltpu
from jax.sharding import PartitionSpec as P

MESH = pl.DeviceIdType.MESH
LANES = 128
CHUNKS = 2
ROW_TILE = 64
DOT_ROWS = 256


def exchange_kernel(n, keys_ref, segs_ref, pay_ref, out_ref, keys_all, segs_all, kcol, scol, mask, slab, res,
                    key_send, key_recv, seg_send, seg_recv, fwd_send, fwd_recv, ret_send, ret_recv):
    me = lax.axis_index('group')
    rows, width = pay_ref.shape
    block = width // n
    cw = block // CHUNKS
    halves = rows // DOT_ROWS
    lane_tiles = rows // LANES

    def peer(k):
        return lax.rem(me + k, n)

    order = [(k + n // 2) % n for k in range(n)]
    order = [k for k in order if k != 0]

    def key_copy(k):
        return pltpu.make_async_remote_copy(
            src_ref=keys_ref.at[0], dst_ref=keys_all.at[me], send_sem=key_send.at[k], recv_sem=key_recv.at[me],
            device_id={'group': peer(k)}, device_id_type=MESH)

    def seg_copy(k):
        return pltpu.make_async_remote_copy(
            src_ref=segs_ref.at[0], dst_ref=segs_all.at[me], send_sem=seg_send.at[k], recv_sem=seg_recv.at[me],
            device_id={'group': peer(k)}, device_id_type=MESH)

    def columns(dev, c):
        return pl.ds(pl.multiple_of(dev * block + c * cw, LANES), cw)

    def my_rows(dev):
        return pl.ds(pl.multiple_of(dev * rows, rows), rows)

    def fwd_copy(k, c):
        return pltpu.make_async_remote_copy(
            src_ref=pay_ref.at[:, columns(peer(k), c)], dst_ref=slab.at[c, my_rows(me), :],
            send_sem=fwd_send.at[k, c], recv_sem=fwd_recv.at[me, c],
            device_id={'group': peer(k)}, device_id_type=MESH)

    def ret_copy(dev, h, c):
        src_rows = pl.ds(pl.multiple_of(dev * rows + h * DOT_ROWS, DOT_ROWS), DOT_ROWS)
        dst_rows = pl.ds(pl.multiple_of(h * DOT_ROWS, DOT_ROWS), DOT_ROWS)
        return pltpu.make_async_remote_copy(
            src_ref=res.at[c, src_rows, :], dst_ref=out_ref.at[dst_rows, columns(me, c)],
            send_sem=ret_send.at[dev, c, h], recv_sem=ret_recv.at[me, c, h],
            device_id={'group': dev}, device_id_type=MESH)

    def ret_local(h, c):
        src_rows = pl.ds(pl.multiple_of(me * rows + h * DOT_ROWS, DOT_ROWS), DOT_ROWS)
        dst_rows = pl.ds(pl.multiple_of(h * DOT_ROWS, DOT_ROWS), DOT_ROWS)
        return pltpu.make_async_copy(res.at[c, src_rows, :], out_ref.at[dst_rows, columns(me, c)],
                                     ret_recv.at[me, c, h])

    own_copies = [pltpu.make_async_copy(keys_ref.at[0], keys_all.at[me], key_recv.at[me]),
                  pltpu.make_async_copy(segs_ref.at[0], segs_all.at[me], seg_recv.at[me])]
    own_copies += [pltpu.make_async_copy(pay_ref.at[:, columns(me, c)], slab.at[c, my_rows(me), :], fwd_recv.at[me, c])
                   for c in range(CHUNKS)]

    barrier = pltpu.get_barrier_semaphore()
    for k in range(1, n):
        pl.semaphore_signal(barrier, inc=1, device_id={'group': peer(k)}, device_id_type=MESH)
    for copy in own_copies:
        copy.start()
    pl.semaphore_wait(barrier, n - 1)

    for k in order:
        key_copy(k).start()
        seg_copy(k).start()
    for c in range(CHUNKS):
        for k in order:
            fwd_copy(k, c).start()

    own_copies[0].wait()
    own_copies[1].wait()
    for k in order:
        src = peer(k)
        pltpu.make_async_copy(keys_ref.at[0], keys_all.at[src], key_recv.at[src]).wait()
        pltpu.make_async_copy(segs_ref.at[0], segs_all.at[src], seg_recv.at[src]).wait()

    def spread(dev, carry):
        for j in range(lane_tiles):
            lanes = slice(j * LANES, (j + 1) * LANES)
            dst = pl.ds(pl.multiple_of(dev * rows + j * LANES, LANES), LANES)
            kcol[dst, :] = jnp.broadcast_to(keys_all[dev, :, lanes], (LANES, LANES)).T
            scol[dst, :] = jnp.broadcast_to(segs_all[dev, :, lanes], (LANES, LANES)).T
        return carry

    lax.fori_loop(0, n, spread, 0)

    def build(t, carry):
        here = pl.ds(pl.multiple_of(t * ROW_TILE, ROW_TILE), ROW_TILE)
        key_r, seg_r = kcol[here, :], scol[here, :]
        last = jnp.full((ROW_TILE, LANES), -jnp.inf, jnp.float32)
        for dev in range(n):
            for j in range(lane_tiles):
                lanes = slice(j * LANES, (j + 1) * LANES)
                key_s, seg_s = keys_all[dev, :, lanes], segs_all[dev, :, lanes]
                other = jnp.logical_and(key_s < key_r, seg_s != seg_r)
                last = jnp.maximum(last, jnp.where(other, key_s, -jnp.inf))
        last = jnp.broadcast_to(jnp.max(last, axis=1, keepdims=True), (ROW_TILE, LANES))
        for dev in range(n):
            for j in range(lane_tiles):
                lanes = slice(j * LANES, (j + 1) * LANES)
                key_s = keys_all[dev, :, lanes]
                inside = jnp.logical_and(key_s <= key_r, key_s > last)
                at = slice(dev * rows + j * LANES, dev * rows + (j + 1) * LANES)
                mask[here, at] = jnp.where(inside, 1.0, 0.0).astype(jnp.bfloat16)
        return carry

    lax.fori_loop(0, n * rows // ROW_TILE, build, 0)

    def send_back(step, c):
        dev = lax.rem(me + n // 2 + step // halves, n)
        h = lax.rem(step, halves)

        @pl.when(dev != me)
        def _():
            ret_copy(dev, h, c).start()

        @pl.when(dev == me)
        def _():
            ret_local(h, c).start()

    for c in range(CHUNKS):
        own_copies[2 + c].wait()
        for k in order:
            src = peer(k)
            pltpu.make_async_copy(pay_ref.at[:, columns(me, c)], slab.at[c, my_rows(src), :], fwd_recv.at[src, c]).wait()

        def dot_step(step, carry, c=c):
            dev = lax.rem(me + n // 2 + step // halves, n)
            at = pl.ds(pl.multiple_of(dev * rows + lax.rem(step, halves) * DOT_ROWS, DOT_ROWS), DOT_ROWS)
            total = jnp.dot(mask[at, :], slab[c], preferred_element_type=jnp.float32)
            res[c, at, :] = total.astype(jnp.bfloat16)

            @pl.when(step > 0)
            def _():
                send_back(step - 1, c)

            return carry

        lax.fori_loop(0, n * halves, dot_step, 0)
        send_back(n * halves - 1, c)

    for k in order:
        key_copy(k).wait_send()
        seg_copy(k).wait_send()
        for c in range(CHUNKS):
            fwd_copy(k, c).wait_send()
    for c in range(CHUNKS):
        for h in range(halves):
            for k in order:
                ret_copy(peer(k), h, c).wait_send()
            ret_local(h, c).wait()
            for k in order:
                src = peer(k)
                dst_rows = pl.ds(h * DOT_ROWS, DOT_ROWS)
                pltpu.make_async_copy(res.at[c, pl.ds(0, DOT_ROWS), :], out_ref.at[dst_rows, columns(src, c)],
                                      ret_recv.at[src, c, h]).wait()


def solution(mesh):
    n = mesh.shape['group']

    def per_device(sort_keys, seg_ids, payload):
        rows, width = payload.shape
        total = n * rows
        cw = width // n // CHUNKS
        halves = rows // DOT_ROWS
        dma = pltpu.SemaphoreType.DMA
        return pl.pallas_call(
            functools.partial(exchange_kernel, n),
            out_shape=jax.ShapeDtypeStruct((rows, width), jnp.bfloat16),
            in_specs=[pl.BlockSpec(memory_space=pl.ANY)] * 3,
            out_specs=pl.BlockSpec(memory_space=pl.ANY),
            scratch_shapes=[
                pltpu.VMEM((n, 1, rows), jnp.float32),
                pltpu.VMEM((n, 1, rows), jnp.int32),
                pltpu.VMEM((total, LANES), jnp.float32),
                pltpu.VMEM((total, LANES), jnp.int32),
                pltpu.VMEM((total, total), jnp.bfloat16),
                pltpu.VMEM((CHUNKS, total, cw), jnp.bfloat16),
                pltpu.VMEM((CHUNKS, total, cw), jnp.bfloat16),
                dma((n,)), dma((n,)), dma((n,)), dma((n,)),
                dma((n, CHUNKS)), dma((n, CHUNKS)),
                dma((n, CHUNKS, halves)), dma((n, CHUNKS, halves)),
            ],
            compiler_params=pltpu.CompilerParams(collective_id=0, has_side_effects=True,
                                                 vmem_limit_bytes=56 * 1024 * 1024),
            name='exchange_sums',
        )(sort_keys.reshape(1, 1, rows), seg_ids.reshape(1, 1, rows), payload)

    row_spec = P(('batch', 'group'))
    mat_spec = P(('batch', 'group'), None)
    return jax.shard_map(per_device, mesh=mesh, in_specs=(row_spec, row_spec, mat_spec),
                         out_specs=mat_spec, check_vma=False)
```

```python
import functools

import jax
import jax.numpy as jnp
from jax import lax
from jax.experimental import pallas as pl
from jax.experimental.pallas import tpu as pltpu
from jax.sharding import PartitionSpec as P

MESH = pl.DeviceIdType.MESH
LANES = 128
CORES = 2
CHUNKS = 2
ROW_TILE = 64
DOT_ROWS = 256


def exchange_kernel(n, keys_ref, segs_ref, pay_ref, out_ref, keys_all, segs_all, kcol, scol, mask, pay, slab, res,
                    pay_sem, key_send, key_recv, seg_send, seg_recv, fwd_send, fwd_recv, ret_send, ret_recv):
    me = lax.axis_index('group')
    rows, width = pay_ref.shape
    block = width // n
    cw = block // CHUNKS
    halves = rows // DOT_ROWS
    lane_tiles = rows // LANES
    ring = n // CORES
    chip, core = lax.div(me, CORES), lax.rem(me, CORES)

    def peer(hop, flip):
        return lax.rem(chip + hop, ring) * CORES + lax.rem(core + flip, CORES)

    near = [(1, 0), (ring - 1, 0), (1, 1), (ring - 1, 1)]
    far = [(2, 0), (2, 1)]
    order = [peer(*p) for p in near + far + [(0, 1)]]

    def near_peer(i):
        return peer(1 + (ring - 2) * lax.rem(i, 2), lax.div(i, 2))

    def far_peer(i):
        return peer(2 + (ring - 2) * lax.div(i, 2), i + lax.div(i, 2))

    def key_copy(dst):
        return pltpu.make_async_remote_copy(
            src_ref=keys_ref.at[0], dst_ref=keys_all.at[me], send_sem=key_send.at[dst], recv_sem=key_recv.at[me],
            device_id={'group': dst}, device_id_type=MESH)

    def seg_copy(dst):
        return pltpu.make_async_remote_copy(
            src_ref=segs_ref.at[0], dst_ref=segs_all.at[me], send_sem=seg_send.at[dst], recv_sem=seg_recv.at[me],
            device_id={'group': dst}, device_id_type=MESH)

    def block_cols(dev):
        return pl.ds(pl.multiple_of(dev * block, LANES), block)

    def columns(dev, c):
        return pl.ds(pl.multiple_of(dev * block + c * cw, LANES), cw)

    def my_rows(dev):
        return pl.ds(pl.multiple_of(dev * rows, rows), rows)

    def pay_copy(dst):
        return pltpu.make_async_copy(pay_ref.at[:, block_cols(dst)], pay.at[:, block_cols(dst)], pay_sem.at[dst])

    def fwd_copy(dst, c):
        return pltpu.make_async_remote_copy(
            src_ref=pay.at[:, columns(dst, c)], dst_ref=slab.at[c, my_rows(me), :],
            send_sem=fwd_send.at[dst, c], recv_sem=fwd_recv.at[me, c],
            device_id={'group': dst}, device_id_type=MESH)

    def ret_copy(dev, h, c):
        src_rows = pl.ds(pl.multiple_of(dev * rows + h * DOT_ROWS, DOT_ROWS), DOT_ROWS)
        dst_rows = pl.ds(pl.multiple_of(h * DOT_ROWS, DOT_ROWS), DOT_ROWS)
        return pltpu.make_async_remote_copy(
            src_ref=res.at[c, src_rows, :], dst_ref=out_ref.at[dst_rows, columns(me, c)],
            send_sem=ret_send.at[dev, c, h], recv_sem=ret_recv.at[me, c, h],
            device_id={'group': dev}, device_id_type=MESH)

    own_copies = [pltpu.make_async_copy(keys_ref.at[0], keys_all.at[me], key_recv.at[me]),
                  pltpu.make_async_copy(segs_ref.at[0], segs_all.at[me], seg_recv.at[me])]
    own_copies += [pltpu.make_async_copy(pay_ref.at[:, columns(me, c)], slab.at[c, my_rows(me), :], fwd_recv.at[me, c])
                   for c in range(CHUNKS)]

    barrier = pltpu.get_barrier_semaphore()
    for dst in order:
        pl.semaphore_signal(barrier, inc=1, device_id={'group': dst}, device_id_type=MESH)
    for dst in order:
        pay_copy(dst).start()
    for copy in own_copies:
        copy.start()
    pl.semaphore_wait(barrier, n - 1)

    for dst in order:
        key_copy(dst).start()
        seg_copy(dst).start()
    for c in range(CHUNKS):
        for dst in order:
            if c == 0:
                pay_copy(dst).wait()
            fwd_copy(dst, c).start()

    own_copies[0].wait()
    own_copies[1].wait()
    for src in order:
        pltpu.make_async_copy(keys_ref.at[0], keys_all.at[src], key_recv.at[src]).wait()
        pltpu.make_async_copy(segs_ref.at[0], segs_all.at[src], seg_recv.at[src]).wait()

    def spread(dev, carry):
        for j in range(lane_tiles):
            lanes = slice(j * LANES, (j + 1) * LANES)
            dst = pl.ds(pl.multiple_of(dev * rows + j * LANES, LANES), LANES)
            kcol[dst, :] = jnp.broadcast_to(keys_all[dev, :, lanes], (LANES, LANES)).T
            scol[dst, :] = jnp.broadcast_to(segs_all[dev, :, lanes], (LANES, LANES)).T
        return carry

    lax.fori_loop(0, n, spread, 0)

    def build(t, carry):
        here = pl.ds(pl.multiple_of(t * ROW_TILE, ROW_TILE), ROW_TILE)
        key_r, seg_r = kcol[here, :], scol[here, :]
        last = jnp.full((ROW_TILE, LANES), -jnp.inf, jnp.float32)
        for dev in range(n):
            for j in range(lane_tiles):
                lanes = slice(j * LANES, (j + 1) * LANES)
                key_s, seg_s = keys_all[dev, :, lanes], segs_all[dev, :, lanes]
                other = jnp.logical_and(key_s < key_r, seg_s != seg_r)
                last = jnp.maximum(last, jnp.where(other, key_s, -jnp.inf))
        last = jnp.broadcast_to(jnp.max(last, axis=1, keepdims=True), (ROW_TILE, LANES))
        for dev in range(n):
            for j in range(lane_tiles):
                lanes = slice(j * LANES, (j + 1) * LANES)
                key_s = keys_all[dev, :, lanes]
                inside = jnp.logical_and(key_s <= key_r, key_s > last)
                at = slice(dev * rows + j * LANES, dev * rows + (j + 1) * LANES)
                mask[here, at] = jnp.where(inside, 1.0, 0.0).astype(jnp.bfloat16)
        return carry

    lax.fori_loop(0, n * rows // ROW_TILE, build, 0)

    def sums(dev, h, c):
        at = pl.ds(pl.multiple_of(dev * rows + h * DOT_ROWS, DOT_ROWS), DOT_ROWS)
        return jnp.dot(mask[at, :], slab[c], preferred_element_type=jnp.float32).astype(jnp.bfloat16)

    for c in range(CHUNKS):
        own_copies[2 + c].wait()
        for src in order:
            pltpu.make_async_copy(pay.at[:, columns(me, c)], slab.at[c, my_rows(src), :], fwd_recv.at[src, c]).wait()

        def dot_pass(pick, c=c):
            def dot_step(step, carry):
                dev, h = pick(lax.div(step, halves)), lax.rem(step, halves)
                at = pl.ds(pl.multiple_of(dev * rows + h * DOT_ROWS, DOT_ROWS), DOT_ROWS)
                res[c, at, :] = sums(dev, h, c)

                @pl.when(step > 0)
                def _():
                    ret_copy(pick(lax.div(step - 1, halves)), lax.rem(step - 1, halves), c).start()

                return carry
            return dot_step

        lax.fori_loop(0, 4 * halves, dot_pass(near_peer), 0)
        ret_copy(near_peer(3), halves - 1, c).start()
        lax.fori_loop(0, 3 * halves, dot_pass(far_peer), 0)
        ret_copy(far_peer(2), halves - 1, c).start()
        for h in range(halves):
            out_ref[pl.ds(h * DOT_ROWS, DOT_ROWS), columns(me, c)] = sums(me, h, c)

    for dst in order:
        key_copy(dst).wait_send()
        seg_copy(dst).wait_send()
        for c in range(CHUNKS):
            fwd_copy(dst, c).wait_send()
    for c in range(CHUNKS):
        for h in range(halves):
            for src in order:
                ret_copy(src, h, c).wait_send()
            for src in order:
                dst_rows = pl.ds(h * DOT_ROWS, DOT_ROWS)
                pltpu.make_async_copy(res.at[c, pl.ds(0, DOT_ROWS), :], out_ref.at[dst_rows, columns(src, c)],
                                      ret_recv.at[src, c, h]).wait()


def solution(mesh):
    n = mesh.shape['group']

    def per_device(sort_keys, seg_ids, payload):
        rows, width = payload.shape
        total = n * rows
        cw = width // n // CHUNKS
        halves = rows // DOT_ROWS
        dma = pltpu.SemaphoreType.DMA
        return pl.pallas_call(
            functools.partial(exchange_kernel, n),
            out_shape=pltpu.VMEM((rows, width), jnp.bfloat16),
            in_specs=[pl.BlockSpec(memory_space=pl.ANY)] * 3,
            out_specs=pl.BlockSpec(memory_space=pltpu.VMEM),
            scratch_shapes=[
                pltpu.VMEM((n, 1, rows), jnp.float32),
                pltpu.VMEM((n, 1, rows), jnp.int32),
                pltpu.VMEM((total, LANES), jnp.float32),
                pltpu.VMEM((total, LANES), jnp.int32),
                pltpu.VMEM((total, total), jnp.bfloat16),
                pltpu.VMEM((rows, width), jnp.bfloat16),
                pltpu.VMEM((CHUNKS, total, cw), jnp.bfloat16),
                pltpu.VMEM((CHUNKS, total, cw), jnp.bfloat16),
                dma((n,)), dma((n,)), dma((n,)), dma((n,)), dma((n,)),
                dma((n, CHUNKS)), dma((n, CHUNKS)),
                dma((n, CHUNKS, halves)), dma((n, CHUNKS, halves)),
            ],
            compiler_params=pltpu.CompilerParams(collective_id=0, has_side_effects=True,
                                                 vmem_limit_bytes=56 * 1024 * 1024),
            name='exchange_sums',
        )(sort_keys.reshape(1, 1, rows), seg_ids.reshape(1, 1, rows), payload)

    row_spec = P(('batch', 'group'))
    mat_spec = P(('batch', 'group'), None)
    return jax.shard_map(per_device, mesh=mesh, in_specs=(row_spec, row_spec, mat_spec),
                         out_specs=mat_spec, check_vma=False)
```

```python
import functools

import jax
import jax.numpy as jnp
from jax import lax
from jax.experimental import pallas as pl
from jax.experimental.pallas import tpu as pltpu
from jax.sharding import PartitionSpec as P

MESH = pl.DeviceIdType.MESH
LANES = 128
CORES = 2
CHUNKS = 2
ROW_TILE = 64
DOT_ROWS = 256


def exchange_kernel(n, keys_ref, segs_ref, pay_ref, out_ref, keys_all, segs_all, kcol, scol, mask, pay, slab, res,
                    far_ok, pay_sem, key_send, key_recv, seg_send, seg_recv, fwd_send, fwd_recv, ret_send, ret_recv):
    me = lax.axis_index('group')
    rows, width = pay_ref.shape
    block = width // n
    cw = block // CHUNKS
    halves = rows // DOT_ROWS
    lane_tiles = rows // LANES
    ring = n // CORES
    chip, core = lax.div(me, CORES), lax.rem(me, CORES)

    def peer(hop, flip):
        return lax.rem(chip + hop, ring) * CORES + lax.rem(core + flip, CORES)

    near = [peer(1, 0), peer(ring - 1, 0), peer(1, 1), peer(ring - 1, 1), peer(0, 1)]
    far = [peer(2, 0), peer(2, 1)]
    order = near + far

    def near_peer(i):
        return peer(1 + (ring - 2) * lax.rem(i, 2), lax.div(i, 2))

    def far_peer(i):
        return peer(2 + (ring - 2) * lax.div(i, 2), i + lax.div(i, 2))

    def key_copy(dst):
        return pltpu.make_async_remote_copy(
            src_ref=keys_ref.at[0], dst_ref=keys_all.at[me], send_sem=key_send.at[dst], recv_sem=key_recv.at[me],
            device_id={'group': dst}, device_id_type=MESH)

    def seg_copy(dst):
        return pltpu.make_async_remote_copy(
            src_ref=segs_ref.at[0], dst_ref=segs_all.at[me], send_sem=seg_send.at[dst], recv_sem=seg_recv.at[me],
            device_id={'group': dst}, device_id_type=MESH)

    def block_cols(dev):
        return pl.ds(pl.multiple_of(dev * block, LANES), block)

    def columns(dev, c):
        return pl.ds(pl.multiple_of(dev * block + c * cw, LANES), cw)

    def my_rows(dev):
        return pl.ds(pl.multiple_of(dev * rows, rows), rows)

    def pay_copy(dst):
        return pltpu.make_async_copy(pay_ref.at[:, block_cols(dst)], pay.at[:, block_cols(dst)], pay_sem.at[dst])

    def fwd_copy(dst, c):
        return pltpu.make_async_remote_copy(
            src_ref=pay.at[:, columns(dst, c)], dst_ref=slab.at[c, my_rows(me), :],
            send_sem=fwd_send.at[dst, c], recv_sem=fwd_recv.at[me, c],
            device_id={'group': dst}, device_id_type=MESH)

    def ret_copy(dev, h, c):
        src_rows = pl.ds(pl.multiple_of(dev * rows + h * DOT_ROWS, DOT_ROWS), DOT_ROWS)
        dst_rows = pl.ds(pl.multiple_of(h * DOT_ROWS, DOT_ROWS), DOT_ROWS)
        return pltpu.make_async_remote_copy(
            src_ref=res.at[c, src_rows, :], dst_ref=out_ref.at[dst_rows, columns(me, c)],
            send_sem=ret_send.at[dev, c, h], recv_sem=ret_recv.at[me, c, h],
            device_id={'group': dev}, device_id_type=MESH)

    own_copies = [pltpu.make_async_copy(keys_ref.at[0], keys_all.at[me], key_recv.at[me]),
                  pltpu.make_async_copy(segs_ref.at[0], segs_all.at[me], seg_recv.at[me])]
    own_copies += [pltpu.make_async_copy(pay_ref.at[:, columns(me, c)], slab.at[c, my_rows(me), :], fwd_recv.at[me, c])
                   for c in range(CHUNKS)]

    barrier = pltpu.get_barrier_semaphore()
    for dst in near:
        pl.semaphore_signal(barrier, inc=1, device_id={'group': dst}, device_id_type=MESH)
    for dst in order:
        pay_copy(dst).start()
    for copy in own_copies:
        copy.start()
    pl.semaphore_wait(barrier, len(near))
    pl.semaphore_signal(far_ok, inc=1, device_id={'group': peer(ring - 1, 0)}, device_id_type=MESH)

    for dst in near:
        key_copy(dst).start()
        seg_copy(dst).start()

    def send_block(dst, c):
        if c == 0:
            pay_copy(dst).wait()
        fwd_copy(dst, c).start()

    for dst in near[:2]:
        send_block(dst, 0)
    pl.semaphore_wait(far_ok, 1)
    for dst in far:
        key_copy(dst).start()
        seg_copy(dst).start()
    for dst in near[2:]:
        send_block(dst, 0)
    for dst in near:
        send_block(dst, 1)
    for c in range(CHUNKS):
        for dst in far:
            send_block(dst, c)

    own_copies[0].wait()
    own_copies[1].wait()
    for src in order:
        pltpu.make_async_copy(keys_ref.at[0], keys_all.at[src], key_recv.at[src]).wait()
        pltpu.make_async_copy(segs_ref.at[0], segs_all.at[src], seg_recv.at[src]).wait()

    def spread(dev, carry):
        for j in range(lane_tiles):
            lanes = slice(j * LANES, (j + 1) * LANES)
            dst = pl.ds(pl.multiple_of(dev * rows + j * LANES, LANES), LANES)
            kcol[dst, :] = jnp.broadcast_to(keys_all[dev, :, lanes], (LANES, LANES)).T
            scol[dst, :] = jnp.broadcast_to(segs_all[dev, :, lanes], (LANES, LANES)).T
        return carry

    lax.fori_loop(0, n, spread, 0)

    def build(t, carry):
        here = pl.ds(pl.multiple_of(t * ROW_TILE, ROW_TILE), ROW_TILE)
        key_r, seg_r = kcol[here, :], scol[here, :]
        last = jnp.full((ROW_TILE, LANES), -jnp.inf, jnp.float32)
        for dev in range(n):
            for j in range(lane_tiles):
                lanes = slice(j * LANES, (j + 1) * LANES)
                key_s, seg_s = keys_all[dev, :, lanes], segs_all[dev, :, lanes]
                other = jnp.logical_and(key_s < key_r, seg_s != seg_r)
                last = jnp.maximum(last, jnp.where(other, key_s, -jnp.inf))
        last = jnp.broadcast_to(jnp.max(last, axis=1, keepdims=True), (ROW_TILE, LANES))
        for dev in range(n):
            for j in range(lane_tiles):
                lanes = slice(j * LANES, (j + 1) * LANES)
                key_s = keys_all[dev, :, lanes]
                inside = jnp.logical_and(key_s <= key_r, key_s > last)
                at = slice(dev * rows + j * LANES, dev * rows + (j + 1) * LANES)
                mask[here, at] = jnp.where(inside, 1.0, 0.0).astype(jnp.bfloat16)
        return carry

    lax.fori_loop(0, n * rows // ROW_TILE, build, 0)

    def sums(dev, h, c):
        at = pl.ds(pl.multiple_of(dev * rows + h * DOT_ROWS, DOT_ROWS), DOT_ROWS)
        return jnp.dot(mask[at, :], slab[c], preferred_element_type=jnp.float32).astype(jnp.bfloat16)

    for c in range(CHUNKS):
        own_copies[2 + c].wait()
        for src in order:
            pltpu.make_async_copy(pay.at[:, columns(me, c)], slab.at[c, my_rows(src), :], fwd_recv.at[src, c]).wait()

        def dot_pass(pick, send, c=c):
            def dot_step(step, carry):
                dev, h = pick(lax.div(step, halves)), lax.rem(step, halves)
                at = pl.ds(pl.multiple_of(dev * rows + h * DOT_ROWS, DOT_ROWS), DOT_ROWS)
                res[c, at, :] = sums(dev, h, c)

                if send:
                    @pl.when(step > 0)
                    def _():
                        ret_copy(pick(lax.div(step - 1, halves)), lax.rem(step - 1, halves), c).start()

                return carry
            return dot_step

        last_chunk = c == CHUNKS - 1
        lax.fori_loop(0, 4 * halves, dot_pass(near_peer, True), 0)
        ret_copy(near_peer(3), halves - 1, c).start()
        if last_chunk:
            for early in range(c):
                for i in range(3):
                    for h in range(halves):
                        ret_copy(far_peer(i), h, early).start()
        lax.fori_loop(0, 3 * halves, dot_pass(far_peer, last_chunk), 0)
        if last_chunk:
            ret_copy(far_peer(2), halves - 1, c).start()
        for h in range(halves):
            out_ref[pl.ds(h * DOT_ROWS, DOT_ROWS), columns(me, c)] = sums(me, h, c)

    for dst in order:
        key_copy(dst).wait_send()
        seg_copy(dst).wait_send()
        for c in range(CHUNKS):
            fwd_copy(dst, c).wait_send()
    for c in range(CHUNKS):
        for h in range(halves):
            for src in order:
                ret_copy(src, h, c).wait_send()
            for src in order:
                dst_rows = pl.ds(h * DOT_ROWS, DOT_ROWS)
                pltpu.make_async_copy(res.at[c, pl.ds(0, DOT_ROWS), :], out_ref.at[dst_rows, columns(src, c)],
                                      ret_recv.at[src, c, h]).wait()


def solution(mesh):
    n = mesh.shape['group']

    def per_device(sort_keys, seg_ids, payload):
        rows, width = payload.shape
        total = n * rows
        cw = width // n // CHUNKS
        halves = rows // DOT_ROWS
        dma = pltpu.SemaphoreType.DMA
        return pl.pallas_call(
            functools.partial(exchange_kernel, n),
            out_shape=pltpu.VMEM((rows, width), jnp.bfloat16),
            in_specs=[pl.BlockSpec(memory_space=pl.ANY)] * 3,
            out_specs=pl.BlockSpec(memory_space=pltpu.VMEM),
            scratch_shapes=[
                pltpu.VMEM((n, 1, rows), jnp.float32),
                pltpu.VMEM((n, 1, rows), jnp.int32),
                pltpu.VMEM((total, LANES), jnp.float32),
                pltpu.VMEM((total, LANES), jnp.int32),
                pltpu.VMEM((total, total), jnp.bfloat16),
                pltpu.VMEM((rows, width), jnp.bfloat16),
                pltpu.VMEM((CHUNKS, total, cw), jnp.bfloat16),
                pltpu.VMEM((CHUNKS, total, cw), jnp.bfloat16),
                pltpu.SemaphoreType.REGULAR, dma((n,)), dma((n,)), dma((n,)), dma((n,)), dma((n,)),
                dma((n, CHUNKS)), dma((n, CHUNKS)),
                dma((n, CHUNKS, halves)), dma((n, CHUNKS, halves)),
            ],
            compiler_params=pltpu.CompilerParams(collective_id=0, has_side_effects=True,
                                                 vmem_limit_bytes=56 * 1024 * 1024),
            name='exchange_sums',
        )(sort_keys.reshape(1, 1, rows), seg_ids.reshape(1, 1, rows), payload)

    row_spec = P(('batch', 'group'))
    mat_spec = P(('batch', 'group'), None)
    return jax.shard_map(per_device, mesh=mesh, in_specs=(row_spec, row_spec, mat_spec),
                         out_specs=mat_spec, check_vma=False)
```

```python
import functools

import jax
import jax.numpy as jnp
from jax import lax
from jax.experimental import pallas as pl
from jax.experimental.pallas import tpu as pltpu
from jax.sharding import PartitionSpec as P

MESH = pl.DeviceIdType.MESH
LANES = 128
CORES = 2
WAYS = 2
CHUNKS = 2
ROW_TILE = 64
EARLY_STEPS = 16


def exchange_kernel(n, keys_ref, segs_ref, pay_ref, out_ref, keys_all, segs_all, kcol, scol, mask, pay, slab, res,
                    relay, relay_back, far_ok, pay_sem, key_send, key_recv, seg_send, seg_recv, fwd_send, fwd_recv,
                    hop_send, hop_recv, on_send, far_recv, ret_send, ret_recv, back_send, back_recv, back_on_send):
    me = lax.axis_index('group')
    rows, width = pay_ref.shape
    block = width // n
    cw = block // CHUNKS
    half = rows // WAYS
    lane_tiles = rows // LANES
    ring = n // CORES
    chip, core = lax.div(me, CORES), lax.rem(me, CORES)

    def peer(hop, flip):
        return lax.rem(chip + hop, ring) * CORES + lax.rem(core + flip, CORES)

    def way(i):
        return 1 + (ring - 2) * i

    near = [peer(way(i), flip) for flip in range(CORES) for i in range(WAYS)] + [peer(0, 1)]
    far = [peer(2, flip) for flip in range(CORES)]
    both = [(i, flip) for flip in range(CORES) for i in range(WAYS)]

    def remote(src, dst, send_sem, recv_sem, dev):
        return pltpu.make_async_remote_copy(src_ref=src, dst_ref=dst, send_sem=send_sem, recv_sem=recv_sem,
                                            device_id={'group': dev}, device_id_type=MESH)

    def columns(dev, c):
        return pl.ds(pl.multiple_of(dev * block + c * cw, LANES), cw)

    def dev_rows(dev):
        return pl.ds(pl.multiple_of(dev * rows, rows), rows)

    def half_rows(dev, i):
        return pl.ds(pl.multiple_of(dev * rows + i * half, half), half)

    def key_copy(dst):
        return remote(keys_ref.at[0], keys_all.at[me], key_send.at[dst], key_recv.at[me], dst)

    def seg_copy(dst):
        return remote(segs_ref.at[0], segs_all.at[me], seg_send.at[dst], seg_recv.at[me], dst)

    def pay_copy(dst):
        cols = pl.ds(pl.multiple_of(dst * block, LANES), block)
        return pltpu.make_async_copy(pay_ref.at[:, cols], pay.at[:, cols], pay_sem.at[dst])

    def fwd_copy(dst, c):
        return remote(pay.at[:, columns(dst, c)], slab.at[c, dev_rows(me), :], fwd_send.at[dst, c], fwd_recv.at[me, c], dst)

    def hop_out(i, flip, c):
        return remote(pay.at[half_rows(0, i), columns(peer(2, flip), c)], relay.at[i, c, flip],
                      hop_send.at[i, c, flip], hop_recv.at[i, c, flip], peer(way(i), 0))

    def hop_on(i, flip, c):
        origin = peer(way(1 - i), 0)
        return remote(relay.at[i, c, flip], slab.at[c, half_rows(origin, i), :],
                      on_send.at[i, c, flip], far_recv.at[origin, c, i], peer(way(i), flip))

    def ret_copy(dst, i, c):
        return remote(res.at[c, half_rows(dst, i), :], out_ref.at[half_rows(0, i), columns(me, c)],
                      ret_send.at[dst, c, i], ret_recv.at[me, c, i], dst)

    def back_out(i, flip, c):
        return remote(res.at[c, half_rows(peer(2, flip), i), :], relay_back.at[i, c, flip],
                      back_send.at[i, c, flip], back_recv.at[i, c, flip], peer(way(i), 0))

    def back_on(i, flip, c):
        origin = peer(way(1 - i), 0)
        return remote(relay_back.at[i, c, flip], out_ref.at[half_rows(0, i), columns(origin, c)],
                      back_on_send.at[i, c, flip], ret_recv.at[origin, c, i], peer(way(i), flip))

    def arrived(dst, sem):
        pltpu.make_async_copy(dst, dst, sem).wait()

    own_copies = [pltpu.make_async_copy(keys_ref.at[0], keys_all.at[me], key_recv.at[me]),
                  pltpu.make_async_copy(segs_ref.at[0], segs_all.at[me], seg_recv.at[me])]
    own_copies += [pltpu.make_async_copy(pay_ref.at[:, columns(me, c)], slab.at[c, dev_rows(me), :], fwd_recv.at[me, c])
                   for c in range(CHUNKS)]

    barrier = pltpu.get_barrier_semaphore()
    for dst in near:
        pl.semaphore_signal(barrier, inc=1, device_id={'group': dst}, device_id_type=MESH)
    for dst in far + near:
        pay_copy(dst).start()
    for copy in own_copies:
        copy.start()
    pl.semaphore_wait(barrier, len(near))
    pl.semaphore_signal(far_ok, inc=1, device_id={'group': peer(way(1), 0)}, device_id_type=MESH)

    for dst in near:
        key_copy(dst).start()
        seg_copy(dst).start()
    for dst in far:
        pay_copy(dst).wait()
    for i, flip in both:
        hop_out(i, flip, 0).start()
    pl.semaphore_wait(far_ok, 1)
    for dst in far:
        key_copy(dst).start()
        seg_copy(dst).start()
    for dst in near:
        pay_copy(dst).wait()
        fwd_copy(dst, 0).start()

    own_copies[0].wait()
    own_copies[1].wait()
    for src in far + near:
        arrived(keys_all.at[src], key_recv.at[src])
        arrived(segs_all.at[src], seg_recv.at[src])

    def spread(dev, carry):
        for j in range(lane_tiles):
            lanes = slice(j * LANES, (j + 1) * LANES)
            dst = pl.ds(pl.multiple_of(dev * rows + j * LANES, LANES), LANES)
            kcol[dst, :] = jnp.broadcast_to(keys_all[dev, :, lanes], (LANES, LANES)).T
            scol[dst, :] = jnp.broadcast_to(segs_all[dev, :, lanes], (LANES, LANES)).T
        return carry

    lax.fori_loop(0, n, spread, 0)

    def build(t, carry):
        here = pl.ds(pl.multiple_of(t * ROW_TILE, ROW_TILE), ROW_TILE)
        key_r, seg_r = kcol[here, :], scol[here, :]
        last = jnp.full((ROW_TILE, LANES), -jnp.inf, jnp.float32)
        for dev in range(n):
            for j in range(lane_tiles):
                lanes = slice(j * LANES, (j + 1) * LANES)
                key_s, seg_s = keys_all[dev, :, lanes], segs_all[dev, :, lanes]
                other = jnp.logical_and(key_s < key_r, seg_s != seg_r)
                last = jnp.maximum(last, jnp.where(other, key_s, -jnp.inf))
        last = jnp.broadcast_to(jnp.max(last, axis=1, keepdims=True), (ROW_TILE, LANES))
        for dev in range(n):
            for j in range(lane_tiles):
                lanes = slice(j * LANES, (j + 1) * LANES)
                key_s = keys_all[dev, :, lanes]
                inside = jnp.logical_and(key_s <= key_r, key_s > last)
                at = slice(dev * rows + j * LANES, dev * rows + (j + 1) * LANES)
                mask[here, at] = jnp.where(inside, 1.0, 0.0).astype(jnp.bfloat16)
        return carry

    steps = n * rows // ROW_TILE
    for c in range(CHUNKS):
        lax.fori_loop(EARLY_STEPS * c, EARLY_STEPS * (c + 1) if c < CHUNKS - 1 else steps, build, 0)
        for i, flip in both:
            arrived(relay.at[i, c, flip], hop_recv.at[i, c, flip])
            hop_on(i, flip, c).start()
        if c + 1 < CHUNKS:
            for i, flip in both:
                hop_out(i, flip, c + 1).start()
            for dst in near:
                fwd_copy(dst, c + 1).start()

    def sums(dev, i, c):
        return jnp.dot(mask[half_rows(dev, i), :], slab[c], preferred_element_type=jnp.float32).astype(jnp.bfloat16)

    def near_pick(k):
        return peer(way(lax.rem(k, WAYS)), lax.div(k, WAYS))

    for c in range(CHUNKS):
        own_copies[2 + c].wait()
        for src in near:
            arrived(slab.at[c, dev_rows(src), :], fwd_recv.at[src, c])
        for src in far:
            for i in range(WAYS):
                arrived(slab.at[c, half_rows(src, i), :], far_recv.at[src, c, i])

        def far_step(step, carry, c=c):
            i, flip = lax.rem(step, WAYS), lax.div(step, WAYS)
            dev = peer(2, flip)
            res[c, half_rows(dev, i), :] = sums(dev, i, c)

            @pl.when(step > 0)
            def _():
                back_out(lax.rem(step - 1, WAYS), lax.div(step - 1, WAYS), c).start()

            return carry

        def near_step(step, carry, c=c):
            i, k = lax.rem(step, WAYS), lax.div(step, WAYS)
            dev = near_pick(k)
            res[c, half_rows(dev, i), :] = sums(dev, i, c)

            @pl.when(step == 0)
            def _():
                back_out(WAYS - 1, CORES - 1, c).start()

            @pl.when(step > 0)
            def _():
                ret_copy(near_pick(lax.div(step - 1, WAYS)), lax.rem(step - 1, WAYS), c).start()

            return carry

        def chip_step(i, carry, c=c):
            dev = peer(0, 1)
            res[c, half_rows(dev, i), :] = sums(dev, i, c)

            @pl.when(i == 0)
            def _():
                ret_copy(near[-2], WAYS - 1, c).start()

            @pl.when(i > 0)
            def _():
                ret_copy(dev, i - 1, c).start()

            return carry

        def own_step(i, carry, c=c):
            out_ref[half_rows(0, i), columns(me, c)] = sums(me, i, c)

            @pl.when(i == 0)
            def _():
                ret_copy(peer(0, 1), WAYS - 1, c).start()

            return carry

        lax.fori_loop(0, CORES * WAYS, far_step, 0)
        lax.fori_loop(0, CORES * WAYS * WAYS, near_step, 0)
        lax.fori_loop(0, WAYS, chip_step, 0)
        lax.fori_loop(0, WAYS, own_step, 0)

    for c in range(CHUNKS):
        for i, flip in both:
            arrived(relay_back.at[i, c, flip], back_recv.at[i, c, flip])
            back_on(i, flip, c).start()

    for dst in far + near:
        key_copy(dst).wait_send()
        seg_copy(dst).wait_send()
    for c in range(CHUNKS):
        for dst in near:
            fwd_copy(dst, c).wait_send()
            for i in range(WAYS):
                ret_copy(dst, i, c).wait_send()
        for i, flip in both:
            hop_out(i, flip, c).wait_send()
            hop_on(i, flip, c).wait_send()
            back_out(i, flip, c).wait_send()
        for src in near + far:
            for i in range(WAYS):
                arrived(out_ref.at[half_rows(0, i), columns(src, c)], ret_recv.at[src, c, i])
    for c in range(CHUNKS):
        for i, flip in both:
            back_on(i, flip, c).wait_send()


def solution(mesh):
    n = mesh.shape['group']

    def per_device(sort_keys, seg_ids, payload):
        rows, width = payload.shape
        total = n * rows
        cw = width // n // CHUNKS
        dma = pltpu.SemaphoreType.DMA
        hops = (WAYS, CHUNKS, CORES)
        return pl.pallas_call(
            functools.partial(exchange_kernel, n),
            out_shape=pltpu.VMEM((rows, width), jnp.bfloat16),
            in_specs=[pl.BlockSpec(memory_space=pl.ANY)] * 3,
            out_specs=pl.BlockSpec(memory_space=pltpu.VMEM),
            scratch_shapes=[
                pltpu.VMEM((n, 1, rows), jnp.float32),
                pltpu.VMEM((n, 1, rows), jnp.int32),
                pltpu.VMEM((total, LANES), jnp.float32),
                pltpu.VMEM((total, LANES), jnp.int32),
                pltpu.VMEM((total, total), jnp.bfloat16),
                pltpu.VMEM((rows, width), jnp.bfloat16),
                pltpu.VMEM((CHUNKS, total, cw), jnp.bfloat16),
                pltpu.VMEM((CHUNKS, total, cw), jnp.bfloat16),
                pltpu.VMEM((*hops, rows // WAYS, cw), jnp.bfloat16),
                pltpu.VMEM((*hops, rows // WAYS, cw), jnp.bfloat16),
                pltpu.SemaphoreType.REGULAR, dma((n,)), dma((n,)), dma((n,)), dma((n,)), dma((n,)),
                dma((n, CHUNKS)), dma((n, CHUNKS)),
                dma(hops), dma(hops), dma(hops), dma((n, CHUNKS, WAYS)),
                dma((n, CHUNKS, WAYS)), dma((n, CHUNKS, WAYS)), dma(hops), dma(hops), dma(hops),
            ],
            compiler_params=pltpu.CompilerParams(collective_id=0, has_side_effects=True,
                                                 vmem_limit_bytes=56 * 1024 * 1024),
            name='exchange_sums',
        )(sort_keys.reshape(1, 1, rows), seg_ids.reshape(1, 1, rows), payload)

    row_spec = P(('batch', 'group'))
    mat_spec = P(('batch', 'group'), None)
    return jax.shard_map(per_device, mesh=mesh, in_specs=(row_spec, row_spec, mat_spec),
                         out_specs=mat_spec, check_vma=False)
```

```python
import functools

import jax
import jax.numpy as jnp
from jax import lax
from jax.experimental import pallas as pl
from jax.experimental.pallas import tpu as pltpu
from jax.sharding import PartitionSpec as P

MESH = pl.DeviceIdType.MESH
LANES = 128
CORES = 2
WAYS = 2
CHUNKS = 2
ROW_TILE = 64
EARLY_STEPS = 16


def exchange_kernel(n, keys_ref, segs_ref, pay_ref, out_ref, keys_all, segs_all, kcol, scol, mask, pay, slab, res,
                    relay, relay_back, far_ok, pay_sem, key_send, key_recv, seg_send, seg_recv, fwd_send, fwd_recv,
                    hop_send, hop_recv, on_send, far_recv, ret_send, ret_recv, back_send, back_recv, back_on_send):
    me = lax.axis_index('group')
    rows, width = pay_ref.shape
    block = width // n
    cw = block // CHUNKS
    half = rows // WAYS
    lane_tiles = rows // LANES
    ring = n // CORES
    chip, core = lax.div(me, CORES), lax.rem(me, CORES)

    def peer(hop, flip):
        return lax.rem(chip + hop, ring) * CORES + lax.rem(core + flip, CORES)

    def way(i):
        return 1 + (ring - 2) * i

    near = [peer(way(i), flip) for flip in range(CORES) for i in range(WAYS)] + [peer(0, 1)]
    far = [peer(2, flip) for flip in range(CORES)]
    both = [(i, flip) for flip in range(CORES) for i in range(WAYS)]

    def remote(src, dst, send_sem, recv_sem, dev):
        return pltpu.make_async_remote_copy(src_ref=src, dst_ref=dst, send_sem=send_sem, recv_sem=recv_sem,
                                            device_id={'group': dev}, device_id_type=MESH)

    def columns(dev, c):
        return pl.ds(pl.multiple_of(dev * block + c * cw, LANES), cw)

    def dev_rows(dev):
        return pl.ds(pl.multiple_of(dev * rows, rows), rows)

    def half_rows(dev, i):
        return pl.ds(pl.multiple_of(dev * rows + i * half, half), half)

    def key_copy(dst):
        return remote(keys_all.at[me], keys_all.at[me], key_send.at[dst], key_recv.at[me], dst)

    def seg_copy(dst):
        return remote(segs_all.at[me], segs_all.at[me], seg_send.at[dst], seg_recv.at[me], dst)

    def pay_copy(dst, c):
        return pltpu.make_async_copy(pay_ref.at[:, columns(dst, c)], pay.at[:, columns(dst, c)], pay_sem.at[dst, c])

    def fwd_copy(dst, c):
        return remote(pay.at[:, columns(dst, c)], slab.at[c, dev_rows(me), :], fwd_send.at[dst, c], fwd_recv.at[me, c], dst)

    def hop_out(i, flip, c):
        return remote(pay.at[half_rows(0, i), columns(peer(2, flip), c)], relay.at[i, c, flip],
                      hop_send.at[i, c, flip], hop_recv.at[i, c, flip], peer(way(i), 0))

    def hop_on(i, flip, c):
        origin = peer(way(1 - i), 0)
        return remote(relay.at[i, c, flip], slab.at[c, half_rows(origin, i), :],
                      on_send.at[i, c, flip], far_recv.at[origin, c, i], peer(way(i), flip))

    def ret_copy(dst, i, c):
        return remote(res.at[c, half_rows(dst, i), :], out_ref.at[half_rows(0, i), columns(me, c)],
                      ret_send.at[dst, c, i], ret_recv.at[me, c, i], dst)

    def back_out(i, flip, c):
        return remote(res.at[c, half_rows(peer(2, flip), i), :], relay_back.at[i, c, flip],
                      back_send.at[i, c, flip], back_recv.at[i, c, flip], peer(way(i), 0))

    def back_on(i, flip, c):
        origin = peer(way(1 - i), 0)
        return remote(relay_back.at[i, c, flip], out_ref.at[half_rows(0, i), columns(origin, c)],
                      back_on_send.at[i, c, flip], ret_recv.at[origin, c, i], peer(way(i), flip))

    def arrived(dst, sem):
        pltpu.make_async_copy(dst, dst, sem).wait()

    own_copies = [pltpu.make_async_copy(keys_ref.at[0], keys_all.at[me], key_recv.at[me]),
                  pltpu.make_async_copy(segs_ref.at[0], segs_all.at[me], seg_recv.at[me])]
    own_copies += [pltpu.make_async_copy(pay_ref.at[:, columns(me, c)], slab.at[c, dev_rows(me), :], fwd_recv.at[me, c])
                   for c in range(CHUNKS)]

    barrier = pltpu.get_barrier_semaphore()
    for dst in near:
        pl.semaphore_signal(barrier, inc=1, device_id={'group': dst}, device_id_type=MESH)
    for dst in far:
        pay_copy(dst, 0).start()
    for copy in own_copies[:2]:
        copy.start()
    for dst in near:
        pay_copy(dst, 0).start()
    pl.semaphore_wait(barrier, len(near))
    pl.semaphore_signal(far_ok, inc=1, device_id={'group': peer(way(1), 0)}, device_id_type=MESH)

    for flip in range(CORES):
        pay_copy(far[flip], 0).wait()
        for i in range(WAYS):
            hop_out(i, flip, 0).start()
    for copy in own_copies[:2]:
        copy.wait()
    for dst in near:
        key_copy(dst).start()
        seg_copy(dst).start()
    for dst in far + near:
        pay_copy(dst, 1).start()
    for copy in own_copies[2:]:
        copy.start()
    pl.semaphore_wait(far_ok, 1)
    for dst in far:
        key_copy(dst).start()
        seg_copy(dst).start()
    for dst in near:
        pay_copy(dst, 0).wait()
        fwd_copy(dst, 0).start()
    for dst in far + near:
        pay_copy(dst, 1).wait()

    for src in far + near:
        arrived(keys_all.at[src], key_recv.at[src])
        arrived(segs_all.at[src], seg_recv.at[src])

    def spread(dev, carry):
        for j in range(lane_tiles):
            lanes = slice(j * LANES, (j + 1) * LANES)
            dst = pl.ds(pl.multiple_of(dev * rows + j * LANES, LANES), LANES)
            kcol[dst, :] = jnp.broadcast_to(keys_all[dev, :, lanes], (LANES, LANES)).T
            scol[dst, :] = jnp.broadcast_to(segs_all[dev, :, lanes], (LANES, LANES)).T
        return carry

    lax.fori_loop(0, n, spread, 0)

    def build(t, carry):
        here = pl.ds(pl.multiple_of(t * ROW_TILE, ROW_TILE), ROW_TILE)
        key_r, seg_r = kcol[here, :], scol[here, :]
        last = jnp.full((ROW_TILE, LANES), -jnp.inf, jnp.float32)
        for dev in range(n):
            for j in range(lane_tiles):
                lanes = slice(j * LANES, (j + 1) * LANES)
                key_s, seg_s = keys_all[dev, :, lanes], segs_all[dev, :, lanes]
                other = jnp.logical_and(key_s < key_r, seg_s != seg_r)
                last = jnp.maximum(last, jnp.where(other, key_s, -jnp.inf))
        last = jnp.broadcast_to(jnp.max(last, axis=1, keepdims=True), (ROW_TILE, LANES))
        for dev in range(n):
            for j in range(lane_tiles):
                lanes = slice(j * LANES, (j + 1) * LANES)
                key_s = keys_all[dev, :, lanes]
                inside = jnp.logical_and(key_s <= key_r, key_s > last)
                at = slice(dev * rows + j * LANES, dev * rows + (j + 1) * LANES)
                mask[here, at] = jnp.where(inside, 1.0, 0.0).astype(jnp.bfloat16)
        return carry

    steps = n * rows // ROW_TILE
    for c in range(CHUNKS):
        lax.fori_loop(EARLY_STEPS * c, EARLY_STEPS * (c + 1) if c < CHUNKS - 1 else steps, build, 0)
        for i, flip in both:
            arrived(relay.at[i, c, flip], hop_recv.at[i, c, flip])
            hop_on(i, flip, c).start()
        if c + 1 < CHUNKS:
            for i, flip in both:
                hop_out(i, flip, c + 1).start()
            for dst in near:
                fwd_copy(dst, c + 1).start()

    def sums(dev, i, c):
        return jnp.dot(mask[half_rows(dev, i), :], slab[c], preferred_element_type=jnp.float32).astype(jnp.bfloat16)

    def near_pick(k):
        return peer(way(lax.rem(k, WAYS)), lax.div(k, WAYS))

    for c in range(CHUNKS):
        own_copies[2 + c].wait()
        for src in near:
            arrived(slab.at[c, dev_rows(src), :], fwd_recv.at[src, c])
        for src in far:
            for i in range(WAYS):
                arrived(slab.at[c, half_rows(src, i), :], far_recv.at[src, c, i])

        def far_step(step, carry, c=c):
            i, flip = lax.rem(step, WAYS), lax.div(step, WAYS)
            dev = peer(2, flip)
            res[c, half_rows(dev, i), :] = sums(dev, i, c)

            @pl.when(step > 0)
            def _():
                back_out(lax.rem(step - 1, WAYS), lax.div(step - 1, WAYS), c).start()

            return carry

        def near_step(step, carry, c=c):
            i, k = lax.rem(step, WAYS), lax.div(step, WAYS)
            dev = near_pick(k)
            res[c, half_rows(dev, i), :] = sums(dev, i, c)

            @pl.when(step == 0)
            def _():
                back_out(WAYS - 1, CORES - 1, c).start()

            @pl.when(step > 0)
            def _():
                ret_copy(near_pick(lax.div(step - 1, WAYS)), lax.rem(step - 1, WAYS), c).start()

            return carry

        def chip_step(i, carry, c=c):
            dev = peer(0, 1)
            res[c, half_rows(dev, i), :] = sums(dev, i, c)

            @pl.when(i == 0)
            def _():
                ret_copy(near[-2], WAYS - 1, c).start()

            @pl.when(i > 0)
            def _():
                ret_copy(dev, i - 1, c).start()

            return carry

        def own_step(i, carry, c=c):
            out_ref[half_rows(0, i), columns(me, c)] = sums(me, i, c)

            @pl.when(i == 0)
            def _():
                ret_copy(peer(0, 1), WAYS - 1, c).start()

            return carry

        lax.fori_loop(0, CORES * WAYS, far_step, 0)
        lax.fori_loop(0, CORES * WAYS * WAYS, near_step, 0)
        lax.fori_loop(0, WAYS, chip_step, 0)
        lax.fori_loop(0, WAYS, own_step, 0)

    for c in range(CHUNKS):
        for i, flip in both:
            arrived(relay_back.at[i, c, flip], back_recv.at[i, c, flip])
            back_on(i, flip, c).start()

    for dst in far + near:
        key_copy(dst).wait_send()
        seg_copy(dst).wait_send()
    for c in range(CHUNKS):
        for dst in near:
            fwd_copy(dst, c).wait_send()
            for i in range(WAYS):
                ret_copy(dst, i, c).wait_send()
        for i, flip in both:
            hop_out(i, flip, c).wait_send()
            hop_on(i, flip, c).wait_send()
            back_out(i, flip, c).wait_send()
        for src in near + far:
            for i in range(WAYS):
                arrived(out_ref.at[half_rows(0, i), columns(src, c)], ret_recv.at[src, c, i])
    for c in range(CHUNKS):
        for i, flip in both:
            back_on(i, flip, c).wait_send()


def solution(mesh):
    n = mesh.shape['group']

    def per_device(sort_keys, seg_ids, payload):
        rows, width = payload.shape
        total = n * rows
        cw = width // n // CHUNKS
        dma = pltpu.SemaphoreType.DMA
        hops = (WAYS, CHUNKS, CORES)
        return pl.pallas_call(
            functools.partial(exchange_kernel, n),
            out_shape=pltpu.VMEM((rows, width), jnp.bfloat16),
            in_specs=[pl.BlockSpec(memory_space=pl.ANY)] * 3,
            out_specs=pl.BlockSpec(memory_space=pltpu.VMEM),
            scratch_shapes=[
                pltpu.VMEM((n, 1, rows), jnp.float32),
                pltpu.VMEM((n, 1, rows), jnp.int32),
                pltpu.VMEM((total, LANES), jnp.float32),
                pltpu.VMEM((total, LANES), jnp.int32),
                pltpu.VMEM((total, total), jnp.bfloat16),
                pltpu.VMEM((rows, width), jnp.bfloat16),
                pltpu.VMEM((CHUNKS, total, cw), jnp.bfloat16),
                pltpu.VMEM((CHUNKS, total, cw), jnp.bfloat16),
                pltpu.VMEM((*hops, rows // WAYS, cw), jnp.bfloat16),
                pltpu.VMEM((*hops, rows // WAYS, cw), jnp.bfloat16),
                pltpu.SemaphoreType.REGULAR, dma((n, CHUNKS)), dma((n,)), dma((n,)), dma((n,)), dma((n,)),
                dma((n, CHUNKS)), dma((n, CHUNKS)),
                dma(hops), dma(hops), dma(hops), dma((n, CHUNKS, WAYS)),
                dma((n, CHUNKS, WAYS)), dma((n, CHUNKS, WAYS)), dma(hops), dma(hops), dma(hops),
            ],
            compiler_params=pltpu.CompilerParams(collective_id=0, has_side_effects=True,
                                                 vmem_limit_bytes=56 * 1024 * 1024),
            name='exchange_sums',
        )(sort_keys.reshape(1, 1, rows), seg_ids.reshape(1, 1, rows), payload)

    row_spec = P(('batch', 'group'))
    mat_spec = P(('batch', 'group'), None)
    return jax.shard_map(per_device, mesh=mesh, in_specs=(row_spec, row_spec, mat_spec),
                         out_specs=mat_spec, check_vma=False)
```

```python
import functools

import jax
import jax.numpy as jnp
from jax import lax
from jax.experimental import pallas as pl
from jax.experimental.pallas import tpu as pltpu
from jax.sharding import PartitionSpec as P

MESH = pl.DeviceIdType.MESH
LANES = 128
CORES = 2
WAYS = 2
CHUNKS = 2
ROW_TILE = 64
EARLY_STEPS = 16
PARTS = 2


def exchange_kernel(n, keys_ref, segs_ref, pay_ref, out_ref, keys_all, segs_all, kcol, scol, mask, pay, slab, res,
                    relay, relay_back, far_ok, pay_sem, key_send, key_recv, seg_send, seg_recv, fwd_send, fwd_recv,
                    hop_send, hop_recv, on_send, ret_send, ret_recv, back_send, back_recv, back_on_send):
    me = lax.axis_index('group')
    rows, width = pay_ref.shape
    block = width // n
    cw = block // CHUNKS
    part = rows // PARTS
    lane_tiles = rows // LANES
    ring = n // CORES
    chip, core = lax.div(me, CORES), lax.rem(me, CORES)

    def peer(hop, flip):
        return lax.rem(chip + hop, ring) * CORES + lax.rem(core + flip, CORES)

    def way(i):
        return 1 + (ring - 2) * i

    near = [peer(way(i), flip) for flip in range(CORES) for i in range(WAYS)] + [peer(0, 1)]
    far = [peer(2, flip) for flip in range(CORES)]

    def remote(src, dst, send_sem, recv_sem, dev):
        return pltpu.make_async_remote_copy(src_ref=src, dst_ref=dst, send_sem=send_sem, recv_sem=recv_sem,
                                            device_id={'group': dev}, device_id_type=MESH)

    def columns(dev, c):
        return pl.ds(pl.multiple_of(dev * block + c * cw, LANES), cw)

    def dev_rows(dev):
        return pl.ds(pl.multiple_of(dev * rows, rows), rows)

    def part_rows(dev, i):
        return pl.ds(pl.multiple_of(dev * rows + i * part, part), part)

    def key_copy(dst):
        return remote(keys_ref.at[0], keys_all.at[me], key_send.at[dst], key_recv.at[me], dst)

    def seg_copy(dst):
        return remote(segs_ref.at[0], segs_all.at[me], seg_send.at[dst], seg_recv.at[me], dst)

    def pay_copy(dst):
        cols = pl.ds(pl.multiple_of(dst * block, LANES), block)
        return pltpu.make_async_copy(pay_ref.at[:, cols], pay.at[:, cols], pay_sem.at[dst])

    def fwd_copy(dst, c):
        return remote(pay.at[:, columns(dst, c)], slab.at[c, dev_rows(me), :], fwd_send.at[dst, c], fwd_recv.at[me, c], dst)

    def hop_out(i, c):
        return remote(pay.at[:, columns(peer(2, i), c)], relay.at[i, c], hop_send.at[i, c], hop_recv.at[i, c], peer(way(i), 0))

    def hop_on(i, c):
        origin = peer(way(1 - i), 0)
        return remote(relay.at[i, c], slab.at[c, dev_rows(origin), :], on_send.at[i, c], fwd_recv.at[origin, c], peer(way(i), i))

    def ret_copy(dst, c):
        return remote(res.at[c, dev_rows(dst), :], out_ref.at[:, columns(me, c)], ret_send.at[dst, c], ret_recv.at[me, c], dst)

    def back_out(i, c):
        return remote(res.at[c, dev_rows(peer(2, i)), :], relay_back.at[i, c], back_send.at[i, c], back_recv.at[i, c],
                      peer(way(i), 0))

    def back_on(i, c):
        origin = peer(way(1 - i), 0)
        return remote(relay_back.at[i, c], out_ref.at[:, columns(origin, c)], back_on_send.at[i, c], ret_recv.at[origin, c],
                      peer(way(i), i))

    def arrived(dst, sem):
        pltpu.make_async_copy(dst, dst, sem).wait()

    own_copies = [pltpu.make_async_copy(keys_ref.at[0], keys_all.at[me], key_recv.at[me]),
                  pltpu.make_async_copy(segs_ref.at[0], segs_all.at[me], seg_recv.at[me])]
    own_copies += [pltpu.make_async_copy(pay_ref.at[:, columns(me, c)], slab.at[c, dev_rows(me), :], fwd_recv.at[me, c])
                   for c in range(CHUNKS)]

    barrier = pltpu.get_barrier_semaphore()
    for dst in near:
        pl.semaphore_signal(barrier, inc=1, device_id={'group': dst}, device_id_type=MESH)
    for dst in far + near:
        pay_copy(dst).start()
    for copy in own_copies:
        copy.start()
    pl.semaphore_wait(barrier, len(near))
    pl.semaphore_signal(far_ok, inc=1, device_id={'group': peer(way(1), 0)}, device_id_type=MESH)

    for dst in near:
        key_copy(dst).start()
        seg_copy(dst).start()
    for dst in far:
        pay_copy(dst).wait()
    for i in range(WAYS):
        hop_out(i, 0).start()
    pl.semaphore_wait(far_ok, 1)
    for dst in far:
        key_copy(dst).start()
        seg_copy(dst).start()
    for dst in near:
        pay_copy(dst).wait()
        fwd_copy(dst, 0).start()

    own_copies[0].wait()
    own_copies[1].wait()
    for src in far + near:
        arrived(keys_all.at[src], key_recv.at[src])
        arrived(segs_all.at[src], seg_recv.at[src])

    def spread(dev, carry):
        for j in range(lane_tiles):
            lanes = slice(j * LANES, (j + 1) * LANES)
            dst = pl.ds(pl.multiple_of(dev * rows + j * LANES, LANES), LANES)
            kcol[dst, :] = jnp.broadcast_to(keys_all[dev, :, lanes], (LANES, LANES)).T
            scol[dst, :] = jnp.broadcast_to(segs_all[dev, :, lanes], (LANES, LANES)).T
        return carry

    lax.fori_loop(0, n, spread, 0)

    def build(t, carry):
        here = pl.ds(pl.multiple_of(t * ROW_TILE, ROW_TILE), ROW_TILE)
        key_r, seg_r = kcol[here, :], scol[here, :]
        last = jnp.full((ROW_TILE, LANES), -jnp.inf, jnp.float32)
        for dev in range(n):
            for j in range(lane_tiles):
                lanes = slice(j * LANES, (j + 1) * LANES)
                key_s, seg_s = keys_all[dev, :, lanes], segs_all[dev, :, lanes]
                other = jnp.logical_and(key_s < key_r, seg_s != seg_r)
                last = jnp.maximum(last, jnp.where(other, key_s, -jnp.inf))
        last = jnp.broadcast_to(jnp.max(last, axis=1, keepdims=True), (ROW_TILE, LANES))
        for dev in range(n):
            for j in range(lane_tiles):
                lanes = slice(j * LANES, (j + 1) * LANES)
                key_s = keys_all[dev, :, lanes]
                inside = jnp.logical_and(key_s <= key_r, key_s > last)
                at = slice(dev * rows + j * LANES, dev * rows + (j + 1) * LANES)
                mask[here, at] = jnp.where(inside, 1.0, 0.0).astype(jnp.bfloat16)
        return carry

    steps = n * rows // ROW_TILE
    for c in range(CHUNKS):
        lax.fori_loop(EARLY_STEPS * c, EARLY_STEPS * (c + 1) if c < CHUNKS - 1 else steps, build, 0)
        for i in range(WAYS):
            arrived(relay.at[i, c], hop_recv.at[i, c])
            hop_on(i, c).start()
        if c + 1 < CHUNKS:
            for i in range(WAYS):
                hop_out(i, c + 1).start()
            for dst in near:
                fwd_copy(dst, c + 1).start()

    def sums(dev, i, c):
        return jnp.dot(mask[part_rows(dev, i), :], slab[c], preferred_element_type=jnp.float32).astype(jnp.bfloat16)

    def near_pick(k):
        return peer(way(lax.rem(k, WAYS)), lax.div(k, WAYS))

    for c in range(CHUNKS):
        own_copies[2 + c].wait()
        for src in near + far:
            arrived(slab.at[c, dev_rows(src), :], fwd_recv.at[src, c])

        def block_step(pick, before, send, c=c):
            def step_fn(step, carry):
                k, i = lax.div(step, PARTS), lax.rem(step, PARTS)
                dev = pick(k)
                res[c, part_rows(dev, i), :] = sums(dev, i, c)

                if before is not None:
                    @pl.when(step == 0)
                    def _():
                        before.start()

                @pl.when(jnp.logical_and(i == 0, step > 0))
                def _():
                    send(k - 1).start()

                return carry
            return step_fn

        lax.fori_loop(0, WAYS * PARTS, block_step(lambda k: peer(2, k), None, lambda k: back_out(k, c)), 0)
        lax.fori_loop(0, WAYS * CORES * PARTS,
                      block_step(near_pick, back_out(WAYS - 1, c), lambda k: ret_copy(near_pick(k), c)), 0)
        lax.fori_loop(0, PARTS, block_step(lambda k: peer(0, 1), ret_copy(near[-2], c), lambda k: ret_copy(near[-1], c)), 0)

        def own_step(i, carry, c=c):
            out_ref[part_rows(0, i), columns(me, c)] = sums(me, i, c)

            @pl.when(i == 0)
            def _():
                ret_copy(near[-1], c).start()

            return carry

        lax.fori_loop(0, PARTS, own_step, 0)

    for c in range(CHUNKS):
        for i in range(WAYS):
            arrived(relay_back.at[i, c], back_recv.at[i, c])
            back_on(i, c).start()

    for dst in far + near:
        key_copy(dst).wait_send()
        seg_copy(dst).wait_send()
    for c in range(CHUNKS):
        for dst in near:
            fwd_copy(dst, c).wait_send()
            ret_copy(dst, c).wait_send()
        for i in range(WAYS):
            hop_out(i, c).wait_send()
            hop_on(i, c).wait_send()
            back_out(i, c).wait_send()
        for src in near + far:
            arrived(out_ref.at[:, columns(src, c)], ret_recv.at[src, c])
    for c in range(CHUNKS):
        for i in range(WAYS):
            back_on(i, c).wait_send()


def solution(mesh):
    n = mesh.shape['group']

    def per_device(sort_keys, seg_ids, payload):
        rows, width = payload.shape
        total = n * rows
        cw = width // n // CHUNKS
        dma = pltpu.SemaphoreType.DMA
        hops = (WAYS, CHUNKS)
        return pl.pallas_call(
            functools.partial(exchange_kernel, n),
            out_shape=pltpu.VMEM((rows, width), jnp.bfloat16),
            in_specs=[pl.BlockSpec(memory_space=pl.ANY)] * 3,
            out_specs=pl.BlockSpec(memory_space=pltpu.VMEM),
            scratch_shapes=[
                pltpu.VMEM((n, 1, rows), jnp.float32),
                pltpu.VMEM((n, 1, rows), jnp.int32),
                pltpu.VMEM((total, LANES), jnp.float32),
                pltpu.VMEM((total, LANES), jnp.int32),
                pltpu.VMEM((total, total), jnp.bfloat16),
                pltpu.VMEM((rows, width), jnp.bfloat16),
                pltpu.VMEM((CHUNKS, total, cw), jnp.bfloat16),
                pltpu.VMEM((CHUNKS, total, cw), jnp.bfloat16),
                pltpu.VMEM((*hops, rows, cw), jnp.bfloat16),
                pltpu.VMEM((*hops, rows, cw), jnp.bfloat16),
                pltpu.SemaphoreType.REGULAR, dma((n,)), dma((n,)), dma((n,)), dma((n,)), dma((n,)),
                dma((n, CHUNKS)), dma((n, CHUNKS)),
                dma(hops), dma(hops), dma(hops),
                dma((n, CHUNKS)), dma((n, CHUNKS)), dma(hops), dma(hops), dma(hops),
            ],
            compiler_params=pltpu.CompilerParams(collective_id=0, has_side_effects=True,
                                                 vmem_limit_bytes=56 * 1024 * 1024),
            name='exchange_sums',
        )(sort_keys.reshape(1, 1, rows), seg_ids.reshape(1, 1, rows), payload)

    row_spec = P(('batch', 'group'))
    mat_spec = P(('batch', 'group'), None)
    return jax.shard_map(per_device, mesh=mesh, in_specs=(row_spec, row_spec, mat_spec),
                         out_specs=mat_spec, check_vma=False)
```

```python
import functools

import jax
import jax.numpy as jnp
from jax import lax
from jax.experimental import pallas as pl
from jax.experimental.pallas import tpu as pltpu
from jax.sharding import PartitionSpec as P

MESH = pl.DeviceIdType.MESH
LANES = 128
CORES = 2
WAYS = 2
CHUNKS = 2
ROW_TILE = 64
EARLY_STEPS = 16
PARTS = 2


def exchange_kernel(n, keys_ref, segs_ref, pay_ref, out_ref, keys_all, segs_all, kcol, scol, mask, pay, slab, res,
                    relay, relay_back, far_ok, pay_sem, key_send, key_recv, seg_send, seg_recv, fwd_send, fwd_recv,
                    hop_send, hop_recv, on_send, ret_send, ret_recv, back_send, back_recv, back_on_send):
    me = lax.axis_index('group')
    rows, width = pay_ref.shape
    block = width // n
    cw = block // CHUNKS
    part = rows // PARTS
    lane_tiles = rows // LANES
    ring = n // CORES
    chip, core = lax.div(me, CORES), lax.rem(me, CORES)

    def peer(hop, flip):
        return lax.rem(chip + hop, ring) * CORES + lax.rem(core + flip, CORES)

    def way(i):
        return 1 + (ring - 2) * i

    near = [peer(way(i), flip) for flip in range(CORES) for i in range(WAYS)] + [peer(0, 1)]
    far = [peer(2, flip) for flip in range(CORES)]

    def remote(src, dst, send_sem, recv_sem, dev):
        return pltpu.make_async_remote_copy(src_ref=src, dst_ref=dst, send_sem=send_sem, recv_sem=recv_sem,
                                            device_id={'group': dev}, device_id_type=MESH)

    def columns(dev, c):
        return pl.ds(pl.multiple_of(dev * block + c * cw, LANES), cw)

    def dev_rows(dev):
        return pl.ds(pl.multiple_of(dev * rows, rows), rows)

    def part_rows(dev, i):
        return pl.ds(pl.multiple_of(dev * rows + i * part, part), part)

    def key_copy(dst):
        return remote(keys_ref.at[0], keys_all.at[me], key_send.at[dst], key_recv.at[me], dst)

    def seg_copy(dst):
        return remote(segs_ref.at[0], segs_all.at[me], seg_send.at[dst], seg_recv.at[me], dst)

    def pay_copy(dst):
        cols = pl.ds(pl.multiple_of(dst * block, LANES), block)
        return pltpu.make_async_copy(pay_ref.at[:, cols], pay.at[:, cols], pay_sem.at[dst])

    def fwd_copy(dst, c):
        return remote(pay.at[:, columns(dst, c)], slab.at[c, dev_rows(me), :], fwd_send.at[dst, c], fwd_recv.at[me, c], dst)

    def hop_out(i, c):
        return remote(pay.at[:, columns(peer(2, i), c)], relay.at[i, c], hop_send.at[i, c], hop_recv.at[i, c], peer(way(i), 0))

    def hop_part(i, c, piece):
        return remote(pay.at[part_rows(0, piece), columns(peer(2, i), c)], relay.at[i, c, part_rows(0, piece), :],
                      hop_send.at[i, c], hop_recv.at[i, c], peer(way(i), 0))

    def hop_on(i, c):
        origin = peer(way(1 - i), 0)
        return remote(relay.at[i, c], slab.at[c, dev_rows(origin), :], on_send.at[i, c], fwd_recv.at[origin, c], peer(way(i), i))

    def ret_copy(dst, c):
        return remote(res.at[c, dev_rows(dst), :], out_ref.at[:, columns(me, c)], ret_send.at[dst, c], ret_recv.at[me, c], dst)

    def back_out(i, c):
        return remote(res.at[c, dev_rows(peer(2, i)), :], relay_back.at[i, c], back_send.at[i, c], back_recv.at[i, c],
                      peer(way(i), 0))

    def back_on(i, c):
        origin = peer(way(1 - i), 0)
        return remote(relay_back.at[i, c], out_ref.at[:, columns(origin, c)], back_on_send.at[i, c], ret_recv.at[origin, c],
                      peer(way(i), i))

    def arrived(dst, sem):
        pltpu.make_async_copy(dst, dst, sem).wait()

    own_copies = [pltpu.make_async_copy(keys_ref.at[0], keys_all.at[me], key_recv.at[me]),
                  pltpu.make_async_copy(segs_ref.at[0], segs_all.at[me], seg_recv.at[me])]
    own_copies += [pltpu.make_async_copy(pay_ref.at[:, columns(me, c)], slab.at[c, dev_rows(me), :], fwd_recv.at[me, c])
                   for c in range(CHUNKS)]

    barrier = pltpu.get_barrier_semaphore()
    for dst in near:
        pl.semaphore_signal(barrier, inc=1, device_id={'group': dst}, device_id_type=MESH)
    for dst in far + near:
        pay_copy(dst).start()
    for copy in own_copies:
        copy.start()
    pl.semaphore_wait(barrier, len(near))
    pl.semaphore_signal(far_ok, inc=1, device_id={'group': peer(way(1), 0)}, device_id_type=MESH)

    for dst in near:
        key_copy(dst).start()
        seg_copy(dst).start()
    for dst in far:
        pay_copy(dst).wait()
    @pl.when(core == 0)
    def _():
        for i in range(WAYS):
            hop_out(i, 0).start()

    @pl.when(core != 0)
    def _():
        for piece in range(PARTS):
            for i in range(WAYS):
                hop_part(i, 0, piece).start()

    pl.semaphore_wait(far_ok, 1)
    for dst in far:
        key_copy(dst).start()
        seg_copy(dst).start()
    for dst in near:
        pay_copy(dst).wait()
        fwd_copy(dst, 0).start()

    own_copies[0].wait()
    own_copies[1].wait()
    for src in far + near:
        arrived(keys_all.at[src], key_recv.at[src])
        arrived(segs_all.at[src], seg_recv.at[src])

    def spread(dev, carry):
        for j in range(lane_tiles):
            lanes = slice(j * LANES, (j + 1) * LANES)
            dst = pl.ds(pl.multiple_of(dev * rows + j * LANES, LANES), LANES)
            kcol[dst, :] = jnp.broadcast_to(keys_all[dev, :, lanes], (LANES, LANES)).T
            scol[dst, :] = jnp.broadcast_to(segs_all[dev, :, lanes], (LANES, LANES)).T
        return carry

    lax.fori_loop(0, n, spread, 0)

    def build(t, carry):
        here = pl.ds(pl.multiple_of(t * ROW_TILE, ROW_TILE), ROW_TILE)
        key_r, seg_r = kcol[here, :], scol[here, :]
        last = jnp.full((ROW_TILE, LANES), -jnp.inf, jnp.float32)
        for dev in range(n):
            for j in range(lane_tiles):
                lanes = slice(j * LANES, (j + 1) * LANES)
                key_s, seg_s = keys_all[dev, :, lanes], segs_all[dev, :, lanes]
                other = jnp.logical_and(key_s < key_r, seg_s != seg_r)
                last = jnp.maximum(last, jnp.where(other, key_s, -jnp.inf))
        last = jnp.broadcast_to(jnp.max(last, axis=1, keepdims=True), (ROW_TILE, LANES))
        for dev in range(n):
            for j in range(lane_tiles):
                lanes = slice(j * LANES, (j + 1) * LANES)
                key_s = keys_all[dev, :, lanes]
                inside = jnp.logical_and(key_s <= key_r, key_s > last)
                at = slice(dev * rows + j * LANES, dev * rows + (j + 1) * LANES)
                mask[here, at] = jnp.where(inside, 1.0, 0.0).astype(jnp.bfloat16)
        return carry

    steps = n * rows // ROW_TILE
    for c in range(CHUNKS):
        lax.fori_loop(EARLY_STEPS * c, EARLY_STEPS * (c + 1) if c < CHUNKS - 1 else steps, build, 0)
        for i in range(WAYS):
            arrived(relay.at[i, c], hop_recv.at[i, c])
            hop_on(i, c).start()
        if c + 1 < CHUNKS:
            for i in range(WAYS):
                hop_out(i, c + 1).start()
            for dst in near:
                fwd_copy(dst, c + 1).start()

    def sums(dev, i, c):
        return jnp.dot(mask[part_rows(dev, i), :], slab[c], preferred_element_type=jnp.float32).astype(jnp.bfloat16)

    def near_pick(k):
        return peer(way(lax.rem(k, WAYS)), lax.div(k, WAYS))

    for c in range(CHUNKS):
        own_copies[2 + c].wait()
        for src in near + far:
            arrived(slab.at[c, dev_rows(src), :], fwd_recv.at[src, c])

        def block_step(pick, before, send, c=c):
            def step_fn(step, carry):
                k, i = lax.div(step, PARTS), lax.rem(step, PARTS)
                dev = pick(k)
                res[c, part_rows(dev, i), :] = sums(dev, i, c)

                if before is not None:
                    @pl.when(step == 0)
                    def _():
                        before.start()

                @pl.when(jnp.logical_and(i == 0, step > 0))
                def _():
                    send(k - 1).start()

                return carry
            return step_fn

        lax.fori_loop(0, WAYS * PARTS, block_step(lambda k: peer(2, k), None, lambda k: back_out(k, c)), 0)
        lax.fori_loop(0, WAYS * CORES * PARTS,
                      block_step(near_pick, back_out(WAYS - 1, c), lambda k: ret_copy(near_pick(k), c)), 0)
        lax.fori_loop(0, PARTS, block_step(lambda k: peer(0, 1), ret_copy(near[-2], c), lambda k: ret_copy(near[-1], c)), 0)

        def own_step(i, carry, c=c):
            out_ref[part_rows(0, i), columns(me, c)] = sums(me, i, c)

            @pl.when(i == 0)
            def _():
                ret_copy(near[-1], c).start()

            return carry

        lax.fori_loop(0, PARTS, own_step, 0)

    for c in range(CHUNKS):
        for i in range(WAYS):
            arrived(relay_back.at[i, c], back_recv.at[i, c])
            back_on(i, c).start()

    for dst in far + near:
        key_copy(dst).wait_send()
        seg_copy(dst).wait_send()
    for c in range(CHUNKS):
        for dst in near:
            fwd_copy(dst, c).wait_send()
            ret_copy(dst, c).wait_send()
        for i in range(WAYS):
            hop_out(i, c).wait_send()
            hop_on(i, c).wait_send()
            back_out(i, c).wait_send()
        for src in near + far:
            arrived(out_ref.at[:, columns(src, c)], ret_recv.at[src, c])
    for c in range(CHUNKS):
        for i in range(WAYS):
            back_on(i, c).wait_send()


def solution(mesh):
    n = mesh.shape['group']

    def per_device(sort_keys, seg_ids, payload):
        rows, width = payload.shape
        total = n * rows
        cw = width // n // CHUNKS
        dma = pltpu.SemaphoreType.DMA
        hops = (WAYS, CHUNKS)
        return pl.pallas_call(
            functools.partial(exchange_kernel, n),
            out_shape=pltpu.VMEM((rows, width), jnp.bfloat16),
            in_specs=[pl.BlockSpec(memory_space=pl.ANY)] * 3,
            out_specs=pl.BlockSpec(memory_space=pltpu.VMEM),
            scratch_shapes=[
                pltpu.VMEM((n, 1, rows), jnp.float32),
                pltpu.VMEM((n, 1, rows), jnp.int32),
                pltpu.VMEM((total, LANES), jnp.float32),
                pltpu.VMEM((total, LANES), jnp.int32),
                pltpu.VMEM((total, total), jnp.bfloat16),
                pltpu.VMEM((rows, width), jnp.bfloat16),
                pltpu.VMEM((CHUNKS, total, cw), jnp.bfloat16),
                pltpu.VMEM((CHUNKS, total, cw), jnp.bfloat16),
                pltpu.VMEM((*hops, rows, cw), jnp.bfloat16),
                pltpu.VMEM((*hops, rows, cw), jnp.bfloat16),
                pltpu.SemaphoreType.REGULAR, dma((n,)), dma((n,)), dma((n,)), dma((n,)), dma((n,)),
                dma((n, CHUNKS)), dma((n, CHUNKS)),
                dma(hops), dma(hops), dma(hops),
                dma((n, CHUNKS)), dma((n, CHUNKS)), dma(hops), dma(hops), dma(hops),
            ],
            compiler_params=pltpu.CompilerParams(collective_id=0, has_side_effects=True,
                                                 vmem_limit_bytes=56 * 1024 * 1024),
            name='exchange_sums',
        )(sort_keys.reshape(1, 1, rows), seg_ids.reshape(1, 1, rows), payload)

    row_spec = P(('batch', 'group'))
    mat_spec = P(('batch', 'group'), None)
    return jax.shard_map(per_device, mesh=mesh, in_specs=(row_spec, row_spec, mat_spec),
                         out_specs=mat_spec, check_vma=False)
```

```python
import functools

import jax
import jax.numpy as jnp
from jax import lax
from jax.experimental import pallas as pl
from jax.experimental.pallas import tpu as pltpu
from jax.sharding import PartitionSpec as P

MESH = pl.DeviceIdType.MESH
LANES = 128
CORES = 2
WAYS = 2
CHUNKS = 2
ROW_TILE = 64
EARLY_STEPS = 16
PARTS = 2


def exchange_kernel(n, keys_ref, segs_ref, pay_ref, out_ref, keys_all, segs_all, kcol, scol, mask, pay, slab, res,
                    relay, relay_back, far_ok, pay_sem, key_send, key_recv, seg_send, seg_recv, fwd_send, fwd_recv,
                    hop_send, hop_recv, on_send, ret_send, ret_recv, back_send, back_recv, back_on_send):
    me = lax.axis_index('group')
    rows, width = pay_ref.shape
    block = width // n
    cw = block // CHUNKS
    part = rows // PARTS
    lane_tiles = rows // LANES
    ring = n // CORES
    chip, core = lax.div(me, CORES), lax.rem(me, CORES)

    def peer(hop, flip):
        return lax.rem(chip + hop, ring) * CORES + lax.rem(core + flip, CORES)

    def way(i):
        return 1 + (ring - 2) * i

    near = [peer(way(i), flip) for flip in range(CORES) for i in range(WAYS)] + [peer(0, 1)]
    far = [peer(2, flip) for flip in range(CORES)]

    def remote(src, dst, send_sem, recv_sem, dev):
        return pltpu.make_async_remote_copy(src_ref=src, dst_ref=dst, send_sem=send_sem, recv_sem=recv_sem,
                                            device_id={'group': dev}, device_id_type=MESH)

    def columns(dev, c):
        return pl.ds(pl.multiple_of(dev * block + c * cw, LANES), cw)

    def dev_rows(dev):
        return pl.ds(pl.multiple_of(dev * rows, rows), rows)

    def part_rows(dev, i):
        return pl.ds(pl.multiple_of(dev * rows + i * part, part), part)

    def key_copy(dst):
        return remote(keys_ref.at[0], keys_all.at[me], key_send.at[dst], key_recv.at[me], dst)

    def seg_copy(dst):
        return remote(segs_ref.at[0], segs_all.at[me], seg_send.at[dst], seg_recv.at[me], dst)

    def pay_copy(dst, c):
        return pltpu.make_async_copy(pay_ref.at[:, columns(dst, c)], pay.at[:, columns(dst, c)], pay_sem.at[dst, c])

    def fwd_copy(dst, c):
        return remote(pay.at[:, columns(dst, c)], slab.at[c, dev_rows(me), :], fwd_send.at[dst, c], fwd_recv.at[me, c], dst)

    def hop_out(i, c):
        return remote(pay.at[:, columns(peer(2, i), c)], relay.at[i, c], hop_send.at[i, c], hop_recv.at[i, c], peer(way(i), 0))

    def hop_on(i, c):
        origin = peer(way(1 - i), 0)
        return remote(relay.at[i, c], slab.at[c, dev_rows(origin), :], on_send.at[i, c], fwd_recv.at[origin, c], peer(way(i), i))

    def ret_copy(dst, c):
        return remote(res.at[c, dev_rows(dst), :], out_ref.at[:, columns(me, c)], ret_send.at[dst, c], ret_recv.at[me, c], dst)

    def back_out(i, c):
        return remote(res.at[c, dev_rows(peer(2, i)), :], relay_back.at[i, c], back_send.at[i, c], back_recv.at[i, c],
                      peer(way(i), 0))

    def back_on(i, c):
        origin = peer(way(1 - i), 0)
        return remote(relay_back.at[i, c], out_ref.at[:, columns(origin, c)], back_on_send.at[i, c], ret_recv.at[origin, c],
                      peer(way(i), i))

    def arrived(dst, sem):
        pltpu.make_async_copy(dst, dst, sem).wait()

    own_copies = [pltpu.make_async_copy(keys_ref.at[0], keys_all.at[me], key_recv.at[me]),
                  pltpu.make_async_copy(segs_ref.at[0], segs_all.at[me], seg_recv.at[me])]
    own_copies += [pltpu.make_async_copy(pay_ref.at[:, columns(me, c)], slab.at[c, dev_rows(me), :], fwd_recv.at[me, c])
                   for c in range(CHUNKS)]

    barrier = pltpu.get_barrier_semaphore()
    for dst in near:
        pl.semaphore_signal(barrier, inc=1, device_id={'group': dst}, device_id_type=MESH)
    for dst in far + near:
        pay_copy(dst, 0).start()
    pl.semaphore_wait(barrier, len(near))
    pl.semaphore_signal(far_ok, inc=1, device_id={'group': peer(way(1), 0)}, device_id_type=MESH)

    for dst in near:
        key_copy(dst).start()
        seg_copy(dst).start()
    for i in range(WAYS):
        pay_copy(far[i], 0).wait()
        hop_out(i, 0).start()
    pl.semaphore_wait(far_ok, 1)
    for dst in far:
        key_copy(dst).start()
        seg_copy(dst).start()
    for dst in near:
        pay_copy(dst, 0).wait()
        fwd_copy(dst, 0).start()
    for copy in own_copies:
        copy.start()
    for dst in far + near:
        pay_copy(dst, 1).start()

    own_copies[0].wait()
    own_copies[1].wait()
    for src in far + near:
        arrived(keys_all.at[src], key_recv.at[src])
        arrived(segs_all.at[src], seg_recv.at[src])

    def spread(dev, carry):
        for j in range(lane_tiles):
            lanes = slice(j * LANES, (j + 1) * LANES)
            dst = pl.ds(pl.multiple_of(dev * rows + j * LANES, LANES), LANES)
            kcol[dst, :] = jnp.broadcast_to(keys_all[dev, :, lanes], (LANES, LANES)).T
            scol[dst, :] = jnp.broadcast_to(segs_all[dev, :, lanes], (LANES, LANES)).T
        return carry

    lax.fori_loop(0, n, spread, 0)

    def build(t, carry):
        here = pl.ds(pl.multiple_of(t * ROW_TILE, ROW_TILE), ROW_TILE)
        key_r, seg_r = kcol[here, :], scol[here, :]
        last = jnp.full((ROW_TILE, LANES), -jnp.inf, jnp.float32)
        for dev in range(n):
            for j in range(lane_tiles):
                lanes = slice(j * LANES, (j + 1) * LANES)
                key_s, seg_s = keys_all[dev, :, lanes], segs_all[dev, :, lanes]
                other = jnp.logical_and(key_s < key_r, seg_s != seg_r)
                last = jnp.maximum(last, jnp.where(other, key_s, -jnp.inf))
        last = jnp.broadcast_to(jnp.max(last, axis=1, keepdims=True), (ROW_TILE, LANES))
        for dev in range(n):
            for j in range(lane_tiles):
                lanes = slice(j * LANES, (j + 1) * LANES)
                key_s = keys_all[dev, :, lanes]
                inside = jnp.logical_and(key_s <= key_r, key_s > last)
                at = slice(dev * rows + j * LANES, dev * rows + (j + 1) * LANES)
                mask[here, at] = jnp.where(inside, 1.0, 0.0).astype(jnp.bfloat16)
        return carry

    steps = n * rows // ROW_TILE
    for c in range(CHUNKS):
        lax.fori_loop(EARLY_STEPS * c, EARLY_STEPS * (c + 1) if c < CHUNKS - 1 else steps, build, 0)
        for i in range(WAYS):
            arrived(relay.at[i, c], hop_recv.at[i, c])
            hop_on(i, c).start()
        if c + 1 < CHUNKS:
            for dst in far + near:
                pay_copy(dst, c + 1).wait()
            for i in range(WAYS):
                hop_out(i, c + 1).start()
            for dst in near:
                fwd_copy(dst, c + 1).start()

    def sums(dev, i, c):
        return jnp.dot(mask[part_rows(dev, i), :], slab[c], preferred_element_type=jnp.float32).astype(jnp.bfloat16)

    def near_pick(k):
        return peer(way(lax.rem(k, WAYS)), lax.div(k, WAYS))

    for c in range(CHUNKS):
        own_copies[2 + c].wait()
        for src in near + far:
            arrived(slab.at[c, dev_rows(src), :], fwd_recv.at[src, c])

        def block_step(pick, before, send, c=c):
            def step_fn(step, carry):
                k, i = lax.div(step, PARTS), lax.rem(step, PARTS)
                dev = pick(k)
                res[c, part_rows(dev, i), :] = sums(dev, i, c)

                if before is not None:
                    @pl.when(step == 0)
                    def _():
                        before.start()

                @pl.when(jnp.logical_and(i == 0, step > 0))
                def _():
                    send(k - 1).start()

                return carry
            return step_fn

        lax.fori_loop(0, WAYS * PARTS, block_step(lambda k: peer(2, k), None, lambda k: back_out(k, c)), 0)
        lax.fori_loop(0, WAYS * CORES * PARTS,
                      block_step(near_pick, back_out(WAYS - 1, c), lambda k: ret_copy(near_pick(k), c)), 0)
        lax.fori_loop(0, PARTS, block_step(lambda k: peer(0, 1), ret_copy(near[-2], c), lambda k: ret_copy(near[-1], c)), 0)

        def own_step(i, carry, c=c):
            out_ref[part_rows(0, i), columns(me, c)] = sums(me, i, c)

            @pl.when(i == 0)
            def _():
                ret_copy(near[-1], c).start()

            return carry

        lax.fori_loop(0, PARTS, own_step, 0)

    for c in range(CHUNKS):
        for i in range(WAYS):
            arrived(relay_back.at[i, c], back_recv.at[i, c])
            back_on(i, c).start()

    for dst in far + near:
        key_copy(dst).wait_send()
        seg_copy(dst).wait_send()
    for c in range(CHUNKS):
        for dst in near:
            fwd_copy(dst, c).wait_send()
            ret_copy(dst, c).wait_send()
        for i in range(WAYS):
            hop_out(i, c).wait_send()
            hop_on(i, c).wait_send()
            back_out(i, c).wait_send()
        for src in near + far:
            arrived(out_ref.at[:, columns(src, c)], ret_recv.at[src, c])
    for c in range(CHUNKS):
        for i in range(WAYS):
            back_on(i, c).wait_send()


def solution(mesh):
    n = mesh.shape['group']

    def per_device(sort_keys, seg_ids, payload):
        rows, width = payload.shape
        total = n * rows
        cw = width // n // CHUNKS
        dma = pltpu.SemaphoreType.DMA
        hops = (WAYS, CHUNKS)
        return pl.pallas_call(
            functools.partial(exchange_kernel, n),
            out_shape=pltpu.VMEM((rows, width), jnp.bfloat16),
            in_specs=[pl.BlockSpec(memory_space=pl.ANY)] * 3,
            out_specs=pl.BlockSpec(memory_space=pltpu.VMEM),
            scratch_shapes=[
                pltpu.VMEM((n, 1, rows), jnp.float32),
                pltpu.VMEM((n, 1, rows), jnp.int32),
                pltpu.VMEM((total, LANES), jnp.float32),
                pltpu.VMEM((total, LANES), jnp.int32),
                pltpu.VMEM((total, total), jnp.bfloat16),
                pltpu.VMEM((rows, width), jnp.bfloat16),
                pltpu.VMEM((CHUNKS, total, cw), jnp.bfloat16),
                pltpu.VMEM((CHUNKS, total, cw), jnp.bfloat16),
                pltpu.VMEM((*hops, rows, cw), jnp.bfloat16),
                pltpu.VMEM((*hops, rows, cw), jnp.bfloat16),
                pltpu.SemaphoreType.REGULAR, dma((n, CHUNKS)), dma((n,)), dma((n,)), dma((n,)), dma((n,)),
                dma((n, CHUNKS)), dma((n, CHUNKS)),
                dma(hops), dma(hops), dma(hops),
                dma((n, CHUNKS)), dma((n, CHUNKS)), dma(hops), dma(hops), dma(hops),
            ],
            compiler_params=pltpu.CompilerParams(collective_id=0, has_side_effects=True,
                                                 vmem_limit_bytes=56 * 1024 * 1024),
            name='exchange_sums',
        )(sort_keys.reshape(1, 1, rows), seg_ids.reshape(1, 1, rows), payload)

    row_spec = P(('batch', 'group'))
    mat_spec = P(('batch', 'group'), None)
    return jax.shard_map(per_device, mesh=mesh, in_specs=(row_spec, row_spec, mat_spec),
                         out_specs=mat_spec, check_vma=False)
```

```python
import functools

import jax
import jax.numpy as jnp
from jax import lax
from jax.experimental import pallas as pl
from jax.experimental.pallas import tpu as pltpu
from jax.sharding import PartitionSpec as P

MESH = pl.DeviceIdType.MESH
LANES = 128
CORES = 2
WAYS = 2
CHUNKS = 2
ROW_TILE = 64
EARLY_STEPS = 32
PARTS = 2


def exchange_kernel(n, keys_ref, segs_ref, pay_ref, out_ref, keys_all, segs_all, kcol, scol, mask, pay, slab, res,
                    relay, relay_back, far_ok, pay_sem, key_send, key_recv, seg_send, seg_recv, fwd_send, fwd_recv,
                    hop_send, hop_recv, on_send, ret_send, ret_recv, back_send, back_recv, back_on_send):
    me = lax.axis_index('group')
    rows, width = pay_ref.shape
    block = width // n
    cw = block // CHUNKS
    part = rows // PARTS
    lane_tiles = rows // LANES
    ring = n // CORES
    chip, core = lax.div(me, CORES), lax.rem(me, CORES)

    def peer(hop, flip):
        return lax.rem(chip + hop, ring) * CORES + lax.rem(core + flip, CORES)

    def way(i):
        return 1 + (ring - 2) * i

    near = [peer(way(i), flip) for flip in range(CORES) for i in range(WAYS)] + [peer(0, 1)]
    far = [peer(2, flip) for flip in range(CORES)]

    def remote(src, dst, send_sem, recv_sem, dev):
        return pltpu.make_async_remote_copy(src_ref=src, dst_ref=dst, send_sem=send_sem, recv_sem=recv_sem,
                                            device_id={'group': dev}, device_id_type=MESH)

    def columns(dev, c):
        return pl.ds(pl.multiple_of(dev * block + c * cw, LANES), cw)

    def block_cols(dev):
        return pl.ds(pl.multiple_of(dev * block, LANES), block)

    def chunk(c):
        return pl.ds(c * cw, cw)

    def dev_rows(dev):
        return pl.ds(pl.multiple_of(dev * rows, rows), rows)

    def part_rows(dev, i):
        return pl.ds(pl.multiple_of(dev * rows + i * part, part), part)

    def key_copy(dst):
        return remote(keys_ref.at[0], keys_all.at[me], key_send.at[dst], key_recv.at[me], dst)

    def seg_copy(dst):
        return remote(segs_ref.at[0], segs_all.at[me], seg_send.at[dst], seg_recv.at[me], dst)

    def pay_copy(dst, c):
        return pltpu.make_async_copy(pay_ref.at[:, columns(dst, c)], pay.at[:, columns(dst, c)], pay_sem.at[dst, c])

    def fwd_copy(dst, c):
        return remote(pay.at[:, columns(dst, c)], slab.at[dev_rows(me), chunk(c)], fwd_send.at[dst, c], fwd_recv.at[me, c], dst)

    def hop_out(i):
        return remote(pay.at[:, block_cols(peer(2, i))], relay.at[i], hop_send.at[i], hop_recv.at[i], peer(way(i), 0))

    def hop_on(i):
        origin = peer(way(1 - i), 0)
        return remote(relay.at[i], slab.at[dev_rows(origin), :], on_send.at[i], fwd_recv.at[origin, 0], peer(way(i), i))

    def ret_copy(dst, c):
        return remote(res.at[dev_rows(dst), chunk(c)], out_ref.at[:, columns(me, c)], ret_send.at[dst, c], ret_recv.at[me], dst)

    def ret_whole(dst):
        return remote(res.at[dev_rows(dst), :], out_ref.at[:, block_cols(me)], ret_send.at[dst, 0], ret_recv.at[me], dst)

    def back_out(i, c):
        return remote(res.at[dev_rows(peer(2, i)), chunk(c)], relay_back.at[i, :, chunk(c)], back_send.at[i, c],
                      back_recv.at[i], peer(way(i), 0))

    def back_on(i):
        origin = peer(way(1 - i), 0)
        return remote(relay_back.at[i], out_ref.at[:, block_cols(origin)], back_on_send.at[i], ret_recv.at[origin],
                      peer(way(i), i))

    def arrived(dst, sem):
        pltpu.make_async_copy(dst, dst, sem).wait()

    own_copies = [pltpu.make_async_copy(keys_ref.at[0], keys_all.at[me], key_recv.at[me]),
                  pltpu.make_async_copy(segs_ref.at[0], segs_all.at[me], seg_recv.at[me])]
    own_copies += [pltpu.make_async_copy(pay_ref.at[:, columns(me, c)], slab.at[dev_rows(me), chunk(c)], fwd_recv.at[me, c])
                   for c in range(CHUNKS)]

    barrier = pltpu.get_barrier_semaphore()
    for dst in near:
        pl.semaphore_signal(barrier, inc=1, device_id={'group': dst}, device_id_type=MESH)
    for dst in far:
        for c in range(CHUNKS):
            pay_copy(dst, c).start()
    for dst in near:
        pay_copy(dst, 0).start()
    pl.semaphore_wait(barrier, len(near))
    pl.semaphore_signal(far_ok, inc=1, device_id={'group': peer(way(1), 0)}, device_id_type=MESH)

    for dst in near:
        key_copy(dst).start()
        seg_copy(dst).start()
    for i in range(WAYS):
        for c in range(CHUNKS):
            pay_copy(far[i], c).wait()
        hop_out(i).start()
    pl.semaphore_wait(far_ok, 1)
    for dst in far:
        key_copy(dst).start()
        seg_copy(dst).start()
    for dst in near:
        pay_copy(dst, 0).wait()
        fwd_copy(dst, 0).start()
    for copy in own_copies:
        copy.start()
    for dst in near:
        pay_copy(dst, 1).start()

    own_copies[0].wait()
    own_copies[1].wait()
    for src in far + near:
        arrived(keys_all.at[src], key_recv.at[src])
        arrived(segs_all.at[src], seg_recv.at[src])

    def spread(dev, carry):
        for j in range(lane_tiles):
            lanes = slice(j * LANES, (j + 1) * LANES)
            dst = pl.ds(pl.multiple_of(dev * rows + j * LANES, LANES), LANES)
            kcol[dst, :] = jnp.broadcast_to(keys_all[dev, :, lanes], (LANES, LANES)).T
            scol[dst, :] = jnp.broadcast_to(segs_all[dev, :, lanes], (LANES, LANES)).T
        return carry

    lax.fori_loop(0, n, spread, 0)

    def build(t, carry):
        here = pl.ds(pl.multiple_of(t * ROW_TILE, ROW_TILE), ROW_TILE)
        key_r, seg_r = kcol[here, :], scol[here, :]
        last = jnp.full((ROW_TILE, LANES), -jnp.inf, jnp.float32)
        for dev in range(n):
            for j in range(lane_tiles):
                lanes = slice(j * LANES, (j + 1) * LANES)
                key_s, seg_s = keys_all[dev, :, lanes], segs_all[dev, :, lanes]
                other = jnp.logical_and(key_s < key_r, seg_s != seg_r)
                last = jnp.maximum(last, jnp.where(other, key_s, -jnp.inf))
        last = jnp.broadcast_to(jnp.max(last, axis=1, keepdims=True), (ROW_TILE, LANES))
        for dev in range(n):
            for j in range(lane_tiles):
                lanes = slice(j * LANES, (j + 1) * LANES)
                key_s = keys_all[dev, :, lanes]
                inside = jnp.logical_and(key_s <= key_r, key_s > last)
                at = slice(dev * rows + j * LANES, dev * rows + (j + 1) * LANES)
                mask[here, at] = jnp.where(inside, 1.0, 0.0).astype(jnp.bfloat16)
        return carry

    lax.fori_loop(0, EARLY_STEPS, build, 0)
    for i in range(WAYS):
        arrived(relay.at[i], hop_recv.at[i])
        hop_on(i).start()
    for dst in near:
        pay_copy(dst, 1).wait()
        fwd_copy(dst, 1).start()
    lax.fori_loop(EARLY_STEPS, n * rows // ROW_TILE, build, 0)

    def sums(dev, i, c):
        return jnp.dot(mask[part_rows(dev, i), :], slab[:, chunk(c)], preferred_element_type=jnp.float32).astype(jnp.bfloat16)

    def blocks(count, pick, c, before, send):
        def step_fn(step, carry):
            k, i = lax.div(step, PARTS), lax.rem(step, PARTS)
            dev = pick(k)
            res[part_rows(dev, i), chunk(c)] = sums(dev, i, c)

            if before is not None:
                @pl.when(step == 0)
                def _():
                    before.start()

            if send is not None:
                @pl.when(jnp.logical_and(i == 0, step > 0))
                def _():
                    send(k - 1).start()

            return carry

        lax.fori_loop(0, count * PARTS, step_fn, 0)

    def own_block(c, before):
        def step_fn(i, carry):
            out_ref[part_rows(0, i), columns(me, c)] = sums(me, i, c)

            if before is not None:
                @pl.when(i == 0)
                def _():
                    before.start()

            return carry

        lax.fori_loop(0, PARTS, step_fn, 0)

    def far_dev(k):
        return peer(2, k)

    def near_a(k):
        return peer(way(k), 0)

    def near_b(k):
        return peer(way(k), 1)

    def chip_dev(k):
        return peer(0, 1)

    own_copies[2].wait()
    for src in near:
        arrived(slab.at[dev_rows(src), chunk(0)], fwd_recv.at[src, 0])
    for src in far:
        arrived(slab.at[dev_rows(src), :], fwd_recv.at[src, 0])
    blocks(WAYS, far_dev, 0, None, lambda k: back_out(k, 0))
    blocks(WAYS, near_a, 0, back_out(WAYS - 1, 0), lambda k: ret_copy(near_a(k), 0))
    blocks(WAYS, near_b, 0, ret_copy(near_a(WAYS - 1), 0), None)
    blocks(1, chip_dev, 0, None, None)
    own_block(0, None)
    own_copies[3].wait()
    for src in near:
        arrived(slab.at[dev_rows(src), chunk(1)], fwd_recv.at[src, 1])
    blocks(WAYS, near_a, 1, None, lambda k: ret_copy(near_a(k), 1))
    blocks(WAYS, far_dev, 1, ret_copy(near_a(WAYS - 1), 1), lambda k: back_out(k, 1))
    blocks(WAYS, near_b, 1, back_out(WAYS - 1, 1), lambda k: ret_whole(near_b(k)))
    blocks(1, chip_dev, 1, ret_whole(near_b(WAYS - 1)), None)
    own_block(1, ret_whole(peer(0, 1)))

    for i in range(WAYS):
        arrived(relay_back.at[i], back_recv.at[i])
        back_on(i).start()

    for dst in far + near:
        key_copy(dst).wait_send()
        seg_copy(dst).wait_send()
    for c in range(CHUNKS):
        for dst in near:
            fwd_copy(dst, c).wait_send()
    for i in range(WAYS):
        hop_out(i).wait_send()
        hop_on(i).wait_send()
        for c in range(CHUNKS):
            back_out(i, c).wait_send()
            ret_copy(near_a(i), c).wait_send()
        ret_whole(near_b(i)).wait_send()
    ret_whole(peer(0, 1)).wait_send()
    for src in near + far:
        arrived(out_ref.at[:, block_cols(src)], ret_recv.at[src])
    for i in range(WAYS):
        back_on(i).wait_send()


def solution(mesh):
    n = mesh.shape['group']

    def per_device(sort_keys, seg_ids, payload):
        rows, width = payload.shape
        total = n * rows
        dma = pltpu.SemaphoreType.DMA
        block = width // n
        return pl.pallas_call(
            functools.partial(exchange_kernel, n),
            out_shape=pltpu.VMEM((rows, width), jnp.bfloat16),
            in_specs=[pl.BlockSpec(memory_space=pl.ANY)] * 3,
            out_specs=pl.BlockSpec(memory_space=pltpu.VMEM),
            scratch_shapes=[
                pltpu.VMEM((n, 1, rows), jnp.float32),
                pltpu.VMEM((n, 1, rows), jnp.int32),
                pltpu.VMEM((total, LANES), jnp.float32),
                pltpu.VMEM((total, LANES), jnp.int32),
                pltpu.VMEM((total, total), jnp.bfloat16),
                pltpu.VMEM((rows, width), jnp.bfloat16),
                pltpu.VMEM((total, block), jnp.bfloat16),
                pltpu.VMEM((total, block), jnp.bfloat16),
                pltpu.VMEM((WAYS, rows, block), jnp.bfloat16),
                pltpu.VMEM((WAYS, rows, block), jnp.bfloat16),
                pltpu.SemaphoreType.REGULAR, dma((n, CHUNKS)), dma((n,)), dma((n,)), dma((n,)), dma((n,)),
                dma((n, CHUNKS)), dma((n, CHUNKS)), dma((WAYS,)), dma((WAYS,)), dma((WAYS,)),
                dma((n, CHUNKS)), dma((n,)), dma((WAYS, CHUNKS)), dma((WAYS,)), dma((WAYS,)),
            ],
            compiler_params=pltpu.CompilerParams(collective_id=0, has_side_effects=True,
                                                 vmem_limit_bytes=56 * 1024 * 1024),
            name='exchange_sums',
        )(sort_keys.reshape(1, 1, rows), seg_ids.reshape(1, 1, rows), payload)

    row_spec = P(('batch', 'group'))
    mat_spec = P(('batch', 'group'), None)
    return jax.shard_map(per_device, mesh=mesh, in_specs=(row_spec, row_spec, mat_spec),
                         out_specs=mat_spec, check_vma=False)
```

```python
import functools

import jax
import jax.numpy as jnp
from jax import lax
from jax.experimental import pallas as pl
from jax.experimental.pallas import tpu as pltpu
from jax.sharding import PartitionSpec as P

MESH = pl.DeviceIdType.MESH
LANES = 128
CORES = 2
WAYS = 2
CHUNKS = 2
ROW_TILE = 64
EARLY_STEPS = 38
PARTS = 2


def exchange_kernel(n, keys_ref, segs_ref, pay_ref, out_ref, keys_all, segs_all, kcol, scol, mask, pay, slab, res,
                    far_ok, pay_sem, key_send, key_recv, seg_send, seg_recv, fwd_send, fwd_recv,
                    ret_send, ret_recv):
    me = lax.axis_index('group')
    rows, width = pay_ref.shape
    block = width // n
    cw = block // CHUNKS
    part = rows // PARTS
    lane_tiles = rows // LANES
    ring = n // CORES
    chip, core = lax.div(me, CORES), lax.rem(me, CORES)

    def peer(hop, flip):
        return lax.rem(chip + hop, ring) * CORES + lax.rem(core + flip, CORES)

    def way(i):
        return 1 + (ring - 2) * i

    near = [peer(way(i), flip) for flip in range(CORES) for i in range(WAYS)] + [peer(0, 1)]
    far = [peer(2, flip) for flip in range(CORES)]

    def remote(src, dst, send_sem, recv_sem, dev):
        return pltpu.make_async_remote_copy(src_ref=src, dst_ref=dst, send_sem=send_sem, recv_sem=recv_sem,
                                            device_id={'group': dev}, device_id_type=MESH)

    def columns(dev, c):
        return pl.ds(pl.multiple_of(dev * block + c * cw, LANES), cw)

    def dev_rows(dev):
        return pl.ds(pl.multiple_of(dev * rows, rows), rows)

    def part_rows(dev, i):
        return pl.ds(pl.multiple_of(dev * rows + i * part, part), part)

    def key_copy(dst):
        return remote(keys_ref.at[0], keys_all.at[me], key_send.at[dst], key_recv.at[me], dst)

    def seg_copy(dst):
        return remote(segs_ref.at[0], segs_all.at[me], seg_send.at[dst], seg_recv.at[me], dst)

    def pay_copy(dst, c):
        return pltpu.make_async_copy(pay_ref.at[:, columns(dst, c)], pay.at[:, columns(dst, c)], pay_sem.at[dst, c])

    def fwd_copy(dst, c):
        return remote(pay.at[:, columns(dst, c)], slab.at[c, dev_rows(me), :], fwd_send.at[dst, c], fwd_recv.at[me, c], dst)

    def ret_copy(dst, c):
        return remote(res.at[c, dev_rows(dst), :], out_ref.at[:, columns(me, c)], ret_send.at[dst, c], ret_recv.at[me, c], dst)

    def arrived(dst, sem):
        pltpu.make_async_copy(dst, dst, sem).wait()

    own_copies = [pltpu.make_async_copy(keys_ref.at[0], keys_all.at[me], key_recv.at[me]),
                  pltpu.make_async_copy(segs_ref.at[0], segs_all.at[me], seg_recv.at[me])]
    own_copies += [pltpu.make_async_copy(pay_ref.at[:, columns(me, c)], slab.at[c, dev_rows(me), :], fwd_recv.at[me, c])
                   for c in range(CHUNKS)]

    barrier = pltpu.get_barrier_semaphore()
    for dst in near:
        pl.semaphore_signal(barrier, inc=1, device_id={'group': dst}, device_id_type=MESH)
    for dst in near + far:
        pay_copy(dst, 0).start()
    pl.semaphore_wait(barrier, len(near))
    pl.semaphore_signal(far_ok, inc=1, device_id={'group': peer(way(1), 0)}, device_id_type=MESH)

    for dst in near:
        key_copy(dst).start()
        seg_copy(dst).start()
    for dst in near:
        pay_copy(dst, 0).wait()
        fwd_copy(dst, 0).start()
    pl.semaphore_wait(far_ok, 1)
    for dst in far:
        key_copy(dst).start()
        seg_copy(dst).start()
    for dst in far:
        pay_copy(dst, 0).wait()
        fwd_copy(dst, 0).start()
    for copy in own_copies:
        copy.start()
    for dst in far + near:
        pay_copy(dst, 1).start()

    own_copies[0].wait()
    own_copies[1].wait()
    for src in far + near:
        arrived(keys_all.at[src], key_recv.at[src])
        arrived(segs_all.at[src], seg_recv.at[src])

    def spread(dev, carry):
        for j in range(lane_tiles):
            lanes = slice(j * LANES, (j + 1) * LANES)
            dst = pl.ds(pl.multiple_of(dev * rows + j * LANES, LANES), LANES)
            kcol[dst, :] = jnp.broadcast_to(keys_all[dev, :, lanes], (LANES, LANES)).T
            scol[dst, :] = jnp.broadcast_to(segs_all[dev, :, lanes], (LANES, LANES)).T
        return carry

    lax.fori_loop(0, n, spread, 0)

    def build(t, carry):
        here = pl.ds(pl.multiple_of(t * ROW_TILE, ROW_TILE), ROW_TILE)
        key_r, seg_r = kcol[here, :], scol[here, :]
        last = jnp.full((ROW_TILE, LANES), -jnp.inf, jnp.float32)
        for dev in range(n):
            for j in range(lane_tiles):
                lanes = slice(j * LANES, (j + 1) * LANES)
                key_s, seg_s = keys_all[dev, :, lanes], segs_all[dev, :, lanes]
                other = jnp.logical_and(key_s < key_r, seg_s != seg_r)
                last = jnp.maximum(last, jnp.where(other, key_s, -jnp.inf))
        last = jnp.broadcast_to(jnp.max(last, axis=1, keepdims=True), (ROW_TILE, LANES))
        for dev in range(n):
            for j in range(lane_tiles):
                lanes = slice(j * LANES, (j + 1) * LANES)
                key_s = keys_all[dev, :, lanes]
                inside = jnp.logical_and(key_s <= key_r, key_s > last)
                at = slice(dev * rows + j * LANES, dev * rows + (j + 1) * LANES)
                mask[here, at] = jnp.where(inside, 1.0, 0.0).astype(jnp.bfloat16)
        return carry

    steps = n * rows // ROW_TILE
    for c in range(CHUNKS):
        lax.fori_loop(EARLY_STEPS * c, EARLY_STEPS * (c + 1) if c < CHUNKS - 1 else steps, build, 0)
        if c + 1 < CHUNKS:
            for dst in far + near:
                pay_copy(dst, c + 1).wait()
                fwd_copy(dst, c + 1).start()

    def sums(dev, i, c):
        return jnp.dot(mask[part_rows(dev, i), :], slab[c], preferred_element_type=jnp.float32).astype(jnp.bfloat16)

    def near_pick(k):
        return peer(way(lax.rem(k, WAYS)), lax.div(k, WAYS))

    for c in range(CHUNKS):
        own_copies[2 + c].wait()
        for src in near + far:
            arrived(slab.at[c, dev_rows(src), :], fwd_recv.at[src, c])

        def block_step(pick, before, send, c=c):
            def step_fn(step, carry):
                k, i = lax.div(step, PARTS), lax.rem(step, PARTS)
                dev = pick(k)
                res[c, part_rows(dev, i), :] = sums(dev, i, c)

                if before is not None:
                    @pl.when(step == 0)
                    def _():
                        before.start()

                @pl.when(jnp.logical_and(i == 0, step > 0))
                def _():
                    send(k - 1).start()

                return carry
            return step_fn

        lax.fori_loop(0, WAYS * PARTS, block_step(lambda k: peer(2, k), None, lambda k: ret_copy(peer(2, k), c)), 0)
        lax.fori_loop(0, WAYS * CORES * PARTS,
                      block_step(near_pick, ret_copy(far[-1], c), lambda k: ret_copy(near_pick(k), c)), 0)
        lax.fori_loop(0, PARTS, block_step(lambda k: peer(0, 1), ret_copy(near[-2], c), lambda k: ret_copy(near[-1], c)), 0)

        def own_step(i, carry, c=c):
            out_ref[part_rows(0, i), columns(me, c)] = sums(me, i, c)

            @pl.when(i == 0)
            def _():
                ret_copy(near[-1], c).start()

            return carry

        lax.fori_loop(0, PARTS, own_step, 0)

    for dst in far + near:
        key_copy(dst).wait_send()
        seg_copy(dst).wait_send()
    for c in range(CHUNKS):
        for dst in near + far:
            fwd_copy(dst, c).wait_send()
            ret_copy(dst, c).wait_send()
        for src in near + far:
            arrived(out_ref.at[:, columns(src, c)], ret_recv.at[src, c])


def solution(mesh):
    n = mesh.shape['group']

    def per_device(sort_keys, seg_ids, payload):
        rows, width = payload.shape
        total = n * rows
        cw = width // n // CHUNKS
        dma = pltpu.SemaphoreType.DMA
        return pl.pallas_call(
            functools.partial(exchange_kernel, n),
            out_shape=pltpu.VMEM((rows, width), jnp.bfloat16),
            in_specs=[pl.BlockSpec(memory_space=pl.ANY)] * 3,
            out_specs=pl.BlockSpec(memory_space=pltpu.VMEM),
            scratch_shapes=[
                pltpu.VMEM((n, 1, rows), jnp.float32),
                pltpu.VMEM((n, 1, rows), jnp.int32),
                pltpu.VMEM((total, LANES), jnp.float32),
                pltpu.VMEM((total, LANES), jnp.int32),
                pltpu.VMEM((total, total), jnp.bfloat16),
                pltpu.VMEM((rows, width), jnp.bfloat16),
                pltpu.VMEM((CHUNKS, total, cw), jnp.bfloat16),
                pltpu.VMEM((CHUNKS, total, cw), jnp.bfloat16),
                pltpu.SemaphoreType.REGULAR, dma((n, CHUNKS)), dma((n,)), dma((n,)), dma((n,)), dma((n,)),
                dma((n, CHUNKS)), dma((n, CHUNKS)),
                dma((n, CHUNKS)), dma((n, CHUNKS)),
            ],
            compiler_params=pltpu.CompilerParams(collective_id=0, has_side_effects=True,
                                                 vmem_limit_bytes=56 * 1024 * 1024),
            name='exchange_sums',
        )(sort_keys.reshape(1, 1, rows), seg_ids.reshape(1, 1, rows), payload)

    row_spec = P(('batch', 'group'))
    mat_spec = P(('batch', 'group'), None)
    return jax.shard_map(per_device, mesh=mesh, in_specs=(row_spec, row_spec, mat_spec),
                         out_specs=mat_spec, check_vma=False)
```

```python
import functools

import jax
import jax.numpy as jnp
from jax import lax
from jax.experimental import pallas as pl
from jax.experimental.pallas import tpu as pltpu
from jax.sharding import PartitionSpec as P

MESH = pl.DeviceIdType.MESH
LANES = 128
CORES = 2
WAYS = 2
CHUNKS = 2
ROW_TILE = 64
EARLY_STEPS = 8
PARTS = 2


def exchange_kernel(n, keys_ref, segs_ref, pay_ref, out_ref, keys_all, segs_all, kcol, scol, mask, pay, slab, res,
                    relay, relay_back, far_ok, pay_sem, key_send, key_recv, seg_send, seg_recv, fwd_send, fwd_recv,
                    hop_send, hop_recv, on_send, ret_send, ret_recv, back_send, back_recv, back_on_send):
    me = lax.axis_index('group')
    rows, width = pay_ref.shape
    block = width // n
    cw = block // CHUNKS
    part = rows // PARTS
    lane_tiles = rows // LANES
    ring = n // CORES
    chip, core = lax.div(me, CORES), lax.rem(me, CORES)

    def peer(hop, flip):
        return lax.rem(chip + hop, ring) * CORES + lax.rem(core + flip, CORES)

    def way(i):
        return 1 + (ring - 2) * i

    near = [peer(way(i), flip) for flip in range(CORES) for i in range(WAYS)] + [peer(0, 1)]
    far = [peer(2, flip) for flip in range(CORES)]

    def remote(src, dst, send_sem, recv_sem, dev):
        return pltpu.make_async_remote_copy(src_ref=src, dst_ref=dst, send_sem=send_sem, recv_sem=recv_sem,
                                            device_id={'group': dev}, device_id_type=MESH)

    def columns(dev, c):
        return pl.ds(pl.multiple_of(dev * block + c * cw, LANES), cw)

    def dev_rows(dev):
        return pl.ds(pl.multiple_of(dev * rows, rows), rows)

    def part_rows(dev, i):
        return pl.ds(pl.multiple_of(dev * rows + i * part, part), part)

    def key_copy(dst):
        return remote(keys_ref.at[0], keys_all.at[me], key_send.at[dst], key_recv.at[me], dst)

    def seg_copy(dst):
        return remote(segs_ref.at[0], segs_all.at[me], seg_send.at[dst], seg_recv.at[me], dst)

    def pay_copy(dst, c):
        return pltpu.make_async_copy(pay_ref.at[:, columns(dst, c)], pay.at[:, columns(dst, c)], pay_sem.at[dst, c])

    def fwd_copy(dst, c):
        return remote(pay.at[:, columns(dst, c)], slab.at[c, dev_rows(me), :], fwd_send.at[dst, c], fwd_recv.at[me, c], dst)

    def hop_out(i, c):
        return remote(pay.at[:, columns(peer(2, i), c)], relay.at[i, c], hop_send.at[i, c], hop_recv.at[i, c], peer(way(i), 0))

    def hop_on(i, c):
        origin = peer(way(1 - i), 0)
        return remote(relay.at[i, c], slab.at[c, dev_rows(origin), :], on_send.at[i, c], fwd_recv.at[origin, c], peer(way(i), i))

    def ret_copy(dst, c):
        return remote(res.at[c, dev_rows(dst), :], out_ref.at[:, columns(me, c)], ret_send.at[dst, c], ret_recv.at[me, c], dst)

    def back_out(i, c):
        return remote(res.at[c, dev_rows(peer(2, i)), :], relay_back.at[i, c], back_send.at[i, c], back_recv.at[i, c],
                      peer(way(i), 0))

    def back_on(i, c):
        origin = peer(way(1 - i), 0)
        return remote(relay_back.at[i, c], out_ref.at[:, columns(origin, c)], back_on_send.at[i, c], ret_recv.at[origin, c],
                      peer(way(i), i))

    def arrived(dst, sem):
        pltpu.make_async_copy(dst, dst, sem).wait()

    own_copies = [pltpu.make_async_copy(keys_ref.at[0], keys_all.at[me], key_recv.at[me]),
                  pltpu.make_async_copy(segs_ref.at[0], segs_all.at[me], seg_recv.at[me])]
    own_copies += [pltpu.make_async_copy(pay_ref.at[:, columns(me, c)], slab.at[c, dev_rows(me), :], fwd_recv.at[me, c])
                   for c in range(CHUNKS)]

    barrier = pltpu.get_barrier_semaphore()
    for dst in near:
        pl.semaphore_signal(barrier, inc=1, device_id={'group': dst}, device_id_type=MESH)
    for dst in far + near:
        pay_copy(dst, 0).start()
    pl.semaphore_wait(barrier, len(near))
    pl.semaphore_signal(far_ok, inc=1, device_id={'group': peer(way(1), 0)}, device_id_type=MESH)

    for dst in near:
        key_copy(dst).start()
        seg_copy(dst).start()
    for i in range(WAYS):
        pay_copy(far[i], 0).wait()
        hop_out(i, 0).start()
    pl.semaphore_wait(far_ok, 1)
    for dst in far:
        key_copy(dst).start()
        seg_copy(dst).start()
    for dst in near:
        pay_copy(dst, 0).wait()
        fwd_copy(dst, 0).start()
    for copy in own_copies:
        copy.start()
    for dst in far + near:
        pay_copy(dst, 1).start()

    own_copies[0].wait()
    own_copies[1].wait()
    for src in far + near:
        arrived(keys_all.at[src], key_recv.at[src])
        arrived(segs_all.at[src], seg_recv.at[src])

    def spread(dev, carry):
        for j in range(lane_tiles):
            lanes = slice(j * LANES, (j + 1) * LANES)
            dst = pl.ds(pl.multiple_of(dev * rows + j * LANES, LANES), LANES)
            kcol[dst, :] = jnp.broadcast_to(keys_all[dev, :, lanes], (LANES, LANES)).T
            scol[dst, :] = jnp.broadcast_to(segs_all[dev, :, lanes], (LANES, LANES)).T
        return carry

    lax.fori_loop(0, n, spread, 0)

    def build(t, carry):
        here = pl.ds(pl.multiple_of(t * ROW_TILE, ROW_TILE), ROW_TILE)
        key_r, seg_r = kcol[here, :], scol[here, :]
        last = jnp.full((ROW_TILE, LANES), -jnp.inf, jnp.float32)
        for dev in range(n):
            for j in range(lane_tiles):
                lanes = slice(j * LANES, (j + 1) * LANES)
                key_s, seg_s = keys_all[dev, :, lanes], segs_all[dev, :, lanes]
                other = jnp.logical_and(key_s < key_r, seg_s != seg_r)
                last = jnp.maximum(last, jnp.where(other, key_s, -jnp.inf))
        last = jnp.broadcast_to(jnp.max(last, axis=1, keepdims=True), (ROW_TILE, LANES))
        for dev in range(n):
            for j in range(lane_tiles):
                lanes = slice(j * LANES, (j + 1) * LANES)
                key_s = keys_all[dev, :, lanes]
                inside = jnp.logical_and(key_s <= key_r, key_s > last)
                at = slice(dev * rows + j * LANES, dev * rows + (j + 1) * LANES)
                mask[here, at] = jnp.where(inside, 1.0, 0.0).astype(jnp.bfloat16)
        return carry

    steps = n * rows // ROW_TILE
    for c in range(CHUNKS):
        lax.fori_loop(EARLY_STEPS * c, EARLY_STEPS * (c + 1) if c < CHUNKS - 1 else steps, build, 0)
        for i in range(WAYS):
            arrived(relay.at[i, c], hop_recv.at[i, c])
            hop_on(i, c).start()
        if c + 1 < CHUNKS:
            for dst in far + near:
                pay_copy(dst, c + 1).wait()
            for i in range(WAYS):
                hop_out(i, c + 1).start()
            for dst in near:
                fwd_copy(dst, c + 1).start()

    def sums(dev, i, c):
        return jnp.dot(mask[part_rows(dev, i), :], slab[c], preferred_element_type=jnp.float32).astype(jnp.bfloat16)

    def near_pick(k):
        return peer(way(lax.rem(k, WAYS)), lax.div(k, WAYS))

    for c in range(CHUNKS):
        own_copies[2 + c].wait()
        for src in near + far:
            arrived(slab.at[c, dev_rows(src), :], fwd_recv.at[src, c])

        def block_step(pick, before, send, c=c):
            def step_fn(step, carry):
                k, i = lax.div(step, PARTS), lax.rem(step, PARTS)
                dev = pick(k)
                res[c, part_rows(dev, i), :] = sums(dev, i, c)

                if before is not None:
                    @pl.when(step == 0)
                    def _():
                        before.start()

                @pl.when(jnp.logical_and(i == 0, step > 0))
                def _():
                    send(k - 1).start()

                return carry
            return step_fn

        lax.fori_loop(0, WAYS * PARTS, block_step(lambda k: peer(2, k), None, lambda k: back_out(k, c)), 0)
        lax.fori_loop(0, WAYS * CORES * PARTS,
                      block_step(near_pick, back_out(WAYS - 1, c), lambda k: ret_copy(near_pick(k), c)), 0)
        lax.fori_loop(0, PARTS, block_step(lambda k: peer(0, 1), ret_copy(near[-2], c), lambda k: ret_copy(near[-1], c)), 0)

        def own_step(i, carry, c=c):
            out_ref[part_rows(0, i), columns(me, c)] = sums(me, i, c)

            @pl.when(i == 0)
            def _():
                ret_copy(near[-1], c).start()

            return carry

        lax.fori_loop(0, PARTS, own_step, 0)

    for c in range(CHUNKS):
        for i in range(WAYS):
            arrived(relay_back.at[i, c], back_recv.at[i, c])
            back_on(i, c).start()

    for dst in far + near:
        key_copy(dst).wait_send()
        seg_copy(dst).wait_send()
    for c in range(CHUNKS):
        for dst in near:
            fwd_copy(dst, c).wait_send()
            ret_copy(dst, c).wait_send()
        for i in range(WAYS):
            hop_out(i, c).wait_send()
            hop_on(i, c).wait_send()
            back_out(i, c).wait_send()
        for src in near + far:
            arrived(out_ref.at[:, columns(src, c)], ret_recv.at[src, c])
    for c in range(CHUNKS):
        for i in range(WAYS):
            back_on(i, c).wait_send()


def solution(mesh):
    n = mesh.shape['group']

    def per_device(sort_keys, seg_ids, payload):
        rows, width = payload.shape
        total = n * rows
        cw = width // n // CHUNKS
        dma = pltpu.SemaphoreType.DMA
        hops = (WAYS, CHUNKS)
        return pl.pallas_call(
            functools.partial(exchange_kernel, n),
            out_shape=pltpu.VMEM((rows, width), jnp.bfloat16),
            in_specs=[pl.BlockSpec(memory_space=pl.ANY)] * 3,
            out_specs=pl.BlockSpec(memory_space=pltpu.VMEM),
            scratch_shapes=[
                pltpu.VMEM((n, 1, rows), jnp.float32),
                pltpu.VMEM((n, 1, rows), jnp.int32),
                pltpu.VMEM((total, LANES), jnp.float32),
                pltpu.VMEM((total, LANES), jnp.int32),
                pltpu.VMEM((total, total), jnp.bfloat16),
                pltpu.VMEM((rows, width), jnp.bfloat16),
                pltpu.VMEM((CHUNKS, total, cw), jnp.bfloat16),
                pltpu.VMEM((CHUNKS, total, cw), jnp.bfloat16),
                pltpu.VMEM((*hops, rows, cw), jnp.bfloat16),
                pltpu.VMEM((*hops, rows, cw), jnp.bfloat16),
                pltpu.SemaphoreType.REGULAR, dma((n, CHUNKS)), dma((n,)), dma((n,)), dma((n,)), dma((n,)),
                dma((n, CHUNKS)), dma((n, CHUNKS)),
                dma(hops), dma(hops), dma(hops),
                dma((n, CHUNKS)), dma((n, CHUNKS)), dma(hops), dma(hops), dma(hops),
            ],
            compiler_params=pltpu.CompilerParams(collective_id=0, has_side_effects=True,
                                                 vmem_limit_bytes=56 * 1024 * 1024),
            name='exchange_sums',
        )(sort_keys.reshape(1, 1, rows), seg_ids.reshape(1, 1, rows), payload)

    row_spec = P(('batch', 'group'))
    mat_spec = P(('batch', 'group'), None)
    return jax.shard_map(per_device, mesh=mesh, in_specs=(row_spec, row_spec, mat_spec),
                         out_specs=mat_spec, check_vma=False)
```

```python
import functools

import jax
import jax.numpy as jnp
from jax import lax
from jax.experimental import pallas as pl
from jax.experimental.pallas import tpu as pltpu
from jax.sharding import PartitionSpec as P

MESH = pl.DeviceIdType.MESH
LANES = 128
CORES = 2
WAYS = 2
CHUNKS = 2
ROW_TILE = 64
EARLY_STEPS = 8
PARTS = 2


def exchange_kernel(n, keys_ref, segs_ref, pay_ref, out_ref, keys_all, segs_all, kcol, scol, mask, pay, slab, res,
                    relay, relay_back, far_ok, pay_sem, key_send, key_recv, seg_send, seg_recv, fwd_send, fwd_recv,
                    hop_send, hop_recv, on_send, ret_send, ret_recv, back_send, back_recv, back_on_send):
    me = lax.axis_index('group')
    rows, width = pay_ref.shape
    block = width // n
    cw = block // CHUNKS
    part = rows // PARTS
    lane_tiles = rows // LANES
    ring = n // CORES
    chip, core = lax.div(me, CORES), lax.rem(me, CORES)

    def peer(hop, flip):
        return lax.rem(chip + hop, ring) * CORES + lax.rem(core + flip, CORES)

    def way(i):
        return 1 + (ring - 2) * i

    near = [peer(way(i), flip) for flip in range(CORES) for i in range(WAYS)] + [peer(0, 1)]
    far = [peer(2, flip) for flip in range(CORES)]

    def remote(src, dst, send_sem, recv_sem, dev):
        return pltpu.make_async_remote_copy(src_ref=src, dst_ref=dst, send_sem=send_sem, recv_sem=recv_sem,
                                            device_id={'group': dev}, device_id_type=MESH)

    def columns(dev, c):
        return pl.ds(pl.multiple_of(dev * block + c * cw, LANES), cw)

    def block_cols(dev):
        return pl.ds(pl.multiple_of(dev * block, LANES), block)

    def chunk(c):
        return pl.ds(c * cw, cw)

    def dev_rows(dev):
        return pl.ds(pl.multiple_of(dev * rows, rows), rows)

    def part_rows(dev, i):
        return pl.ds(pl.multiple_of(dev * rows + i * part, part), part)

    def key_copy(dst):
        return remote(keys_ref.at[0], keys_all.at[me], key_send.at[dst], key_recv.at[me], dst)

    def seg_copy(dst):
        return remote(segs_ref.at[0], segs_all.at[me], seg_send.at[dst], seg_recv.at[me], dst)

    def pay_copy(dst, c):
        return pltpu.make_async_copy(pay_ref.at[:, columns(dst, c)], pay.at[:, columns(dst, c)], pay_sem.at[dst, c])

    def fwd_copy(dst, c):
        return remote(pay.at[:, columns(dst, c)], slab.at[dev_rows(me), chunk(c)], fwd_send.at[dst, c], fwd_recv.at[me, c], dst)

    def hop_out(i):
        return remote(pay.at[:, block_cols(peer(2, i))], relay.at[i], hop_send.at[i], hop_recv.at[i], peer(way(i), 0))

    def hop_on(i):
        origin = peer(way(1 - i), 0)
        return remote(relay.at[i], slab.at[dev_rows(origin), :], on_send.at[i], fwd_recv.at[origin, 0], peer(way(i), i))

    def ret_copy(dst, c):
        return remote(res.at[dev_rows(dst), chunk(c)], out_ref.at[:, columns(me, c)], ret_send.at[dst, c], ret_recv.at[me], dst)

    def ret_whole(dst):
        return remote(res.at[dev_rows(dst), :], out_ref.at[:, block_cols(me)], ret_send.at[dst, 0], ret_recv.at[me], dst)

    def back_out(i, c):
        return remote(res.at[dev_rows(peer(2, i)), chunk(c)], relay_back.at[i, :, chunk(c)], back_send.at[i, c],
                      back_recv.at[i], peer(way(i), 0))

    def back_on(i):
        origin = peer(way(1 - i), 0)
        return remote(relay_back.at[i], out_ref.at[:, block_cols(origin)], back_on_send.at[i], ret_recv.at[origin],
                      peer(way(i), i))

    def arrived(dst, sem):
        pltpu.make_async_copy(dst, dst, sem).wait()

    own_copies = [pltpu.make_async_copy(keys_ref.at[0], keys_all.at[me], key_recv.at[me]),
                  pltpu.make_async_copy(segs_ref.at[0], segs_all.at[me], seg_recv.at[me])]
    own_copies += [pltpu.make_async_copy(pay_ref.at[:, columns(me, c)], slab.at[dev_rows(me), chunk(c)], fwd_recv.at[me, c])
                   for c in range(CHUNKS)]

    barrier = pltpu.get_barrier_semaphore()
    for dst in near:
        pl.semaphore_signal(barrier, inc=1, device_id={'group': dst}, device_id_type=MESH)
    for dst in far:
        for c in range(CHUNKS):
            pay_copy(dst, c).start()
    for dst in near:
        pay_copy(dst, 0).start()
    pl.semaphore_wait(barrier, len(near))
    pl.semaphore_signal(far_ok, inc=1, device_id={'group': peer(way(1), 0)}, device_id_type=MESH)

    for dst in near:
        key_copy(dst).start()
        seg_copy(dst).start()
    for i in range(WAYS):
        for c in range(CHUNKS):
            pay_copy(far[i], c).wait()
        hop_out(i).start()
    pl.semaphore_wait(far_ok, 1)
    for dst in far:
        key_copy(dst).start()
        seg_copy(dst).start()
    for dst in near:
        pay_copy(dst, 0).wait()
        fwd_copy(dst, 0).start()
    for copy in own_copies:
        copy.start()
    for dst in near:
        pay_copy(dst, 1).start()

    own_copies[0].wait()
    own_copies[1].wait()
    for src in far + near:
        arrived(keys_all.at[src], key_recv.at[src])
        arrived(segs_all.at[src], seg_recv.at[src])

    def spread(dev, carry):
        for j in range(lane_tiles):
            lanes = slice(j * LANES, (j + 1) * LANES)
            dst = pl.ds(pl.multiple_of(dev * rows + j * LANES, LANES), LANES)
            kcol[dst, :] = jnp.broadcast_to(keys_all[dev, :, lanes], (LANES, LANES)).T
            scol[dst, :] = jnp.broadcast_to(segs_all[dev, :, lanes], (LANES, LANES)).T
        return carry

    lax.fori_loop(0, n, spread, 0)

    def build(t, carry):
        here = pl.ds(pl.multiple_of(t * ROW_TILE, ROW_TILE), ROW_TILE)
        key_r, seg_r = kcol[here, :], scol[here, :]
        last = jnp.full((ROW_TILE, LANES), -jnp.inf, jnp.float32)
        for dev in range(n):
            for j in range(lane_tiles):
                lanes = slice(j * LANES, (j + 1) * LANES)
                key_s, seg_s = keys_all[dev, :, lanes], segs_all[dev, :, lanes]
                other = jnp.logical_and(key_s < key_r, seg_s != seg_r)
                last = jnp.maximum(last, jnp.where(other, key_s, -jnp.inf))
        last = jnp.broadcast_to(jnp.max(last, axis=1, keepdims=True), (ROW_TILE, LANES))
        for dev in range(n):
            for j in range(lane_tiles):
                lanes = slice(j * LANES, (j + 1) * LANES)
                key_s = keys_all[dev, :, lanes]
                inside = jnp.logical_and(key_s <= key_r, key_s > last)
                at = slice(dev * rows + j * LANES, dev * rows + (j + 1) * LANES)
                mask[here, at] = jnp.where(inside, 1.0, 0.0).astype(jnp.bfloat16)
        return carry

    lax.fori_loop(0, EARLY_STEPS, build, 0)
    for i in range(WAYS):
        arrived(relay.at[i], hop_recv.at[i])
        hop_on(i).start()
    for dst in near:
        pay_copy(dst, 1).wait()
        fwd_copy(dst, 1).start()
    lax.fori_loop(EARLY_STEPS, n * rows // ROW_TILE, build, 0)

    def sums(dev, i, c):
        return jnp.dot(mask[part_rows(dev, i), :], slab[:, chunk(c)], preferred_element_type=jnp.float32).astype(jnp.bfloat16)

    def blocks(count, pick, c, before, send):
        def step_fn(step, carry):
            k, i = lax.div(step, PARTS), lax.rem(step, PARTS)
            dev = pick(k)
            res[part_rows(dev, i), chunk(c)] = sums(dev, i, c)

            if before is not None:
                @pl.when(step == 0)
                def _():
                    before.start()

            if send is not None:
                @pl.when(jnp.logical_and(i == 0, step > 0))
                def _():
                    send(k - 1).start()

            return carry

        lax.fori_loop(0, count * PARTS, step_fn, 0)

    def own_block(c, before):
        def step_fn(i, carry):
            out_ref[part_rows(0, i), columns(me, c)] = sums(me, i, c)

            if before is not None:
                @pl.when(i == 0)
                def _():
                    before.start()

            return carry

        lax.fori_loop(0, PARTS, step_fn, 0)

    def far_dev(k):
        return peer(2, k)

    def near_a(k):
        return peer(way(k), 0)

    def near_b(k):
        return peer(way(k), 1)

    def chip_dev(k):
        return peer(0, 1)

    own_copies[2].wait()
    for src in near:
        arrived(slab.at[dev_rows(src), chunk(0)], fwd_recv.at[src, 0])
    for src in far:
        arrived(slab.at[dev_rows(src), :], fwd_recv.at[src, 0])
    blocks(WAYS, far_dev, 0, None, lambda k: back_out(k, 0))
    blocks(WAYS, near_a, 0, back_out(WAYS - 1, 0), lambda k: ret_copy(near_a(k), 0))
    blocks(WAYS, near_b, 0, ret_copy(near_a(WAYS - 1), 0), None)
    blocks(1, chip_dev, 0, None, None)
    own_block(0, None)
    own_copies[3].wait()
    for src in near:
        arrived(slab.at[dev_rows(src), chunk(1)], fwd_recv.at[src, 1])
    blocks(WAYS, near_a, 1, None, lambda k: ret_copy(near_a(k), 1))
    blocks(WAYS, far_dev, 1, ret_copy(near_a(WAYS - 1), 1), lambda k: back_out(k, 1))
    blocks(WAYS, near_b, 1, back_out(WAYS - 1, 1), lambda k: ret_whole(near_b(k)))
    blocks(1, chip_dev, 1, ret_whole(near_b(WAYS - 1)), None)
    own_block(1, ret_whole(peer(0, 1)))

    for i in range(WAYS):
        arrived(relay_back.at[i], back_recv.at[i])
        back_on(i).start()

    for dst in far + near:
        key_copy(dst).wait_send()
        seg_copy(dst).wait_send()
    for c in range(CHUNKS):
        for dst in near:
            fwd_copy(dst, c).wait_send()
    for i in range(WAYS):
        hop_out(i).wait_send()
        hop_on(i).wait_send()
        for c in range(CHUNKS):
            back_out(i, c).wait_send()
            ret_copy(near_a(i), c).wait_send()
        ret_whole(near_b(i)).wait_send()
    ret_whole(peer(0, 1)).wait_send()
    for src in near + far:
        arrived(out_ref.at[:, block_cols(src)], ret_recv.at[src])
    for i in range(WAYS):
        back_on(i).wait_send()


def solution(mesh):
    n = mesh.shape['group']

    def per_device(sort_keys, seg_ids, payload):
        rows, width = payload.shape
        total = n * rows
        dma = pltpu.SemaphoreType.DMA
        block = width // n
        return pl.pallas_call(
            functools.partial(exchange_kernel, n),
            out_shape=pltpu.VMEM((rows, width), jnp.bfloat16),
            in_specs=[pl.BlockSpec(memory_space=pl.ANY)] * 3,
            out_specs=pl.BlockSpec(memory_space=pltpu.VMEM),
            scratch_shapes=[
                pltpu.VMEM((n, 1, rows), jnp.float32),
                pltpu.VMEM((n, 1, rows), jnp.int32),
                pltpu.VMEM((total, LANES), jnp.float32),
                pltpu.VMEM((total, LANES), jnp.int32),
                pltpu.VMEM((total, total), jnp.bfloat16),
                pltpu.VMEM((rows, width), jnp.bfloat16),
                pltpu.VMEM((total, block), jnp.bfloat16),
                pltpu.VMEM((total, block), jnp.bfloat16),
                pltpu.VMEM((WAYS, rows, block), jnp.bfloat16),
                pltpu.VMEM((WAYS, rows, block), jnp.bfloat16),
                pltpu.SemaphoreType.REGULAR, dma((n, CHUNKS)), dma((n,)), dma((n,)), dma((n,)), dma((n,)),
                dma((n, CHUNKS)), dma((n, CHUNKS)), dma((WAYS,)), dma((WAYS,)), dma((WAYS,)),
                dma((n, CHUNKS)), dma((n,)), dma((WAYS, CHUNKS)), dma((WAYS,)), dma((WAYS,)),
            ],
            compiler_params=pltpu.CompilerParams(collective_id=0, has_side_effects=True,
                                                 vmem_limit_bytes=56 * 1024 * 1024),
            name='exchange_sums',
        )(sort_keys.reshape(1, 1, rows), seg_ids.reshape(1, 1, rows), payload)

    row_spec = P(('batch', 'group'))
    mat_spec = P(('batch', 'group'), None)
    return jax.shard_map(per_device, mesh=mesh, in_specs=(row_spec, row_spec, mat_spec),
                         out_specs=mat_spec, check_vma=False)
```

```python
import functools

import jax
import jax.numpy as jnp
from jax import lax
from jax.experimental import pallas as pl
from jax.experimental.pallas import tpu as pltpu
from jax.sharding import PartitionSpec as P

MESH = pl.DeviceIdType.MESH
LANES = 128
CORES = 2
WAYS = 2
CHUNKS = 2
ROW_TILE = 64
EARLY_STEPS = 8
PARTS = 2


def exchange_kernel(n, keys_ref, segs_ref, pay_ref, out_ref, keys_all, segs_all, kcol, scol, mask, pay, slab, res,
                    relay, relay_back, far_ok, pay_sem, key_send, key_recv, seg_send, seg_recv, fwd_send, fwd_recv,
                    hop_send, hop_recv, on_send, ret_send, ret_recv, back_send, back_recv, back_on_send):
    me = lax.axis_index('group')
    rows, width = pay_ref.shape
    block = width // n
    cw = block // CHUNKS
    part = rows // PARTS
    lane_tiles = rows // LANES
    ring = n // CORES
    chip, core = lax.div(me, CORES), lax.rem(me, CORES)

    def peer(hop, flip):
        return lax.rem(chip + hop, ring) * CORES + lax.rem(core + flip, CORES)

    def way(i):
        return 1 + (ring - 2) * i

    near = [peer(way(i), flip) for flip in range(CORES) for i in range(WAYS)] + [peer(0, 1)]
    far = [peer(2, flip) for flip in range(CORES)]
    same, other = near[:WAYS], near[WAYS:]

    def remote(src, dst, send_sem, recv_sem, dev):
        return pltpu.make_async_remote_copy(src_ref=src, dst_ref=dst, send_sem=send_sem, recv_sem=recv_sem,
                                            device_id={'group': dev}, device_id_type=MESH)

    def columns(dev, c):
        return pl.ds(pl.multiple_of(dev * block + c * cw, LANES), cw)

    def block_cols(dev):
        return pl.ds(pl.multiple_of(dev * block, LANES), block)

    def chunk(c):
        return pl.ds(c * cw, cw)

    def dev_rows(dev):
        return pl.ds(pl.multiple_of(dev * rows, rows), rows)

    def part_rows(dev, i):
        return pl.ds(pl.multiple_of(dev * rows + i * part, part), part)

    def key_copy(dst):
        return remote(keys_ref.at[0], keys_all.at[me], key_send.at[dst], key_recv.at[me], dst)

    def seg_copy(dst):
        return remote(segs_ref.at[0], segs_all.at[me], seg_send.at[dst], seg_recv.at[me], dst)

    def pay_copy(dst, c):
        return pltpu.make_async_copy(pay_ref.at[:, columns(dst, c)], pay.at[:, columns(dst, c)], pay_sem.at[dst, c])

    def fwd_copy(dst, c):
        return remote(pay.at[:, columns(dst, c)], slab.at[dev_rows(me), chunk(c)], fwd_send.at[dst, c], fwd_recv.at[me, c], dst)

    def fwd_whole(dst):
        return remote(pay.at[:, block_cols(dst)], slab.at[dev_rows(me), :], fwd_send.at[dst, 0], fwd_recv.at[me, 0], dst)

    def hop_out(i):
        return remote(pay.at[:, block_cols(peer(2, i))], relay.at[i], hop_send.at[i], hop_recv.at[i], peer(way(i), 0))

    def hop_on(i):
        origin = peer(way(1 - i), 0)
        return remote(relay.at[i], slab.at[dev_rows(origin), :], on_send.at[i], fwd_recv.at[origin, 0], peer(way(i), i))

    def ret_copy(dst, c):
        return remote(res.at[dev_rows(dst), chunk(c)], out_ref.at[:, columns(me, c)], ret_send.at[dst, c], ret_recv.at[me], dst)

    def ret_whole(dst):
        return remote(res.at[dev_rows(dst), :], out_ref.at[:, block_cols(me)], ret_send.at[dst, 0], ret_recv.at[me], dst)

    def back_out(i, c):
        return remote(res.at[dev_rows(peer(2, i)), chunk(c)], relay_back.at[i, :, chunk(c)], back_send.at[i, c],
                      back_recv.at[i], peer(way(i), 0))

    def back_on(i):
        origin = peer(way(1 - i), 0)
        return remote(relay_back.at[i], out_ref.at[:, block_cols(origin)], back_on_send.at[i], ret_recv.at[origin],
                      peer(way(i), i))

    def arrived(dst, sem):
        pltpu.make_async_copy(dst, dst, sem).wait()

    own_copies = [pltpu.make_async_copy(keys_ref.at[0], keys_all.at[me], key_recv.at[me]),
                  pltpu.make_async_copy(segs_ref.at[0], segs_all.at[me], seg_recv.at[me])]
    own_copies += [pltpu.make_async_copy(pay_ref.at[:, columns(me, c)], slab.at[dev_rows(me), chunk(c)], fwd_recv.at[me, c])
                   for c in range(CHUNKS)]

    barrier = pltpu.get_barrier_semaphore()
    for dst in near:
        pl.semaphore_signal(barrier, inc=1, device_id={'group': dst}, device_id_type=MESH)
    for dst in far:
        for c in range(CHUNKS):
            pay_copy(dst, c).start()
    pl.semaphore_wait(barrier, len(near))
    pl.semaphore_signal(far_ok, inc=1, device_id={'group': peer(way(1), 0)}, device_id_type=MESH)

    for dst in near:
        key_copy(dst).start()
        seg_copy(dst).start()
    for i in range(WAYS):
        for c in range(CHUNKS):
            pay_copy(far[i], c).wait()
        hop_out(i).start()
    for dst in same:
        for c in range(CHUNKS):
            pay_copy(dst, c).start()
    for c in range(CHUNKS):
        for dst in other:
            pay_copy(dst, c).start()
    for copy in own_copies:
        copy.start()
    pl.semaphore_wait(far_ok, 1)
    for dst in far:
        key_copy(dst).start()
        seg_copy(dst).start()
    for dst in same:
        for c in range(CHUNKS):
            pay_copy(dst, c).wait()
        fwd_whole(dst).start()
    for dst in other:
        pay_copy(dst, 0).wait()
        fwd_copy(dst, 0).start()

    own_copies[0].wait()
    own_copies[1].wait()
    for src in far + near:
        arrived(keys_all.at[src], key_recv.at[src])
        arrived(segs_all.at[src], seg_recv.at[src])

    def spread(dev, carry):
        for j in range(lane_tiles):
            lanes = slice(j * LANES, (j + 1) * LANES)
            dst = pl.ds(pl.multiple_of(dev * rows + j * LANES, LANES), LANES)
            kcol[dst, :] = jnp.broadcast_to(keys_all[dev, :, lanes], (LANES, LANES)).T
            scol[dst, :] = jnp.broadcast_to(segs_all[dev, :, lanes], (LANES, LANES)).T
        return carry

    lax.fori_loop(0, n, spread, 0)

    def build(t, carry):
        here = pl.ds(pl.multiple_of(t * ROW_TILE, ROW_TILE), ROW_TILE)
        key_r, seg_r = kcol[here, :], scol[here, :]
        last = jnp.full((ROW_TILE, LANES), -jnp.inf, jnp.float32)
        for dev in range(n):
            for j in range(lane_tiles):
                lanes = slice(j * LANES, (j + 1) * LANES)
                key_s, seg_s = keys_all[dev, :, lanes], segs_all[dev, :, lanes]
                other = jnp.logical_and(key_s < key_r, seg_s != seg_r)
                last = jnp.maximum(last, jnp.where(other, key_s, -jnp.inf))
        last = jnp.broadcast_to(jnp.max(last, axis=1, keepdims=True), (ROW_TILE, LANES))
        for dev in range(n):
            for j in range(lane_tiles):
                lanes = slice(j * LANES, (j + 1) * LANES)
                key_s = keys_all[dev, :, lanes]
                inside = jnp.logical_and(key_s <= key_r, key_s > last)
                at = slice(dev * rows + j * LANES, dev * rows + (j + 1) * LANES)
                mask[here, at] = jnp.where(inside, 1.0, 0.0).astype(jnp.bfloat16)
        return carry

    lax.fori_loop(0, EARLY_STEPS, build, 0)
    for i in range(WAYS):
        arrived(relay.at[i], hop_recv.at[i])
        hop_on(i).start()
    for dst in other:
        pay_copy(dst, 1).wait()
        fwd_copy(dst, 1).start()
    lax.fori_loop(EARLY_STEPS, n * rows // ROW_TILE, build, 0)

    def sums(dev, i, c):
        return jnp.dot(mask[part_rows(dev, i), :], slab[:, chunk(c)], preferred_element_type=jnp.float32).astype(jnp.bfloat16)

    def blocks(count, pick, c, before, send):
        def step_fn(step, carry):
            k, i = lax.div(step, PARTS), lax.rem(step, PARTS)
            dev = pick(k)
            res[part_rows(dev, i), chunk(c)] = sums(dev, i, c)

            if before is not None:
                @pl.when(step == 0)
                def _():
                    before.start()

            if send is not None:
                @pl.when(jnp.logical_and(i == 0, step > 0))
                def _():
                    send(k - 1).start()

            return carry

        lax.fori_loop(0, count * PARTS, step_fn, 0)

    def own_block(c, before):
        def step_fn(i, carry):
            out_ref[part_rows(0, i), columns(me, c)] = sums(me, i, c)

            if before is not None:
                @pl.when(i == 0)
                def _():
                    before.start()

            return carry

        lax.fori_loop(0, PARTS, step_fn, 0)

    def far_dev(k):
        return peer(2, k)

    def near_a(k):
        return peer(way(k), 0)

    def near_b(k):
        return peer(way(k), 1)

    def chip_dev(k):
        return peer(0, 1)

    own_copies[2].wait()
    for src in other:
        arrived(slab.at[dev_rows(src), chunk(0)], fwd_recv.at[src, 0])
    for src in same + far:
        arrived(slab.at[dev_rows(src), :], fwd_recv.at[src, 0])
    blocks(WAYS, far_dev, 0, None, lambda k: back_out(k, 0))
    blocks(WAYS, near_a, 0, back_out(WAYS - 1, 0), lambda k: ret_copy(near_a(k), 0))
    blocks(WAYS, near_b, 0, ret_copy(near_a(WAYS - 1), 0), None)
    blocks(1, chip_dev, 0, None, None)
    own_block(0, None)
    own_copies[3].wait()
    for src in other:
        arrived(slab.at[dev_rows(src), chunk(1)], fwd_recv.at[src, 1])
    blocks(WAYS, near_a, 1, None, lambda k: ret_copy(near_a(k), 1))
    blocks(WAYS, far_dev, 1, ret_copy(near_a(WAYS - 1), 1), lambda k: back_out(k, 1))
    blocks(WAYS, near_b, 1, back_out(WAYS - 1, 1), lambda k: ret_whole(near_b(k)))
    blocks(1, chip_dev, 1, ret_whole(near_b(WAYS - 1)), None)
    own_block(1, ret_whole(peer(0, 1)))

    for i in range(WAYS):
        arrived(relay_back.at[i], back_recv.at[i])
        back_on(i).start()

    for dst in far + near:
        key_copy(dst).wait_send()
        seg_copy(dst).wait_send()
    for dst in same:
        fwd_whole(dst).wait_send()
    for dst in other:
        for c in range(CHUNKS):
            fwd_copy(dst, c).wait_send()
    for i in range(WAYS):
        hop_out(i).wait_send()
        hop_on(i).wait_send()
        for c in range(CHUNKS):
            back_out(i, c).wait_send()
            ret_copy(near_a(i), c).wait_send()
        ret_whole(near_b(i)).wait_send()
    ret_whole(peer(0, 1)).wait_send()
    for src in near + far:
        arrived(out_ref.at[:, block_cols(src)], ret_recv.at[src])
    for i in range(WAYS):
        back_on(i).wait_send()


def solution(mesh):
    n = mesh.shape['group']

    def per_device(sort_keys, seg_ids, payload):
        rows, width = payload.shape
        total = n * rows
        dma = pltpu.SemaphoreType.DMA
        block = width // n
        return pl.pallas_call(
            functools.partial(exchange_kernel, n),
            out_shape=pltpu.VMEM((rows, width), jnp.bfloat16),
            in_specs=[pl.BlockSpec(memory_space=pl.ANY)] * 3,
            out_specs=pl.BlockSpec(memory_space=pltpu.VMEM),
            scratch_shapes=[
                pltpu.VMEM((n, 1, rows), jnp.float32),
                pltpu.VMEM((n, 1, rows), jnp.int32),
                pltpu.VMEM((total, LANES), jnp.float32),
                pltpu.VMEM((total, LANES), jnp.int32),
                pltpu.VMEM((total, total), jnp.bfloat16),
                pltpu.VMEM((rows, width), jnp.bfloat16),
                pltpu.VMEM((total, block), jnp.bfloat16),
                pltpu.VMEM((total, block), jnp.bfloat16),
                pltpu.VMEM((WAYS, rows, block), jnp.bfloat16),
                pltpu.VMEM((WAYS, rows, block), jnp.bfloat16),
                pltpu.SemaphoreType.REGULAR, dma((n, CHUNKS)), dma((n,)), dma((n,)), dma((n,)), dma((n,)),
                dma((n, CHUNKS)), dma((n, CHUNKS)), dma((WAYS,)), dma((WAYS,)), dma((WAYS,)),
                dma((n, CHUNKS)), dma((n,)), dma((WAYS, CHUNKS)), dma((WAYS,)), dma((WAYS,)),
            ],
            compiler_params=pltpu.CompilerParams(collective_id=0, has_side_effects=True,
                                                 vmem_limit_bytes=56 * 1024 * 1024),
            name='exchange_sums',
        )(sort_keys.reshape(1, 1, rows), seg_ids.reshape(1, 1, rows), payload)

    row_spec = P(('batch', 'group'))
    mat_spec = P(('batch', 'group'), None)
    return jax.shard_map(per_device, mesh=mesh, in_specs=(row_spec, row_spec, mat_spec),
                         out_specs=mat_spec, check_vma=False)
```

```python
import functools

import jax
import jax.numpy as jnp
from jax import lax
from jax.experimental import pallas as pl
from jax.experimental.pallas import tpu as pltpu
from jax.sharding import PartitionSpec as P

MESH = pl.DeviceIdType.MESH
LANES = 128
CORES = 2
WAYS = 2
CHUNKS = 2
ROW_TILE = 64
EARLY_STEPS = 8
PARTS = 2


def exchange_kernel(n, keys_ref, segs_ref, pay_ref, out_ref, keys_all, segs_all, kcol, scol, mask, pay, slab, res,
                    relay, relay_back, far_ok, pay_sem, key_send, key_recv, seg_send, seg_recv, fwd_send, fwd_recv,
                    hop_send, hop_recv, on_send, ret_send, ret_recv, back_send, back_recv, back_on_send):
    me = lax.axis_index('group')
    rows, width = pay_ref.shape
    block = width // n
    cw = block // CHUNKS
    part = rows // PARTS
    lane_tiles = rows // LANES
    ring = n // CORES
    chip, core = lax.div(me, CORES), lax.rem(me, CORES)

    def peer(hop, flip):
        return lax.rem(chip + hop, ring) * CORES + lax.rem(core + flip, CORES)

    def way(i):
        return 1 + (ring - 2) * i

    near = [peer(way(i), flip) for flip in range(CORES) for i in range(WAYS)] + [peer(0, 1)]
    far = [peer(2, flip) for flip in range(CORES)]

    def remote(src, dst, send_sem, recv_sem, dev):
        return pltpu.make_async_remote_copy(src_ref=src, dst_ref=dst, send_sem=send_sem, recv_sem=recv_sem,
                                            device_id={'group': dev}, device_id_type=MESH)

    def columns(dev, c):
        return pl.ds(pl.multiple_of(dev * block + c * cw, LANES), cw)

    def block_cols(dev):
        return pl.ds(pl.multiple_of(dev * block, LANES), block)

    def chunk(c):
        return pl.ds(c * cw, cw)

    def dev_rows(dev):
        return pl.ds(pl.multiple_of(dev * rows, rows), rows)

    def part_rows(dev, i):
        return pl.ds(pl.multiple_of(dev * rows + i * part, part), part)

    def key_copy(dst):
        return remote(keys_ref.at[0], keys_all.at[me], key_send.at[dst], key_recv.at[me], dst)

    def seg_copy(dst):
        return remote(segs_ref.at[0], segs_all.at[me], seg_send.at[dst], seg_recv.at[me], dst)

    def pay_copy(dst, c):
        return pltpu.make_async_copy(pay_ref.at[:, columns(dst, c)], pay.at[:, columns(dst, c)], pay_sem.at[dst, c])

    def fwd_copy(dst, c):
        return remote(pay.at[:, columns(dst, c)], slab.at[dev_rows(me), chunk(c)], fwd_send.at[dst, c], fwd_recv.at[me, c], dst)

    def hop_out(i):
        return remote(pay.at[:, block_cols(peer(2, i))], relay.at[i], hop_send.at[i], hop_recv.at[i], peer(way(i), 0))

    def hop_on(i):
        origin = peer(way(1 - i), 0)
        return remote(relay.at[i], slab.at[dev_rows(origin), :], on_send.at[i], fwd_recv.at[origin, 0], peer(way(i), i))

    def ret_copy(dst, c):
        return remote(res.at[dev_rows(dst), chunk(c)], out_ref.at[:, columns(me, c)], ret_send.at[dst, c], ret_recv.at[me], dst)

    def ret_whole(dst):
        return remote(res.at[dev_rows(dst), :], out_ref.at[:, block_cols(me)], ret_send.at[dst, 0], ret_recv.at[me], dst)

    def back_out(i, c):
        return remote(res.at[dev_rows(peer(2, i)), chunk(c)], relay_back.at[i, :, chunk(c)], back_send.at[i, c],
                      back_recv.at[i], peer(way(i), 0))

    def back_on(i):
        origin = peer(way(1 - i), 0)
        return remote(relay_back.at[i], out_ref.at[:, block_cols(origin)], back_on_send.at[i], ret_recv.at[origin],
                      peer(way(i), i))

    def arrived(dst, sem):
        pltpu.make_async_copy(dst, dst, sem).wait()

    own_copies = [pltpu.make_async_copy(keys_ref.at[0], keys_all.at[me], key_recv.at[me]),
                  pltpu.make_async_copy(segs_ref.at[0], segs_all.at[me], seg_recv.at[me])]
    own_copies += [pltpu.make_async_copy(pay_ref.at[:, columns(me, c)], slab.at[dev_rows(me), chunk(c)], fwd_recv.at[me, c])
                   for c in range(CHUNKS)]

    barrier = pltpu.get_barrier_semaphore()
    for dst in near:
        pl.semaphore_signal(barrier, inc=1, device_id={'group': dst}, device_id_type=MESH)
    for dst in far:
        for c in range(CHUNKS):
            pay_copy(dst, c).start()
    pl.semaphore_wait(barrier, len(near))
    pl.semaphore_signal(far_ok, inc=1, device_id={'group': peer(way(1), 0)}, device_id_type=MESH)

    for dst in near:
        key_copy(dst).start()
        seg_copy(dst).start()
    for i in range(WAYS):
        for c in range(CHUNKS):
            pay_copy(far[i], c).wait()
        hop_out(i).start()
    for dst in near:
        pay_copy(dst, 0).start()
    pl.semaphore_wait(far_ok, 1)
    for dst in far:
        key_copy(dst).start()
        seg_copy(dst).start()
    for dst in near:
        pay_copy(dst, 0).wait()
        fwd_copy(dst, 0).start()
    for copy in own_copies:
        copy.start()
    for dst in near:
        pay_copy(dst, 1).start()

    own_copies[0].wait()
    own_copies[1].wait()
    for src in far + near:
        arrived(keys_all.at[src], key_recv.at[src])
        arrived(segs_all.at[src], seg_recv.at[src])

    def spread(dev, carry):
        for j in range(lane_tiles):
            lanes = slice(j * LANES, (j + 1) * LANES)
            dst = pl.ds(pl.multiple_of(dev * rows + j * LANES, LANES), LANES)
            kcol[dst, :] = jnp.broadcast_to(keys_all[dev, :, lanes], (LANES, LANES)).T
            scol[dst, :] = jnp.broadcast_to(segs_all[dev, :, lanes], (LANES, LANES)).T
        return carry

    lax.fori_loop(0, n, spread, 0)

    def build(t, carry):
        here = pl.ds(pl.multiple_of(t * ROW_TILE, ROW_TILE), ROW_TILE)
        key_r, seg_r = kcol[here, :], scol[here, :]
        last = jnp.full((ROW_TILE, LANES), -jnp.inf, jnp.float32)
        for dev in range(n):
            for j in range(lane_tiles):
                lanes = slice(j * LANES, (j + 1) * LANES)
                key_s, seg_s = keys_all[dev, :, lanes], segs_all[dev, :, lanes]
                other = jnp.logical_and(key_s < key_r, seg_s != seg_r)
                last = jnp.maximum(last, jnp.where(other, key_s, -jnp.inf))
        last = jnp.broadcast_to(jnp.max(last, axis=1, keepdims=True), (ROW_TILE, LANES))
        for dev in range(n):
            for j in range(lane_tiles):
                lanes = slice(j * LANES, (j + 1) * LANES)
                key_s = keys_all[dev, :, lanes]
                inside = jnp.logical_and(key_s <= key_r, key_s > last)
                at = slice(dev * rows + j * LANES, dev * rows + (j + 1) * LANES)
                mask[here, at] = jnp.where(inside, 1.0, 0.0).astype(jnp.bfloat16)
        return carry

    lax.fori_loop(0, EARLY_STEPS, build, 0)
    for i in range(WAYS):
        arrived(relay.at[i], hop_recv.at[i])
        hop_on(i).start()
    for dst in near:
        pay_copy(dst, 1).wait()
        fwd_copy(dst, 1).start()
    lax.fori_loop(EARLY_STEPS, n * rows // ROW_TILE, build, 0)

    def sums(dev, i, c):
        return jnp.dot(mask[part_rows(dev, i), :], slab[:, chunk(c)], preferred_element_type=jnp.float32).astype(jnp.bfloat16)

    def blocks(count, pick, c, before, send):
        def step_fn(step, carry):
            k, i = lax.div(step, PARTS), lax.rem(step, PARTS)
            dev = pick(k)
            res[part_rows(dev, i), chunk(c)] = sums(dev, i, c)

            if before is not None:
                @pl.when(step == 0)
                def _():
                    before.start()

            if send is not None:
                @pl.when(jnp.logical_and(i == 0, step > 0))
                def _():
                    send(k - 1).start()

            return carry

        lax.fori_loop(0, count * PARTS, step_fn, 0)

    def own_block(c, before):
        def step_fn(i, carry):
            out_ref[part_rows(0, i), columns(me, c)] = sums(me, i, c)

            if before is not None:
                @pl.when(i == 0)
                def _():
                    before.start()

            return carry

        lax.fori_loop(0, PARTS, step_fn, 0)

    def far_dev(k):
        return peer(2, k)

    def near_a(k):
        return peer(way(k), 0)

    def near_b(k):
        return peer(way(k), 1)

    def chip_dev(k):
        return peer(0, 1)

    own_copies[2].wait()
    for src in near:
        arrived(slab.at[dev_rows(src), chunk(0)], fwd_recv.at[src, 0])
    for src in far:
        arrived(slab.at[dev_rows(src), :], fwd_recv.at[src, 0])
    blocks(WAYS, far_dev, 0, None, lambda k: back_out(k, 0))
    blocks(WAYS, near_a, 0, back_out(WAYS - 1, 0), lambda k: ret_copy(near_a(k), 0))
    blocks(WAYS, near_b, 0, ret_copy(near_a(WAYS - 1), 0), None)
    blocks(1, chip_dev, 0, None, None)
    own_block(0, None)
    own_copies[3].wait()
    for src in near:
        arrived(slab.at[dev_rows(src), chunk(1)], fwd_recv.at[src, 1])
    blocks(WAYS, near_a, 1, None, lambda k: ret_copy(near_a(k), 1))
    blocks(WAYS, far_dev, 1, ret_copy(near_a(WAYS - 1), 1), lambda k: back_out(k, 1))
    blocks(WAYS, near_b, 1, back_out(WAYS - 1, 1), lambda k: ret_whole(near_b(k)))
    blocks(1, chip_dev, 1, ret_whole(near_b(WAYS - 1)), None)
    own_block(1, ret_whole(peer(0, 1)))

    for i in range(WAYS):
        arrived(relay_back.at[i], back_recv.at[i])
        back_on(i).start()

    for dst in far + near:
        key_copy(dst).wait_send()
        seg_copy(dst).wait_send()
    for c in range(CHUNKS):
        for dst in near:
            fwd_copy(dst, c).wait_send()
    for i in range(WAYS):
        hop_out(i).wait_send()
        hop_on(i).wait_send()
        for c in range(CHUNKS):
            back_out(i, c).wait_send()
            ret_copy(near_a(i), c).wait_send()
        ret_whole(near_b(i)).wait_send()
    ret_whole(peer(0, 1)).wait_send()
    for src in near + far:
        arrived(out_ref.at[:, block_cols(src)], ret_recv.at[src])
    for i in range(WAYS):
        back_on(i).wait_send()


def solution(mesh):
    n = mesh.shape['group']

    def per_device(sort_keys, seg_ids, payload):
        rows, width = payload.shape
        total = n * rows
        dma = pltpu.SemaphoreType.DMA
        block = width // n
        return pl.pallas_call(
            functools.partial(exchange_kernel, n),
            out_shape=pltpu.VMEM((rows, width), jnp.bfloat16),
            in_specs=[pl.BlockSpec(memory_space=pl.ANY)] * 3,
            out_specs=pl.BlockSpec(memory_space=pltpu.VMEM),
            scratch_shapes=[
                pltpu.VMEM((n, 1, rows), jnp.float32),
                pltpu.VMEM((n, 1, rows), jnp.int32),
                pltpu.VMEM((total, LANES), jnp.float32),
                pltpu.VMEM((total, LANES), jnp.int32),
                pltpu.VMEM((total, total), jnp.bfloat16),
                pltpu.VMEM((rows, width), jnp.bfloat16),
                pltpu.VMEM((total, block), jnp.bfloat16),
                pltpu.VMEM((total, block), jnp.bfloat16),
                pltpu.VMEM((WAYS, rows, block), jnp.bfloat16),
                pltpu.VMEM((WAYS, rows, block), jnp.bfloat16),
                pltpu.SemaphoreType.REGULAR, dma((n, CHUNKS)), dma((n,)), dma((n,)), dma((n,)), dma((n,)),
                dma((n, CHUNKS)), dma((n, CHUNKS)), dma((WAYS,)), dma((WAYS,)), dma((WAYS,)),
                dma((n, CHUNKS)), dma((n,)), dma((WAYS, CHUNKS)), dma((WAYS,)), dma((WAYS,)),
            ],
            compiler_params=pltpu.CompilerParams(collective_id=0, has_side_effects=True,
                                                 vmem_limit_bytes=56 * 1024 * 1024),
            name='exchange_sums',
        )(sort_keys.reshape(1, 1, rows), seg_ids.reshape(1, 1, rows), payload)

    row_spec = P(('batch', 'group'))
    mat_spec = P(('batch', 'group'), None)
    return jax.shard_map(per_device, mesh=mesh, in_specs=(row_spec, row_spec, mat_spec),
                         out_specs=mat_spec, check_vma=False)
```

```python
import functools

import jax
import jax.numpy as jnp
from jax import lax
from jax.experimental import pallas as pl
from jax.experimental.pallas import tpu as pltpu
from jax.sharding import PartitionSpec as P

MESH = pl.DeviceIdType.MESH
LANES = 128
CORES = 2
WAYS = 2
CHUNKS = 2
ROW_TILE = 64
EARLY_STEPS = 8
PARTS = 2


def exchange_kernel(n, keys_ref, segs_ref, pay_ref, out_ref, keys_all, segs_all, kcol, scol, mask, pay, slab, res,
                    relay, relay_back, far_ok, pay_sem, key_send, key_recv, seg_send, seg_recv, fwd_send, fwd_recv,
                    hop_send, hop_recv, on_send, ret_send, ret_recv, back_send, back_recv, back_on_send):
    me = lax.axis_index('group')
    rows, width = pay_ref.shape
    block = width // n
    cw = block // CHUNKS
    part = rows // PARTS
    lane_tiles = rows // LANES
    ring = n // CORES
    chip, core = lax.div(me, CORES), lax.rem(me, CORES)

    def peer(hop, flip):
        return lax.rem(chip + hop, ring) * CORES + lax.rem(core + flip, CORES)

    def way(i):
        return 1 + (ring - 2) * i

    near = [peer(way(i), flip) for flip in range(CORES) for i in range(WAYS)] + [peer(0, 1)]
    far = [peer(2, flip) for flip in range(CORES)]

    def remote(src, dst, send_sem, recv_sem, dev):
        return pltpu.make_async_remote_copy(src_ref=src, dst_ref=dst, send_sem=send_sem, recv_sem=recv_sem,
                                            device_id={'group': dev}, device_id_type=MESH)

    def columns(dev, c):
        return pl.ds(pl.multiple_of(dev * block + c * cw, LANES), cw)

    def block_cols(dev):
        return pl.ds(pl.multiple_of(dev * block, LANES), block)

    def chunk(c):
        return pl.ds(c * cw, cw)

    def dev_rows(dev):
        return pl.ds(pl.multiple_of(dev * rows, rows), rows)

    def part_rows(dev, i):
        return pl.ds(pl.multiple_of(dev * rows + i * part, part), part)

    def key_copy(dst):
        return remote(keys_ref.at[0], keys_all.at[me], key_send.at[dst], key_recv.at[me], dst)

    def seg_copy(dst):
        return remote(segs_ref.at[0], segs_all.at[me], seg_send.at[dst], seg_recv.at[me], dst)

    def pay_copy(dst, c):
        return pltpu.make_async_copy(pay_ref.at[:, columns(dst, c)], pay.at[:, columns(dst, c)], pay_sem.at[dst, c])

    def fwd_copy(dst, c):
        return remote(pay.at[:, columns(dst, c)], slab.at[dev_rows(me), chunk(c)], fwd_send.at[dst, c], fwd_recv.at[me, c], dst)

    def hop_out(i):
        return remote(pay.at[:, block_cols(peer(2, i))], relay.at[i], hop_send.at[i], hop_recv.at[i], peer(way(i), 0))

    def hop_on(i):
        origin = peer(way(1 - i), 0)
        return remote(relay.at[i], slab.at[dev_rows(origin), :], on_send.at[i], fwd_recv.at[origin, 0], peer(way(i), i))

    def ret_copy(dst, c):
        return remote(res.at[dev_rows(dst), chunk(c)], out_ref.at[:, columns(me, c)], ret_send.at[dst, c], ret_recv.at[me], dst)

    def ret_whole(dst):
        return remote(res.at[dev_rows(dst), :], out_ref.at[:, block_cols(me)], ret_send.at[dst, 0], ret_recv.at[me], dst)

    def back_out(i, c):
        return remote(res.at[dev_rows(peer(2, i)), chunk(c)], relay_back.at[i, :, chunk(c)], back_send.at[i, c],
                      back_recv.at[i], peer(way(i), 0))

    def back_on(i):
        origin = peer(way(1 - i), 0)
        return remote(relay_back.at[i], out_ref.at[:, block_cols(origin)], back_on_send.at[i], ret_recv.at[origin],
                      peer(way(i), i))

    def arrived(dst, sem):
        pltpu.make_async_copy(dst, dst, sem).wait()

    own_copies = [pltpu.make_async_copy(keys_ref.at[0], keys_all.at[me], key_recv.at[me]),
                  pltpu.make_async_copy(segs_ref.at[0], segs_all.at[me], seg_recv.at[me])]
    own_copies += [pltpu.make_async_copy(pay_ref.at[:, columns(me, c)], slab.at[dev_rows(me), chunk(c)], fwd_recv.at[me, c])
                   for c in range(CHUNKS)]

    barrier = pltpu.get_barrier_semaphore()
    for dst in near:
        pl.semaphore_signal(barrier, inc=1, device_id={'group': dst}, device_id_type=MESH)
    for dst in far:
        for c in range(CHUNKS):
            pay_copy(dst, c).start()
    for dst in near:
        pay_copy(dst, 0).start()
    pl.semaphore_wait(barrier, len(near))
    pl.semaphore_signal(far_ok, inc=1, device_id={'group': peer(way(1), 0)}, device_id_type=MESH)

    for dst in near:
        key_copy(dst).start()
        seg_copy(dst).start()
    for i in range(WAYS):
        for c in range(CHUNKS):
            pay_copy(far[i], c).wait()
        hop_out(i).start()
    pl.semaphore_wait(far_ok, 1)
    for dst in far:
        key_copy(dst).start()
        seg_copy(dst).start()
    for dst in near:
        pay_copy(dst, 0).wait()
        fwd_copy(dst, 0).start()
    for copy in own_copies:
        copy.start()
    for dst in near:
        pay_copy(dst, 1).start()

    own_copies[0].wait()
    own_copies[1].wait()
    for src in far + near:
        arrived(keys_all.at[src], key_recv.at[src])
        arrived(segs_all.at[src], seg_recv.at[src])

    def spread(dev, carry):
        for j in range(lane_tiles):
            lanes = slice(j * LANES, (j + 1) * LANES)
            dst = pl.ds(pl.multiple_of(dev * rows + j * LANES, LANES), LANES)
            kcol[dst, :] = jnp.broadcast_to(keys_all[dev, :, lanes], (LANES, LANES)).T
            scol[dst, :] = jnp.broadcast_to(segs_all[dev, :, lanes], (LANES, LANES)).T
        return carry

    lax.fori_loop(0, n, spread, 0)

    def build(t, carry):
        here = pl.ds(pl.multiple_of(t * ROW_TILE, ROW_TILE), ROW_TILE)
        key_r, seg_r = kcol[here, :], scol[here, :]
        last = jnp.full((ROW_TILE, LANES), -jnp.inf, jnp.float32)
        for dev in range(n):
            for j in range(lane_tiles):
                lanes = slice(j * LANES, (j + 1) * LANES)
                key_s, seg_s = keys_all[dev, :, lanes], segs_all[dev, :, lanes]
                other = jnp.logical_and(key_s < key_r, seg_s != seg_r)
                last = jnp.maximum(last, jnp.where(other, key_s, -jnp.inf))
        last = jnp.broadcast_to(jnp.max(last, axis=1, keepdims=True), (ROW_TILE, LANES))
        for dev in range(n):
            for j in range(lane_tiles):
                lanes = slice(j * LANES, (j + 1) * LANES)
                key_s = keys_all[dev, :, lanes]
                inside = jnp.logical_and(key_s <= key_r, key_s > last)
                at = slice(dev * rows + j * LANES, dev * rows + (j + 1) * LANES)
                mask[here, at] = jnp.where(inside, 1.0, 0.0).astype(jnp.bfloat16)
        return carry

    lax.fori_loop(0, EARLY_STEPS, build, 0)
    for i in range(WAYS):
        arrived(relay.at[i], hop_recv.at[i])
        hop_on(i).start()
    for dst in near:
        pay_copy(dst, 1).wait()
        fwd_copy(dst, 1).start()
    lax.fori_loop(EARLY_STEPS, n * rows // ROW_TILE, build, 0)

    def sums(dev, i, c):
        return jnp.dot(mask[part_rows(dev, i), :], slab[:, chunk(c)], preferred_element_type=jnp.float32).astype(jnp.bfloat16)

    def blocks(count, pick, c, before, send):
        def step_fn(step, carry):
            k, i = lax.div(step, PARTS), lax.rem(step, PARTS)
            dev = pick(k)
            res[part_rows(dev, i), chunk(c)] = sums(dev, i, c)

            if before is not None:
                @pl.when(step == 0)
                def _():
                    before.start()

            if send is not None:
                @pl.when(jnp.logical_and(i == 0, step > 0))
                def _():
                    send(k - 1).start()

            return carry

        lax.fori_loop(0, count * PARTS, step_fn, 0)

    def own_block(c, before):
        def step_fn(i, carry):
            out_ref[part_rows(0, i), columns(me, c)] = sums(me, i, c)

            if before is not None:
                @pl.when(i == 0)
                def _():
                    before.start()

            return carry

        lax.fori_loop(0, PARTS, step_fn, 0)

    def far_dev(k):
        return peer(2, k)

    def near_a(k):
        return peer(way(k), 0)

    def near_b(k):
        return peer(way(k), 1)

    def chip_dev(k):
        return peer(0, 1)

    own_copies[2].wait()
    for src in near:
        arrived(slab.at[dev_rows(src), chunk(0)], fwd_recv.at[src, 0])
    for src in far:
        arrived(slab.at[dev_rows(src), :], fwd_recv.at[src, 0])
    blocks(WAYS, far_dev, 0, None, lambda k: back_out(k, 0))
    blocks(WAYS, near_a, 0, back_out(WAYS - 1, 0), lambda k: ret_copy(near_a(k), 0))
    blocks(WAYS, near_b, 0, ret_copy(near_a(WAYS - 1), 0), None)
    blocks(1, chip_dev, 0, None, None)
    own_block(0, None)
    own_copies[3].wait()
    for src in near:
        arrived(slab.at[dev_rows(src), chunk(1)], fwd_recv.at[src, 1])
    blocks(WAYS, far_dev, 1, None, lambda k: back_out(k, 1))
    blocks(WAYS, near_a, 1, back_out(WAYS - 1, 1), lambda k: ret_copy(near_a(k), 1))
    blocks(WAYS, near_b, 1, ret_copy(near_a(WAYS - 1), 1), lambda k: ret_whole(near_b(k)))
    blocks(1, chip_dev, 1, ret_whole(near_b(WAYS - 1)), None)
    own_block(1, ret_whole(peer(0, 1)))

    for i in range(WAYS):
        arrived(relay_back.at[i], back_recv.at[i])
        back_on(i).start()

    for dst in far + near:
        key_copy(dst).wait_send()
        seg_copy(dst).wait_send()
    for c in range(CHUNKS):
        for dst in near:
            fwd_copy(dst, c).wait_send()
    for i in range(WAYS):
        hop_out(i).wait_send()
        hop_on(i).wait_send()
        for c in range(CHUNKS):
            back_out(i, c).wait_send()
            ret_copy(near_a(i), c).wait_send()
        ret_whole(near_b(i)).wait_send()
    ret_whole(peer(0, 1)).wait_send()
    for src in near + far:
        arrived(out_ref.at[:, block_cols(src)], ret_recv.at[src])
    for i in range(WAYS):
        back_on(i).wait_send()


def solution(mesh):
    n = mesh.shape['group']

    def per_device(sort_keys, seg_ids, payload):
        rows, width = payload.shape
        total = n * rows
        dma = pltpu.SemaphoreType.DMA
        block = width // n
        return pl.pallas_call(
            functools.partial(exchange_kernel, n),
            out_shape=pltpu.VMEM((rows, width), jnp.bfloat16),
            in_specs=[pl.BlockSpec(memory_space=pl.ANY)] * 3,
            out_specs=pl.BlockSpec(memory_space=pltpu.VMEM),
            scratch_shapes=[
                pltpu.VMEM((n, 1, rows), jnp.float32),
                pltpu.VMEM((n, 1, rows), jnp.int32),
                pltpu.VMEM((total, LANES), jnp.float32),
                pltpu.VMEM((total, LANES), jnp.int32),
                pltpu.VMEM((total, total), jnp.bfloat16),
                pltpu.VMEM((rows, width), jnp.bfloat16),
                pltpu.VMEM((total, block), jnp.bfloat16),
                pltpu.VMEM((total, block), jnp.bfloat16),
                pltpu.VMEM((WAYS, rows, block), jnp.bfloat16),
                pltpu.VMEM((WAYS, rows, block), jnp.bfloat16),
                pltpu.SemaphoreType.REGULAR, dma((n, CHUNKS)), dma((n,)), dma((n,)), dma((n,)), dma((n,)),
                dma((n, CHUNKS)), dma((n, CHUNKS)), dma((WAYS,)), dma((WAYS,)), dma((WAYS,)),
                dma((n, CHUNKS)), dma((n,)), dma((WAYS, CHUNKS)), dma((WAYS,)), dma((WAYS,)),
            ],
            compiler_params=pltpu.CompilerParams(collective_id=0, has_side_effects=True,
                                                 vmem_limit_bytes=56 * 1024 * 1024),
            name='exchange_sums',
        )(sort_keys.reshape(1, 1, rows), seg_ids.reshape(1, 1, rows), payload)

    row_spec = P(('batch', 'group'))
    mat_spec = P(('batch', 'group'), None)
    return jax.shard_map(per_device, mesh=mesh, in_specs=(row_spec, row_spec, mat_spec),
                         out_specs=mat_spec, check_vma=False)
```

```python
import functools

import jax
import jax.numpy as jnp
from jax import lax
from jax.experimental import pallas as pl
from jax.experimental.pallas import tpu as pltpu
from jax.sharding import PartitionSpec as P

MESH = pl.DeviceIdType.MESH
LANES = 128
CORES = 2
WAYS = 2
CHUNKS = 2
ROW_TILE = 64
EARLY_STEPS = 8
PARTS = 2


def exchange_kernel(n, keys_ref, segs_ref, pay_ref, out_ref, keys_all, segs_all, kcol, scol, mask, pay, slab, res,
                    relay, relay_back, far_ok, pay_sem, key_send, key_recv, seg_send, seg_recv, fwd_send, fwd_recv,
                    hop_send, hop_recv, on_send, ret_send, ret_recv, back_send, back_recv, back_on_send):
    me = lax.axis_index('group')
    rows, width = pay_ref.shape
    block = width // n
    cw = block // CHUNKS
    part = rows // PARTS
    lane_tiles = rows // LANES
    ring = n // CORES
    chip, core = lax.div(me, CORES), lax.rem(me, CORES)

    def peer(hop, flip):
        return lax.rem(chip + hop, ring) * CORES + lax.rem(core + flip, CORES)

    def way(i):
        return 1 + (ring - 2) * i

    near = [peer(way(i), flip) for flip in range(CORES) for i in range(WAYS)] + [peer(0, 1)]
    far = [peer(2, flip) for flip in range(CORES)]

    def remote(src, dst, send_sem, recv_sem, dev):
        return pltpu.make_async_remote_copy(src_ref=src, dst_ref=dst, send_sem=send_sem, recv_sem=recv_sem,
                                            device_id={'group': dev}, device_id_type=MESH)

    def columns(dev, c):
        return pl.ds(pl.multiple_of(dev * block + c * cw, LANES), cw)

    def block_cols(dev):
        return pl.ds(pl.multiple_of(dev * block, LANES), block)

    def chunk(c):
        return pl.ds(c * cw, cw)

    def dev_rows(dev):
        return pl.ds(pl.multiple_of(dev * rows, rows), rows)

    def part_rows(dev, i):
        return pl.ds(pl.multiple_of(dev * rows + i * part, part), part)

    def key_copy(dst):
        return remote(keys_ref.at[0], keys_all.at[me], key_send.at[dst], key_recv.at[me], dst)

    def seg_copy(dst):
        return remote(segs_ref.at[0], segs_all.at[me], seg_send.at[dst], seg_recv.at[me], dst)

    def pay_copy(dst, c):
        return pltpu.make_async_copy(pay_ref.at[:, columns(dst, c)], pay.at[:, columns(dst, c)], pay_sem.at[dst, c])

    def fwd_copy(dst, c):
        return remote(pay.at[:, columns(dst, c)], slab.at[dev_rows(me), chunk(c)], fwd_send.at[dst, c], fwd_recv.at[me, c], dst)

    def hop_out(i):
        return remote(pay.at[:, block_cols(peer(2, i))], relay.at[i], hop_send.at[i], hop_recv.at[i], peer(way(i), 0))

    def hop_on(i):
        origin = peer(way(1 - i), 0)
        return remote(relay.at[i], slab.at[dev_rows(origin), :], on_send.at[i], fwd_recv.at[origin, 0], peer(way(i), i))

    def ret_copy(dst, c):
        return remote(res.at[dev_rows(dst), chunk(c)], out_ref.at[:, columns(me, c)], ret_send.at[dst, c], ret_recv.at[me], dst)

    def ret_whole(dst):
        return remote(res.at[dev_rows(dst), :], out_ref.at[:, block_cols(me)], ret_send.at[dst, 0], ret_recv.at[me], dst)

    def back_out(i, c):
        return remote(res.at[dev_rows(peer(2, i)), chunk(c)], relay_back.at[i, :, chunk(c)], back_send.at[i, c],
                      back_recv.at[i], peer(way(i), 0))

    def back_on(i):
        origin = peer(way(1 - i), 0)
        return remote(relay_back.at[i], out_ref.at[:, block_cols(origin)], back_on_send.at[i], ret_recv.at[origin],
                      peer(way(i), i))

    def arrived(dst, sem):
        pltpu.make_async_copy(dst, dst, sem).wait()

    own_copies = [pltpu.make_async_copy(keys_ref.at[0], keys_all.at[me], key_recv.at[me]),
                  pltpu.make_async_copy(segs_ref.at[0], segs_all.at[me], seg_recv.at[me])]
    own_copies += [pltpu.make_async_copy(pay_ref.at[:, columns(me, c)], slab.at[dev_rows(me), chunk(c)], fwd_recv.at[me, c])
                   for c in range(CHUNKS)]

    barrier = pltpu.get_barrier_semaphore()
    for dst in near:
        pl.semaphore_signal(barrier, inc=1, device_id={'group': dst}, device_id_type=MESH)
    for dst in far:
        for c in range(CHUNKS):
            pay_copy(dst, c).start()
    for dst in near:
        pay_copy(dst, 0).start()
    pl.semaphore_wait(barrier, len(near))
    pl.semaphore_signal(far_ok, inc=1, device_id={'group': peer(way(1), 0)}, device_id_type=MESH)

    for i in range(WAYS):
        for c in range(CHUNKS):
            pay_copy(far[i], c).wait()
        hop_out(i).start()
    for dst in near:
        key_copy(dst).start()
        seg_copy(dst).start()
    pl.semaphore_wait(far_ok, 1)
    for dst in far:
        key_copy(dst).start()
        seg_copy(dst).start()
    for dst in near:
        pay_copy(dst, 0).wait()
        fwd_copy(dst, 0).start()
    for copy in own_copies:
        copy.start()
    for dst in near:
        pay_copy(dst, 1).start()

    own_copies[0].wait()
    own_copies[1].wait()
    for src in far + near:
        arrived(keys_all.at[src], key_recv.at[src])
        arrived(segs_all.at[src], seg_recv.at[src])

    def spread(dev, carry):
        for j in range(lane_tiles):
            lanes = slice(j * LANES, (j + 1) * LANES)
            dst = pl.ds(pl.multiple_of(dev * rows + j * LANES, LANES), LANES)
            kcol[dst, :] = jnp.broadcast_to(keys_all[dev, :, lanes], (LANES, LANES)).T
            scol[dst, :] = jnp.broadcast_to(segs_all[dev, :, lanes], (LANES, LANES)).T
        return carry

    lax.fori_loop(0, n, spread, 0)

    def build(t, carry):
        here = pl.ds(pl.multiple_of(t * ROW_TILE, ROW_TILE), ROW_TILE)
        key_r, seg_r = kcol[here, :], scol[here, :]
        last = jnp.full((ROW_TILE, LANES), -jnp.inf, jnp.float32)
        for dev in range(n):
            for j in range(lane_tiles):
                lanes = slice(j * LANES, (j + 1) * LANES)
                key_s, seg_s = keys_all[dev, :, lanes], segs_all[dev, :, lanes]
                other = jnp.logical_and(key_s < key_r, seg_s != seg_r)
                last = jnp.maximum(last, jnp.where(other, key_s, -jnp.inf))
        last = jnp.broadcast_to(jnp.max(last, axis=1, keepdims=True), (ROW_TILE, LANES))
        for dev in range(n):
            for j in range(lane_tiles):
                lanes = slice(j * LANES, (j + 1) * LANES)
                key_s = keys_all[dev, :, lanes]
                inside = jnp.logical_and(key_s <= key_r, key_s > last)
                at = slice(dev * rows + j * LANES, dev * rows + (j + 1) * LANES)
                mask[here, at] = jnp.where(inside, 1.0, 0.0).astype(jnp.bfloat16)
        return carry

    lax.fori_loop(0, EARLY_STEPS, build, 0)
    for i in range(WAYS):
        arrived(relay.at[i], hop_recv.at[i])
        hop_on(i).start()
    for dst in near:
        pay_copy(dst, 1).wait()
        fwd_copy(dst, 1).start()
    lax.fori_loop(EARLY_STEPS, n * rows // ROW_TILE, build, 0)

    def sums(dev, i, c):
        return jnp.dot(mask[part_rows(dev, i), :], slab[:, chunk(c)], preferred_element_type=jnp.float32).astype(jnp.bfloat16)

    def blocks(count, pick, c, before, send):
        def step_fn(step, carry):
            k, i = lax.div(step, PARTS), lax.rem(step, PARTS)
            dev = pick(k)
            res[part_rows(dev, i), chunk(c)] = sums(dev, i, c)

            if before is not None:
                @pl.when(step == 0)
                def _():
                    before.start()

            if send is not None:
                @pl.when(jnp.logical_and(i == 0, step > 0))
                def _():
                    send(k - 1).start()

            return carry

        lax.fori_loop(0, count * PARTS, step_fn, 0)

    def own_block(c, before):
        def step_fn(i, carry):
            out_ref[part_rows(0, i), columns(me, c)] = sums(me, i, c)

            if before is not None:
                @pl.when(i == 0)
                def _():
                    before.start()

            return carry

        lax.fori_loop(0, PARTS, step_fn, 0)

    def far_dev(k):
        return peer(2, k)

    def near_a(k):
        return peer(way(k), 0)

    def near_b(k):
        return peer(way(k), 1)

    def chip_dev(k):
        return peer(0, 1)

    own_copies[2].wait()
    for src in near:
        arrived(slab.at[dev_rows(src), chunk(0)], fwd_recv.at[src, 0])
    for src in far:
        arrived(slab.at[dev_rows(src), :], fwd_recv.at[src, 0])
    blocks(WAYS, far_dev, 0, None, lambda k: back_out(k, 0))
    blocks(WAYS, near_a, 0, back_out(WAYS - 1, 0), lambda k: ret_copy(near_a(k), 0))
    blocks(WAYS, near_b, 0, ret_copy(near_a(WAYS - 1), 0), None)
    blocks(1, chip_dev, 0, None, None)
    own_block(0, None)
    own_copies[3].wait()
    for src in near:
        arrived(slab.at[dev_rows(src), chunk(1)], fwd_recv.at[src, 1])
    blocks(WAYS, near_a, 1, None, lambda k: ret_copy(near_a(k), 1))
    blocks(WAYS, far_dev, 1, ret_copy(near_a(WAYS - 1), 1), lambda k: back_out(k, 1))
    blocks(WAYS, near_b, 1, back_out(WAYS - 1, 1), lambda k: ret_whole(near_b(k)))
    blocks(1, chip_dev, 1, ret_whole(near_b(WAYS - 1)), None)
    own_block(1, ret_whole(peer(0, 1)))

    for i in range(WAYS):
        arrived(relay_back.at[i], back_recv.at[i])
        back_on(i).start()

    for dst in far + near:
        key_copy(dst).wait_send()
        seg_copy(dst).wait_send()
    for c in range(CHUNKS):
        for dst in near:
            fwd_copy(dst, c).wait_send()
    for i in range(WAYS):
        hop_out(i).wait_send()
        hop_on(i).wait_send()
        for c in range(CHUNKS):
            back_out(i, c).wait_send()
            ret_copy(near_a(i), c).wait_send()
        ret_whole(near_b(i)).wait_send()
    ret_whole(peer(0, 1)).wait_send()
    for src in near + far:
        arrived(out_ref.at[:, block_cols(src)], ret_recv.at[src])
    for i in range(WAYS):
        back_on(i).wait_send()


def solution(mesh):
    n = mesh.shape['group']

    def per_device(sort_keys, seg_ids, payload):
        rows, width = payload.shape
        total = n * rows
        dma = pltpu.SemaphoreType.DMA
        block = width // n
        return pl.pallas_call(
            functools.partial(exchange_kernel, n),
            out_shape=pltpu.VMEM((rows, width), jnp.bfloat16),
            in_specs=[pl.BlockSpec(memory_space=pl.ANY)] * 3,
            out_specs=pl.BlockSpec(memory_space=pltpu.VMEM),
            scratch_shapes=[
                pltpu.VMEM((n, 1, rows), jnp.float32),
                pltpu.VMEM((n, 1, rows), jnp.int32),
                pltpu.VMEM((total, LANES), jnp.float32),
                pltpu.VMEM((total, LANES), jnp.int32),
                pltpu.VMEM((total, total), jnp.bfloat16),
                pltpu.VMEM((rows, width), jnp.bfloat16),
                pltpu.VMEM((total, block), jnp.bfloat16),
                pltpu.VMEM((total, block), jnp.bfloat16),
                pltpu.VMEM((WAYS, rows, block), jnp.bfloat16),
                pltpu.VMEM((WAYS, rows, block), jnp.bfloat16),
                pltpu.SemaphoreType.REGULAR, dma((n, CHUNKS)), dma((n,)), dma((n,)), dma((n,)), dma((n,)),
                dma((n, CHUNKS)), dma((n, CHUNKS)), dma((WAYS,)), dma((WAYS,)), dma((WAYS,)),
                dma((n, CHUNKS)), dma((n,)), dma((WAYS, CHUNKS)), dma((WAYS,)), dma((WAYS,)),
            ],
            compiler_params=pltpu.CompilerParams(collective_id=0, has_side_effects=True,
                                                 vmem_limit_bytes=56 * 1024 * 1024),
            name='exchange_sums',
        )(sort_keys.reshape(1, 1, rows), seg_ids.reshape(1, 1, rows), payload)

    row_spec = P(('batch', 'group'))
    mat_spec = P(('batch', 'group'), None)
    return jax.shard_map(per_device, mesh=mesh, in_specs=(row_spec, row_spec, mat_spec),
                         out_specs=mat_spec, check_vma=False)
```

```python
import functools

import jax
import jax.numpy as jnp
from jax import lax
from jax.experimental import pallas as pl
from jax.experimental.pallas import tpu as pltpu
from jax.sharding import PartitionSpec as P

MESH = pl.DeviceIdType.MESH
LANES = 128
CORES = 2
WAYS = 2
CHUNKS = 2
ROW_TILE = 64
EARLY_STEPS = 8
STORES = 8
PARTS = 2


def exchange_kernel(n, keys_ref, segs_ref, pay_ref, out_ref, keys_all, segs_all, kcol, scol, mask, pay, slab, res,
                    relay, relay_back, far_ok, pay_sem, key_send, key_recv, seg_send, seg_recv, fwd_send, fwd_recv,
                    hop_send, hop_recv, on_send, ret_send, ret_recv, back_send, back_recv, back_on_send):
    me = lax.axis_index('group')
    rows, width = pay_ref.shape
    block = width // n
    cw = block // CHUNKS
    part = rows // PARTS
    lane_tiles = rows // LANES
    ring = n // CORES
    chip, core = lax.div(me, CORES), lax.rem(me, CORES)

    def peer(hop, flip):
        return lax.rem(chip + hop, ring) * CORES + lax.rem(core + flip, CORES)

    def way(i):
        return 1 + (ring - 2) * i

    near = [peer(way(i), flip) for flip in range(CORES) for i in range(WAYS)] + [peer(0, 1)]
    far = [peer(2, flip) for flip in range(CORES)]

    def remote(src, dst, send_sem, recv_sem, dev):
        return pltpu.make_async_remote_copy(src_ref=src, dst_ref=dst, send_sem=send_sem, recv_sem=recv_sem,
                                            device_id={'group': dev}, device_id_type=MESH)

    def columns(dev, c):
        return pl.ds(pl.multiple_of(dev * block + c * cw, LANES), cw)

    def block_cols(dev):
        return pl.ds(pl.multiple_of(dev * block, LANES), block)

    def chunk(c):
        return pl.ds(c * cw, cw)

    def dev_rows(dev):
        return pl.ds(pl.multiple_of(dev * rows, rows), rows)

    def part_rows(dev, i):
        return pl.ds(pl.multiple_of(dev * rows + i * part, part), part)

    def key_copy(dst):
        return remote(keys_ref.at[0], keys_all.at[me], key_send.at[dst], key_recv.at[me], dst)

    def seg_copy(dst):
        return remote(segs_ref.at[0], segs_all.at[me], seg_send.at[dst], seg_recv.at[me], dst)

    def pay_copy(dst, c):
        return pltpu.make_async_copy(pay_ref.at[:, columns(dst, c)], pay.at[:, columns(dst, c)], pay_sem.at[dst, c])

    def fwd_copy(dst, c):
        return remote(pay.at[:, columns(dst, c)], slab.at[dev_rows(me), chunk(c)], fwd_send.at[dst, c], fwd_recv.at[me, c], dst)

    def hop_out(i):
        return remote(pay.at[:, block_cols(peer(2, i))], relay.at[i], hop_send.at[i], hop_recv.at[i], peer(way(i), 0))

    def hop_on(i):
        origin = peer(way(1 - i), 0)
        return remote(relay.at[i], slab.at[dev_rows(origin), :], on_send.at[i], fwd_recv.at[origin, 0], peer(way(i), i))

    def ret_copy(dst, c):
        return remote(res.at[dev_rows(dst), chunk(c)], out_ref.at[:, columns(me, c)], ret_send.at[dst, c], ret_recv.at[me], dst)

    def ret_whole(dst):
        return remote(res.at[dev_rows(dst), :], out_ref.at[:, block_cols(me)], ret_send.at[dst, 0], ret_recv.at[me], dst)

    def back_out(i, c):
        return remote(res.at[dev_rows(peer(2, i)), chunk(c)], relay_back.at[i, :, chunk(c)], back_send.at[i, c],
                      back_recv.at[i], peer(way(i), 0))

    def back_on(i):
        origin = peer(way(1 - i), 0)
        return remote(relay_back.at[i], out_ref.at[:, block_cols(origin)], back_on_send.at[i], ret_recv.at[origin],
                      peer(way(i), i))

    def arrived(dst, sem):
        pltpu.make_async_copy(dst, dst, sem).wait()

    own_copies = [pltpu.make_async_copy(keys_ref.at[0], keys_all.at[me], key_recv.at[me]),
                  pltpu.make_async_copy(segs_ref.at[0], segs_all.at[me], seg_recv.at[me])]
    own_copies += [pltpu.make_async_copy(pay_ref.at[:, columns(me, c)], slab.at[dev_rows(me), chunk(c)], fwd_recv.at[me, c])
                   for c in range(CHUNKS)]

    barrier = pltpu.get_barrier_semaphore()
    for dst in near:
        pl.semaphore_signal(barrier, inc=1, device_id={'group': dst}, device_id_type=MESH)
    for dst in far:
        for c in range(CHUNKS):
            pay_copy(dst, c).start()
    for dst in near:
        pay_copy(dst, 0).start()
    pl.semaphore_wait(barrier, len(near))
    pl.semaphore_signal(far_ok, inc=1, device_id={'group': peer(way(1), 0)}, device_id_type=MESH)

    for dst in near:
        key_copy(dst).start()
        seg_copy(dst).start()
    for i in range(WAYS):
        for c in range(CHUNKS):
            pay_copy(far[i], c).wait()
        hop_out(i).start()
    pl.semaphore_wait(far_ok, 1)
    for dst in far:
        key_copy(dst).start()
        seg_copy(dst).start()
    for dst in near:
        pay_copy(dst, 0).wait()
        fwd_copy(dst, 0).start()
    for copy in own_copies:
        copy.start()
    for dst in near:
        pay_copy(dst, 1).start()

    own_copies[0].wait()
    own_copies[1].wait()
    for src in far + near:
        arrived(keys_all.at[src], key_recv.at[src])
        arrived(segs_all.at[src], seg_recv.at[src])

    def spread(dev, carry):
        for j in range(lane_tiles):
            lanes = slice(j * LANES, (j + 1) * LANES)
            dst = pl.ds(pl.multiple_of(dev * rows + j * LANES, LANES), LANES)
            kcol[dst, :] = jnp.broadcast_to(keys_all[dev, :, lanes], (LANES, LANES)).T
            scol[dst, :] = jnp.broadcast_to(segs_all[dev, :, lanes], (LANES, LANES)).T
        return carry

    lax.fori_loop(0, n, spread, 0)

    def build(t, carry):
        here = pl.ds(pl.multiple_of(t * ROW_TILE, ROW_TILE), ROW_TILE)
        key_r, seg_r = kcol[here, :], scol[here, :]
        last = jnp.full((ROW_TILE, LANES), -jnp.inf, jnp.float32)
        for dev in range(n):
            for j in range(lane_tiles):
                lanes = slice(j * LANES, (j + 1) * LANES)
                key_s, seg_s = keys_all[dev, :, lanes], segs_all[dev, :, lanes]
                other = jnp.logical_and(key_s < key_r, seg_s != seg_r)
                last = jnp.maximum(last, jnp.where(other, key_s, -jnp.inf))
        last = jnp.broadcast_to(jnp.max(last, axis=1, keepdims=True), (ROW_TILE, LANES))
        for dev in range(n):
            for j in range(lane_tiles):
                lanes = slice(j * LANES, (j + 1) * LANES)
                key_s = keys_all[dev, :, lanes]
                inside = jnp.logical_and(key_s <= key_r, key_s > last)
                at = slice(dev * rows + j * LANES, dev * rows + (j + 1) * LANES)
                mask[here, at] = jnp.where(inside, 1.0, 0.0).astype(jnp.bfloat16)
        return carry

    lax.fori_loop(0, EARLY_STEPS, build, 0)
    for i in range(WAYS):
        arrived(relay.at[i], hop_recv.at[i])
        hop_on(i).start()
    for dst in near:
        pay_copy(dst, 1).wait()
        fwd_copy(dst, 1).start()
    lax.fori_loop(EARLY_STEPS, n * rows // ROW_TILE, build, 0)

    def sums(dev, i, c):
        return jnp.dot(mask[part_rows(dev, i), :], slab[:, chunk(c)], preferred_element_type=jnp.float32).astype(jnp.bfloat16)

    def blocks(count, pick, c, before, send):
        def step_fn(step, carry):
            k, i = lax.div(step, PARTS), lax.rem(step, PARTS)
            dev = pick(k)
            res[part_rows(dev, i), chunk(c)] = sums(dev, i, c)

            if before is not None:
                @pl.when(step == 0)
                def _():
                    before.start()

            if send is not None:
                @pl.when(jnp.logical_and(i == 0, step > 0))
                def _():
                    send(k - 1).start()

            return carry

        lax.fori_loop(0, count * PARTS, step_fn, 0)

    def own_block(c, before):
        def step_fn(i, carry):
            out_ref[part_rows(0, i), columns(me, c)] = sums(me, i, c)

            if before is not None:
                @pl.when(i == 0)
                def _():
                    before.start()

            return carry

        lax.fori_loop(0, PARTS, step_fn, 0)

    def far_dev(k):
        return peer(2, k)

    def near_a(k):
        return peer(way(k), 0)

    def near_b(k):
        return peer(way(k), 1)

    def chip_dev(k):
        return peer(0, 1)

    own_copies[2].wait()
    for src in near:
        arrived(slab.at[dev_rows(src), chunk(0)], fwd_recv.at[src, 0])
    for src in far:
        arrived(slab.at[dev_rows(src), :], fwd_recv.at[src, 0])
    blocks(WAYS, far_dev, 0, None, lambda k: back_out(k, 0))
    blocks(WAYS, near_a, 0, back_out(WAYS - 1, 0), lambda k: ret_copy(near_a(k), 0))
    blocks(WAYS, near_b, 0, ret_copy(near_a(WAYS - 1), 0), None)
    blocks(1, chip_dev, 0, None, None)
    own_block(0, None)
    own_copies[3].wait()
    for src in near:
        arrived(slab.at[dev_rows(src), chunk(1)], fwd_recv.at[src, 1])
    blocks(WAYS, near_a, 1, None, lambda k: ret_copy(near_a(k), 1))
    blocks(WAYS, far_dev, 1, ret_copy(near_a(WAYS - 1), 1), lambda k: back_out(k, 1))
    blocks(WAYS, near_b, 1, back_out(WAYS - 1, 1), lambda k: ret_whole(near_b(k)))
    blocks(1, chip_dev, 1, ret_whole(near_b(WAYS - 1)), None)
    own_block(1, ret_whole(peer(0, 1)))

    for i in range(WAYS):
        arrived(relay_back.at[i], back_recv.at[i])
        back_on(i).start()

    for dst in far + near:
        key_copy(dst).wait_send()
        seg_copy(dst).wait_send()
    for c in range(CHUNKS):
        for dst in near:
            fwd_copy(dst, c).wait_send()
    for i in range(WAYS):
        hop_out(i).wait_send()
        hop_on(i).wait_send()
        for c in range(CHUNKS):
            back_out(i, c).wait_send()
            ret_copy(near_a(i), c).wait_send()
        ret_whole(near_b(i)).wait_send()
    ret_whole(peer(0, 1)).wait_send()
    for src in near + far:
        arrived(out_ref.at[:, block_cols(src)], ret_recv.at[src])
    for i in range(WAYS):
        back_on(i).wait_send()


def store_kernel(src_ref, dst_ref, sem):
    rows = src_ref.shape[0] // STORES
    copies = [pltpu.make_async_copy(src_ref.at[pl.ds(i * rows, rows), :], dst_ref.at[pl.ds(i * rows, rows), :], sem.at[i])
              for i in range(STORES)]
    for copy in copies:
        copy.start()
    for copy in copies:
        copy.wait()


def solution(mesh):
    n = mesh.shape['group']

    def per_device(sort_keys, seg_ids, payload):
        rows, width = payload.shape
        total = n * rows
        dma = pltpu.SemaphoreType.DMA
        block = width // n
        result = pl.pallas_call(
            functools.partial(exchange_kernel, n),
            out_shape=pltpu.VMEM((rows, width), jnp.bfloat16),
            in_specs=[pl.BlockSpec(memory_space=pl.ANY)] * 3,
            out_specs=pl.BlockSpec(memory_space=pltpu.VMEM),
            scratch_shapes=[
                pltpu.VMEM((n, 1, rows), jnp.float32),
                pltpu.VMEM((n, 1, rows), jnp.int32),
                pltpu.VMEM((total, LANES), jnp.float32),
                pltpu.VMEM((total, LANES), jnp.int32),
                pltpu.VMEM((total, total), jnp.bfloat16),
                pltpu.VMEM((rows, width), jnp.bfloat16),
                pltpu.VMEM((total, block), jnp.bfloat16),
                pltpu.VMEM((total, block), jnp.bfloat16),
                pltpu.VMEM((WAYS, rows, block), jnp.bfloat16),
                pltpu.VMEM((WAYS, rows, block), jnp.bfloat16),
                pltpu.SemaphoreType.REGULAR, dma((n, CHUNKS)), dma((n,)), dma((n,)), dma((n,)), dma((n,)),
                dma((n, CHUNKS)), dma((n, CHUNKS)), dma((WAYS,)), dma((WAYS,)), dma((WAYS,)),
                dma((n, CHUNKS)), dma((n,)), dma((WAYS, CHUNKS)), dma((WAYS,)), dma((WAYS,)),
            ],
            compiler_params=pltpu.CompilerParams(collective_id=0, has_side_effects=True,
                                                 vmem_limit_bytes=56 * 1024 * 1024),
            name='exchange_sums',
        )(sort_keys.reshape(1, 1, rows), seg_ids.reshape(1, 1, rows), payload)
        return pl.pallas_call(
            store_kernel,
            out_shape=jax.ShapeDtypeStruct((rows, width), jnp.bfloat16),
            in_specs=[pl.BlockSpec(memory_space=pl.ANY)],
            out_specs=pl.BlockSpec(memory_space=pl.ANY),
            scratch_shapes=[dma((STORES,))],
            compiler_params=pltpu.CompilerParams(vmem_limit_bytes=1024 * 1024),
            name='store_result',
        )(pltpu.with_memory_space_constraint(result, pltpu.VMEM))

    row_spec = P(('batch', 'group'))
    mat_spec = P(('batch', 'group'), None)
    return jax.shard_map(per_device, mesh=mesh, in_specs=(row_spec, row_spec, mat_spec),
                         out_specs=mat_spec, check_vma=False)
```

```python
import functools

import jax
import jax.numpy as jnp
from jax import lax
from jax.experimental import pallas as pl
from jax.experimental.pallas import tpu as pltpu
from jax.sharding import PartitionSpec as P

MESH = pl.DeviceIdType.MESH
LANES = 128
CORES = 2
WAYS = 2
CHUNKS = 2
ROW_TILE = 64
EARLY_STEPS = 4
PARTS = 2


def exchange_kernel(n, keys_ref, segs_ref, pay_ref, out_ref, keys_all, segs_all, kcol, scol, mask, pay, slab, res,
                    relay, relay_back, far_ok, pay_sem, key_send, key_recv, seg_send, seg_recv, fwd_send, fwd_recv,
                    hop_send, hop_recv, on_send, ret_send, ret_recv, back_send, back_recv, back_on_send):
    me = lax.axis_index('group')
    rows, width = pay_ref.shape
    block = width // n
    cw = block // CHUNKS
    part = rows // PARTS
    lane_tiles = rows // LANES
    ring = n // CORES
    chip, core = lax.div(me, CORES), lax.rem(me, CORES)

    def peer(hop, flip):
        return lax.rem(chip + hop, ring) * CORES + lax.rem(core + flip, CORES)

    def way(i):
        return 1 + (ring - 2) * i

    near = [peer(way(i), flip) for flip in range(CORES) for i in range(WAYS)] + [peer(0, 1)]
    far = [peer(2, flip) for flip in range(CORES)]

    def remote(src, dst, send_sem, recv_sem, dev):
        return pltpu.make_async_remote_copy(src_ref=src, dst_ref=dst, send_sem=send_sem, recv_sem=recv_sem,
                                            device_id={'group': dev}, device_id_type=MESH)

    def columns(dev, c):
        return pl.ds(pl.multiple_of(dev * block + c * cw, LANES), cw)

    def block_cols(dev):
        return pl.ds(pl.multiple_of(dev * block, LANES), block)

    def chunk(c):
        return pl.ds(c * cw, cw)

    def dev_rows(dev):
        return pl.ds(pl.multiple_of(dev * rows, rows), rows)

    def part_rows(dev, i):
        return pl.ds(pl.multiple_of(dev * rows + i * part, part), part)

    def key_copy(dst):
        return remote(keys_ref.at[0], keys_all.at[me], key_send.at[dst], key_recv.at[me], dst)

    def seg_copy(dst):
        return remote(segs_ref.at[0], segs_all.at[me], seg_send.at[dst], seg_recv.at[me], dst)

    def pay_copy(dst, c):
        return pltpu.make_async_copy(pay_ref.at[:, columns(dst, c)], pay.at[:, columns(dst, c)], pay_sem.at[dst, c])

    def fwd_copy(dst, c):
        return remote(pay.at[:, columns(dst, c)], slab.at[dev_rows(me), chunk(c)], fwd_send.at[dst, c], fwd_recv.at[me, c], dst)

    def hop_out(i):
        return remote(pay.at[:, block_cols(peer(2, i))], relay.at[i], hop_send.at[i], hop_recv.at[i], peer(way(i), 0))

    def hop_on(i):
        origin = peer(way(1 - i), 0)
        return remote(relay.at[i], slab.at[dev_rows(origin), :], on_send.at[i], fwd_recv.at[origin, 0], peer(way(i), i))

    def ret_copy(dst, c):
        return remote(res.at[dev_rows(dst), chunk(c)], out_ref.at[:, columns(me, c)], ret_send.at[dst, c], ret_recv.at[me], dst)

    def ret_whole(dst):
        return remote(res.at[dev_rows(dst), :], out_ref.at[:, block_cols(me)], ret_send.at[dst, 0], ret_recv.at[me], dst)

    def back_out(i, c):
        return remote(res.at[dev_rows(peer(2, i)), chunk(c)], relay_back.at[i, :, chunk(c)], back_send.at[i, c],
                      back_recv.at[i], peer(way(i), 0))

    def back_on(i):
        origin = peer(way(1 - i), 0)
        return remote(relay_back.at[i], out_ref.at[:, block_cols(origin)], back_on_send.at[i], ret_recv.at[origin],
                      peer(way(i), i))

    def arrived(dst, sem):
        pltpu.make_async_copy(dst, dst, sem).wait()

    own_copies = [pltpu.make_async_copy(keys_ref.at[0], keys_all.at[me], key_recv.at[me]),
                  pltpu.make_async_copy(segs_ref.at[0], segs_all.at[me], seg_recv.at[me])]
    own_copies += [pltpu.make_async_copy(pay_ref.at[:, columns(me, c)], slab.at[dev_rows(me), chunk(c)], fwd_recv.at[me, c])
                   for c in range(CHUNKS)]

    barrier = pltpu.get_barrier_semaphore()
    for dst in near:
        pl.semaphore_signal(barrier, inc=1, device_id={'group': dst}, device_id_type=MESH)
    for dst in far:
        for c in range(CHUNKS):
            pay_copy(dst, c).start()
    for dst in near:
        pay_copy(dst, 0).start()
    pl.semaphore_wait(barrier, len(near))
    pl.semaphore_signal(far_ok, inc=1, device_id={'group': peer(way(1), 0)}, device_id_type=MESH)

    for dst in near:
        key_copy(dst).start()
        seg_copy(dst).start()
    for i in range(WAYS):
        for c in range(CHUNKS):
            pay_copy(far[i], c).wait()
        hop_out(i).start()
    pl.semaphore_wait(far_ok, 1)
    for dst in far:
        key_copy(dst).start()
        seg_copy(dst).start()
    for dst in near:
        pay_copy(dst, 0).wait()
        fwd_copy(dst, 0).start()
    for copy in own_copies:
        copy.start()
    for dst in near:
        pay_copy(dst, 1).start()

    own_copies[0].wait()
    own_copies[1].wait()
    for src in far + near:
        arrived(keys_all.at[src], key_recv.at[src])
        arrived(segs_all.at[src], seg_recv.at[src])

    def spread(dev, carry):
        for j in range(lane_tiles):
            lanes = slice(j * LANES, (j + 1) * LANES)
            dst = pl.ds(pl.multiple_of(dev * rows + j * LANES, LANES), LANES)
            kcol[dst, :] = jnp.broadcast_to(keys_all[dev, :, lanes], (LANES, LANES)).T
            scol[dst, :] = jnp.broadcast_to(segs_all[dev, :, lanes], (LANES, LANES)).T
        return carry

    lax.fori_loop(0, n, spread, 0)

    def build(t, carry):
        here = pl.ds(pl.multiple_of(t * ROW_TILE, ROW_TILE), ROW_TILE)
        key_r, seg_r = kcol[here, :], scol[here, :]
        last = jnp.full((ROW_TILE, LANES), -jnp.inf, jnp.float32)
        for dev in range(n):
            for j in range(lane_tiles):
                lanes = slice(j * LANES, (j + 1) * LANES)
                key_s, seg_s = keys_all[dev, :, lanes], segs_all[dev, :, lanes]
                other = jnp.logical_and(key_s < key_r, seg_s != seg_r)
                last = jnp.maximum(last, jnp.where(other, key_s, -jnp.inf))
        last = jnp.broadcast_to(jnp.max(last, axis=1, keepdims=True), (ROW_TILE, LANES))
        for dev in range(n):
            for j in range(lane_tiles):
                lanes = slice(j * LANES, (j + 1) * LANES)
                key_s = keys_all[dev, :, lanes]
                inside = jnp.logical_and(key_s <= key_r, key_s > last)
                at = slice(dev * rows + j * LANES, dev * rows + (j + 1) * LANES)
                mask[here, at] = jnp.where(inside, 1.0, 0.0).astype(jnp.bfloat16)
        return carry

    lax.fori_loop(0, EARLY_STEPS, build, 0)
    for i in range(WAYS):
        arrived(relay.at[i], hop_recv.at[i])
        hop_on(i).start()
    for dst in near:
        pay_copy(dst, 1).wait()
        fwd_copy(dst, 1).start()
    lax.fori_loop(EARLY_STEPS, n * rows // ROW_TILE, build, 0)

    def sums(dev, i, c):
        return jnp.dot(mask[part_rows(dev, i), :], slab[:, chunk(c)], preferred_element_type=jnp.float32).astype(jnp.bfloat16)

    def blocks(count, pick, c, before, send):
        def step_fn(step, carry):
            k, i = lax.div(step, PARTS), lax.rem(step, PARTS)
            dev = pick(k)
            res[part_rows(dev, i), chunk(c)] = sums(dev, i, c)

            if before is not None:
                @pl.when(step == 0)
                def _():
                    before.start()

            if send is not None:
                @pl.when(jnp.logical_and(i == 0, step > 0))
                def _():
                    send(k - 1).start()

            return carry

        lax.fori_loop(0, count * PARTS, step_fn, 0)

    def own_block(c, before):
        def step_fn(i, carry):
            out_ref[part_rows(0, i), columns(me, c)] = sums(me, i, c)

            if before is not None:
                @pl.when(i == 0)
                def _():
                    before.start()

            return carry

        lax.fori_loop(0, PARTS, step_fn, 0)

    def far_dev(k):
        return peer(2, k)

    def near_a(k):
        return peer(way(k), 0)

    def near_b(k):
        return peer(way(k), 1)

    def chip_dev(k):
        return peer(0, 1)

    own_copies[2].wait()
    for src in near:
        arrived(slab.at[dev_rows(src), chunk(0)], fwd_recv.at[src, 0])
    for src in far:
        arrived(slab.at[dev_rows(src), :], fwd_recv.at[src, 0])
    blocks(WAYS, far_dev, 0, None, lambda k: back_out(k, 0))
    blocks(WAYS, near_a, 0, back_out(WAYS - 1, 0), lambda k: ret_copy(near_a(k), 0))
    blocks(WAYS, near_b, 0, ret_copy(near_a(WAYS - 1), 0), None)
    blocks(1, chip_dev, 0, None, None)
    own_block(0, None)
    own_copies[3].wait()
    for src in near:
        arrived(slab.at[dev_rows(src), chunk(1)], fwd_recv.at[src, 1])
    blocks(WAYS, near_a, 1, None, lambda k: ret_copy(near_a(k), 1))
    blocks(WAYS, far_dev, 1, ret_copy(near_a(WAYS - 1), 1), lambda k: back_out(k, 1))
    blocks(WAYS, near_b, 1, back_out(WAYS - 1, 1), lambda k: ret_whole(near_b(k)))
    blocks(1, chip_dev, 1, ret_whole(near_b(WAYS - 1)), None)
    own_block(1, ret_whole(peer(0, 1)))

    for i in range(WAYS):
        arrived(relay_back.at[i], back_recv.at[i])
        back_on(i).start()

    for dst in far + near:
        key_copy(dst).wait_send()
        seg_copy(dst).wait_send()
    for c in range(CHUNKS):
        for dst in near:
            fwd_copy(dst, c).wait_send()
    for i in range(WAYS):
        hop_out(i).wait_send()
        hop_on(i).wait_send()
        for c in range(CHUNKS):
            back_out(i, c).wait_send()
            ret_copy(near_a(i), c).wait_send()
        ret_whole(near_b(i)).wait_send()
    ret_whole(peer(0, 1)).wait_send()
    for src in near + far:
        arrived(out_ref.at[:, block_cols(src)], ret_recv.at[src])
    for i in range(WAYS):
        back_on(i).wait_send()


def solution(mesh):
    n = mesh.shape['group']

    def per_device(sort_keys, seg_ids, payload):
        rows, width = payload.shape
        total = n * rows
        dma = pltpu.SemaphoreType.DMA
        block = width // n
        return pl.pallas_call(
            functools.partial(exchange_kernel, n),
            out_shape=pltpu.VMEM((rows, width), jnp.bfloat16),
            in_specs=[pl.BlockSpec(memory_space=pl.ANY)] * 3,
            out_specs=pl.BlockSpec(memory_space=pltpu.VMEM),
            scratch_shapes=[
                pltpu.VMEM((n, 1, rows), jnp.float32),
                pltpu.VMEM((n, 1, rows), jnp.int32),
                pltpu.VMEM((total, LANES), jnp.float32),
                pltpu.VMEM((total, LANES), jnp.int32),
                pltpu.VMEM((total, total), jnp.bfloat16),
                pltpu.VMEM((rows, width), jnp.bfloat16),
                pltpu.VMEM((total, block), jnp.bfloat16),
                pltpu.VMEM((total, block), jnp.bfloat16),
                pltpu.VMEM((WAYS, rows, block), jnp.bfloat16),
                pltpu.VMEM((WAYS, rows, block), jnp.bfloat16),
                pltpu.SemaphoreType.REGULAR, dma((n, CHUNKS)), dma((n,)), dma((n,)), dma((n,)), dma((n,)),
                dma((n, CHUNKS)), dma((n, CHUNKS)), dma((WAYS,)), dma((WAYS,)), dma((WAYS,)),
                dma((n, CHUNKS)), dma((n,)), dma((WAYS, CHUNKS)), dma((WAYS,)), dma((WAYS,)),
            ],
            compiler_params=pltpu.CompilerParams(collective_id=0, has_side_effects=True,
                                                 vmem_limit_bytes=56 * 1024 * 1024),
            name='exchange_sums',
        )(sort_keys.reshape(1, 1, rows), seg_ids.reshape(1, 1, rows), payload)

    row_spec = P(('batch', 'group'))
    mat_spec = P(('batch', 'group'), None)
    return jax.shard_map(per_device, mesh=mesh, in_specs=(row_spec, row_spec, mat_spec),
                         out_specs=mat_spec, check_vma=False)
```
